512 devices in a mesh: gz: 4 (over z_lo), gy: 16 (over z_hi, y), gx: 8 (over x, core).
Axes of the slice: x: 4, y: 4, z: 16 (z_hi: 4, z_lo: 4; z = z_hi * 4 + z_lo), core: 2. Of those that a mesh axis runs over, the one named last changes fastest.
Arguments:
- fine_now: float32 [3, 16, 256, 2048], P(None, 'gz', 'gy', 'gx'), may hold values from -6 to 6
- fine_prev: float32 [3, 16, 256, 2048], P(None, 'gz', 'gy', 'gx'), may hold values from -6 to 6
- stiffness: float32 [9, 16, 256, 2048], P(None, 'gz', 'gy', 'gx'), may hold values from 0 to 6, as said below
- metric: float32 [16, 256, 2048], P('gz', 'gy', 'gx'), may hold values from 0.7 to 1.4
- density: float32 [16, 256, 2048], P('gz', 'gy', 'gx'), may hold values from 1 to 2
- coarse_now: float32 [3, 32, 128, 1024], P(None, 'gz', 'gy', 'gx'), may hold values from -6 to 6
- coarse_prev: float32 [3, 32, 128, 1024], P(None, 'gz', 'gy', 'gx'), may hold values from -6 to 6
- coarse_stiffness: float32 [9, 32, 128, 1024], P(None, 'gz', 'gy', 'gx'), may hold values from 0 to 24, as said below
- coarse_density: float32 [32, 128, 1024], P('gz', 'gy', 'gx'), may hold values from 1.5 to 3
Outputs:
- fine_next: float32 [3, 16, 256, 2048], P(None, 'gz', 'gy', 'gx')
- coarse_next: float32 [3, 32, 128, 1024], P(None, 'gz', 'gy', 'gx')
The draws below stay inside these ranges and needn't reach their ends.
Inputs may be any that keep to these rules, and one draw needn't show every extreme that they name: `stiffness`: channels 0 to 5 lie in [2, 6] and channels 6 to 8 in [0, 0.9]. `coarse_stiffness`: channels 0 to 5 lie in [8, 24] and channels 6 to 8 in [0, 3.6].
All inputs are finite; a program needn't handle non-finite values.
Results may differ from the reference program's by a relative error of at most 0.00002.
Values sent between devices are 32-bit elements; how exact they have to be, the bound alone decides.
A program may use at most 64 MiB of HBM per device.

```python
import math
import jax
import jax.numpy as jnp
from jax import lax

ITERS = 3
NX = 2048
NY = 256
NZF = 16
NZC = 32


def stiff_values(key, lowest, highest, shape):
    first_key, second_key = jax.random.split(key)
    main_part = jnp.exp(jax.random.uniform(first_key, (6,) + shape, jnp.float32, jnp.log(lowest), jnp.log(highest)))
    cross_part = jax.random.uniform(second_key, (3,) + shape, jnp.float32, 0.0, 0.45 * lowest)
    return jnp.concatenate([main_part, cross_part], 0)


def draw_stiffness(key, part):
    return stiff_values(jax.random.fold_in(key, 11), 2.0, 6.0, (NZF, NY, NX))


def draw_coarse_stiffness(key, part):
    return stiff_values(jax.random.fold_in(key, 23), 8.0, 24.0, (NZC, NY // 2, NX // 2))


def levels(key, extent, cuts, least, high):
    gain = 1.0
    for axis_at, shards_of in cuts:
        heights = jax.random.uniform(jax.random.fold_in(jax.random.fold_in(key, 6), axis_at), (shards_of,), jnp.float32, least / len(cuts), high / len(cuts))
        gain = gain * jnp.repeat(jnp.exp(heights), extent[axis_at] // shards_of).reshape((-1,) + (1,) * (len(extent) - 1 - axis_at))
    return gain


def bell_draw(stream_key, shape, width, reach, cuts=(), kind=jnp.bfloat16):
    values = jax.random.normal(stream_key, shape, jnp.float32) * width
    if len(cuts) > 0:
        values = levels(stream_key, shape, cuts, -0.22, 0.18) * values
    return jnp.clip(values, min=-reach, max=reach).astype(kind)


def setup_inputs(seed: int = 0) -> dict:
    key_of = jax.random.split(jax.random.key(seed), 10)
    return {
        "fine_now": bell_draw(key_of[0], (3, NZF, NY, NX), 1.0, 6.0, ((1, 4), (2, 16), (3, 8)), jnp.float32),
        "fine_prev": bell_draw(key_of[1], (3, NZF, NY, NX), 1.0, 6.0, ((1, 4), (2, 16), (3, 8)), jnp.float32),
        "stiffness": draw_stiffness(jax.random.fold_in(key_of[9], 71), 0),
        "metric": jnp.clip(jnp.exp(math.log(1.4) - 0.6931472 * jax.random.uniform(key_of[3], (NZF, NY, NX), jnp.float32) ** levels(key_of[3], (NZF, NY, NX), ((0, 4), (1, 16), (2, 8)), -0.2, 0.2)), 0.7, 1.4),
        "density": jnp.clip(jnp.exp(math.log(2.0) - 0.6931472 * jax.random.uniform(key_of[4], (NZF, NY, NX), jnp.float32) ** levels(key_of[4], (NZF, NY, NX), ((0, 4), (1, 16), (2, 8)), -0.2, 0.2)), 1.0, 2.0),
        "coarse_now": bell_draw(key_of[5], (3, NZC, NY // 2, NX // 2), 1.0, 6.0, ((1, 4), (2, 16), (3, 8)), jnp.float32),
        "coarse_prev": bell_draw(key_of[6], (3, NZC, NY // 2, NX // 2), 1.0, 6.0, ((1, 4), (2, 16), (3, 8)), jnp.float32),
        "coarse_stiffness": draw_coarse_stiffness(jax.random.fold_in(key_of[9], 71), 0),
        "coarse_density": jnp.clip(jnp.exp(math.log(3.0) - 0.6931472 * jax.random.uniform(key_of[8], (NZC, NY // 2, NX // 2), jnp.float32) ** levels(key_of[8], (NZC, NY // 2, NX // 2), ((0, 4), (1, 16), (2, 8)), -0.2, 0.2)), 1.5, 3.0),
    }


TIME_STEP = 0.2


def along_x(volume, inverse_step):
    return (volume[..., 1:-1, 1:-1, 2:] - volume[..., 1:-1, 1:-1, :-2]) * inverse_step


def along_y(volume, inverse_step):
    return (volume[..., 1:-1, 2:, 1:-1] - volume[..., 1:-1, :-2, 1:-1]) * inverse_step


def along_z(volume, inverse_step, stretch):
    return (volume[..., 2:, 1:-1, 1:-1] - volume[..., :-2, 1:-1, 1:-1]) * inverse_step * stretch


def stresses(padded, stiffness, stretch, inverse_step):
    disp_x, disp_y, disp_z = padded[0], padded[1], padded[2]
    normal_x = along_x(disp_x, inverse_step)
    normal_y = along_y(disp_y, inverse_step)
    normal_z = along_z(disp_z, inverse_step, stretch)
    stress_xx = stiffness[0] * normal_x + stiffness[6] * normal_y + stiffness[7] * normal_z
    stress_yy = stiffness[6] * normal_x + stiffness[1] * normal_y + stiffness[8] * normal_z
    stress_zz = stiffness[7] * normal_x + stiffness[8] * normal_y + stiffness[2] * normal_z
    stress_yz = stiffness[3] * (along_z(disp_y, inverse_step, stretch) + along_y(disp_z, inverse_step))
    stress_xz = stiffness[4] * (along_z(disp_x, inverse_step, stretch) + along_x(disp_z, inverse_step))
    stress_xy = stiffness[5] * (along_y(disp_x, inverse_step) + along_x(disp_y, inverse_step))
    return jnp.stack([stress_xx, stress_yy, stress_zz, stress_yz, stress_xz, stress_xy])


def divergence(stress, stretch, inverse_step):
    total_x = along_x(stress[0], inverse_step) + along_y(stress[5], inverse_step) + along_z(stress[4], inverse_step, stretch)
    total_y = along_x(stress[5], inverse_step) + along_y(stress[1], inverse_step) + along_z(stress[3], inverse_step, stretch)
    total_z = along_x(stress[4], inverse_step) + along_y(stress[3], inverse_step) + along_z(stress[2], inverse_step, stretch)
    return jnp.stack([total_x, total_y, total_z])


def prolong_axis(padded, axis):
    length = padded.shape[axis] - 2
    centre = lax.slice_in_dim(padded, 1, length + 1, axis=axis)
    before = lax.slice_in_dim(padded, 0, length, axis=axis)
    behind = lax.slice_in_dim(padded, 2, length + 2, axis=axis)
    even_cells = 0.75 * centre + 0.25 * before
    odd_cells = 0.75 * centre + 0.25 * behind
    new_shape = list(centre.shape)
    new_shape[axis] = 2 * length
    return jnp.stack([even_cells, odd_cells], axis + 1).reshape(new_shape)


def prolong(padded):
    return prolong_axis(prolong_axis(padded, 1), 2)


def restrict(surface):
    row_pairs = surface.reshape(surface.shape[0], surface.shape[1] // 2, 2, surface.shape[2])
    summed = row_pairs[:, :, 0] + row_pairs[:, :, 1]
    col_pairs = summed.reshape(summed.shape[0], summed.shape[1], summed.shape[2] // 2, 2)
    return (col_pairs[..., 0] + col_pairs[..., 1]) * 0.25


def advance(now, prev, stiffness, stretch, density, inverse_step):
    padded = jnp.pad(now, ((0, 0), (2, 2), (2, 2), (2, 2)))
    coef_wide = jnp.pad(stiffness, ((0, 0), (1, 1), (1, 1), (1, 1)))
    stretch_wide = jnp.pad(stretch, 1)
    inside = jnp.pad(jnp.ones(now.shape[1:], now.dtype), 1)
    stress = stresses(padded, coef_wide, stretch_wide, inverse_step) * inside
    internal = divergence(stress, stretch, inverse_step)
    return (2.0 * now - prev) + (TIME_STEP * TIME_STEP) * internal / density


def reference(fine_now, fine_prev, stiffness, metric, density, coarse_now, coarse_prev, coarse_stiffness, coarse_density):
    layers = fine_now.shape[1]
    layer_index = jnp.arange(layers)
    stretch = jnp.where((layer_index < layers // 2)[:, None, None], metric, 1.0)
    fine_step = advance(fine_now, fine_prev, stiffness, stretch, density, 0.5)
    coarse_step = advance(coarse_now, coarse_prev, coarse_stiffness, jnp.ones_like(coarse_density), coarse_density, 0.25)
    fine_start = fine_step[:, -1]
    above = fine_step[:, -2]
    fine_coef = jnp.stack([stiffness[4, -1], stiffness[3, -1], stiffness[2, -1]])
    coarse_start = coarse_step[:, 0]
    below = coarse_step[:, 1]
    coarse_coef = jnp.stack([coarse_stiffness[4, 0], coarse_stiffness[3, 0], coarse_stiffness[2, 0]])
    fine_iter = fine_start
    coarse_iter = coarse_start
    for repeat in range(ITERS):
        traction = coarse_coef * (below - coarse_iter) * 0.25
        widened = jnp.pad(traction, ((0, 0), (1, 1), (1, 1)), mode="edge")
        fine_later = above + prolong(widened) / fine_coef
        coarse_iter = 0.5 * (coarse_start + restrict(fine_iter))
        fine_iter = fine_later
    fine_next = fine_step.at[:, -1].set(fine_iter)
    coarse_next = coarse_step.at[:, 0].set(coarse_iter)
    return fine_next, coarse_next
```

```python
import functools

import jax
import jax.numpy as jnp
from jax import lax
from jax.experimental import pallas as pl
from jax.experimental.pallas import tpu as pltpu
from jax.sharding import PartitionSpec as P

TIME_STEP = 0.2
ITERS = 3
F32 = jnp.float32
XX, XY, YY, XZ, YZ, ZZ = range(6)
FACE_X = (XX, XY, XZ)
FACE_Y = (XY, YY, YZ)
CH = (4, 3, 2)
PAD = 8
LANES = 128


def lanes_of(rows):
    return lax.broadcasted_iota(jnp.int32, (rows, LANES), 1)


def pack_x(ref, comps, z_count, y_count, width):
    lane = lanes_of(y_count)
    packed = jnp.zeros((y_count, LANES), F32)
    k = 0
    for c in comps:
        for z in range(z_count):
            rows = pl.ds(PAD, y_count)
            tile = ref[c, z + 1, rows, 0:LANES]
            if width > LANES:
                last = ref[c, z + 1, rows, width - LANES : width]
                tile = jnp.where(lane >= LANES // 2, last, tile)
            packed = jnp.where(lane // 2 == k, pltpu.roll(tile, 2 * k + 1, 1), packed)
            k += 1
    return packed


def unpack_x(ref, comps, z_count, y_count, width, from_left, from_right):
    lane = lanes_of(y_count)
    both = jnp.where(lane % 2 == 0, from_left, from_right)
    k = 0
    for c in comps:
        for z in range(z_count):
            ref[c, z + 1, pl.ds(PAD, y_count), width : width + LANES] = pltpu.roll(
                both, LANES - 1 - 2 * k, 1
            )
            k += 1


def diff_x(ref, c, z0, zn, y_count, width, scale):
    v = ref[c, z0 : z0 + zn, PAD : PAD + y_count, :]
    span = width + LANES
    return (pltpu.roll(v, span - 1, 2) - pltpu.roll(v, 1, 2))[:, :, :width] * scale


def diff_y(ref, c, z0, zn, y_count, width, scale):
    after = ref[c, z0 : z0 + zn, PAD + 1 : PAD + 1 + y_count, 0:width]
    before = ref[c, z0 : z0 + zn, PAD - 1 : PAD - 1 + y_count, 0:width]
    return (after - before) * scale


def diff_z(ref, c, z0, zn, y_count, width, scale):
    after = ref[c, z0 + 1 : z0 + 1 + zn, PAD : PAD + y_count, 0:width]
    before = ref[c, z0 - 1 : z0 - 1 + zn, PAD : PAD + y_count, 0:width]
    return (after - before) * scale


def stress_block(u, stiff, s, z, zn, y_count, width, inv, stretch):
    args = (z + 1, zn, y_count, width, inv)
    own = (slice(z + 1, z + 1 + zn), slice(PAD, PAD + y_count), slice(0, width))
    c = [stiff[i, z : z + zn] for i in range(9)]
    nx = diff_x(u, 0, *args)
    ny = diff_y(u, 1, *args)
    nz = diff_z(u, 2, *args) * stretch
    s[(XX,) + own] = c[0] * nx + c[6] * ny + c[7] * nz
    s[(YY,) + own] = c[6] * nx + c[1] * ny + c[8] * nz
    s[(ZZ,) + own] = c[7] * nx + c[8] * ny + c[2] * nz
    s[(YZ,) + own] = c[3] * (diff_z(u, 1, *args) * stretch + diff_y(u, 2, *args))
    s[(XZ,) + own] = c[4] * (diff_z(u, 0, *args) * stretch + diff_x(u, 2, *args))
    s[(XY,) + own] = c[5] * (diff_y(u, 0, *args) + diff_x(u, 1, *args))


def step_block(u, s, prev, dens, out, z, zn, y_count, width, inv, stretch):
    args = (z + 1, zn, y_count, width, inv)
    gain = (TIME_STEP * TIME_STEP) / dens[z : z + zn]
    for c, (sx, sy, sz) in enumerate(((XX, XY, XZ), (XY, YY, YZ), (XZ, YZ, ZZ))):
        total = diff_x(s, sx, *args) + diff_y(s, sy, *args) + diff_z(s, sz, *args) * stretch
        now = u[c, z + 1 : z + 1 + zn, PAD : PAD + y_count, 0:width]
        out[c, z : z + zn] = (2.0 * now - prev[c, z : z + zn]) + gain * total


def pick(x, index):
    return jnp.take_along_axis(x, index, axis=1, mode="promise_in_bounds")


def kernel(
    counts,
    fn, fp, st, me, de, cn, cp, cst, cde,
    fo_hbm, co_hbm,
    u, uc, s, sc, fprev, stiff, metric, dens, cprev, cstiff, cdens, fout, cout,
    xs, xr, yfs, yfr, ycs, ycr,
    tiles, own, own_opp, ikf_opp, ys3, yr3, yo3, xs3, xr3, xo3, ext,
    load_sem, out_sem, send_sem, recv_sem,
):
    n_z, n_y, n_x = counts
    zf, yf, xf = me.shape
    zc, yc, xc = cde.shape
    gz, gy, gx = lax.axis_index("gz"), lax.axis_index("gy"), lax.axis_index("gx")
    opp = n_z - 1 - gz
    is_c, is_f = gz == 0, gz == n_z - 1
    active = jnp.logical_or(is_c, is_f)
    has_y = {-1: gy > 0, 0: gy >= 0, 1: gy < n_y - 1}
    has_x = {-1: gx > 0, 0: gx >= 0, 1: gx < n_x - 1}
    has = (gz > 0, gz < n_z - 1, has_y[-1], has_y[1], has_x[-1], has_x[1])
    near = (
        (gz - 1, gy, gx), (gz + 1, gy, gx),
        (gz, gy - 1, gx), (gz, gy + 1, gx),
        (gz, gy, gx - 1), (gz, gy, gx + 1),
    )
    own_f = (slice(1, zf + 1), slice(PAD, PAD + yf), slice(0, xf))
    own_c = (slice(1, zc + 1), slice(PAD, PAD + yc), slice(0, xc))

    loads = [
        pltpu.make_async_copy(src, dst, load_sem.at[i])
        for i, (src, dst) in enumerate((
            (fn, u.at[(slice(None),) + own_f]),
            (cn, uc.at[(slice(None),) + own_c]),
            (st, stiff), (cst, cstiff), (me, metric),
            (fp, fprev), (cp, cprev), (de, dens), (cde, cdens),
        ))
    ]
    for load in loads:
        load.start()

    barrier = pltpu.get_barrier_semaphore()
    expected = jnp.int32(0)

    def greet(there, device):
        @pl.when(there)
        def _():
            pl.semaphore_signal(barrier, 1, device_id=device, device_id_type=pl.DeviceIdType.MESH)

        return there.astype(jnp.int32)

    for d in range(6):
        expected += greet(has[d], near[d])
    diagonals = [(a, b) for a in (-1, 1) for b in (-1, 1)]
    for a, b in diagonals:
        there = jnp.logical_and(active, jnp.logical_and(has_y[a], has_x[b]))
        expected += greet(there, (gz, gy + a, gx + b))
    expected += greet(active, (opp, gy, gx))

    for d in range(6):
        @pl.when(jnp.logical_not(has[d]))
        def _(d=d):
            side = d % 2
            if d < 2:
                plane_f, plane_c = (0, 0) if side == 0 else (zf + 1, zc + 1)
                for ref, plane, (_, rows, cols) in (
                    (u, plane_f, own_f), (uc, plane_c, own_c), (s, plane_f, own_f), (sc, plane_c, own_c),
                ):
                    part = ref.at[:, plane, rows, cols]
                    part[...] = jnp.zeros(part.shape, F32)
            elif d < 4:
                for r in range(2):
                    for ref in (yfr, ycr):
                        ref[r, side] = jnp.zeros(ref.shape[2:], F32)
            else:
                for r in range(2):
                    xr[r, side] = jnp.zeros(xr.shape[2:], F32)

    def rdma(src, dst, slot, device):
        return pltpu.make_async_remote_copy(
            src_ref=src, dst_ref=dst, send_sem=send_sem.at[slot], recv_sem=recv_sem.at[slot],
            device_id=device, device_id_type=pl.DeviceIdType.MESH,
        )

    def round_copies(r, d):
        side = d % 2
        arrival = 1 - side
        slot = (r * 6 + d) * 2
        if d < 2:
            fine, coarse = ((u, uc), (s, sc))[r]
            comps = (slice(0, 3), slice(3, 6))[r]
            made = []
            for g, (ref, z_count, (_, rows, cols)) in enumerate(((fine, zf, own_f), (coarse, zc, own_c))):
                sent, landed = (1, z_count + 1) if side == 0 else (z_count, 0)
                made.append(rdma(ref.at[comps, sent, rows, cols], ref.at[comps, landed, rows, cols], slot + g, near[d]))
            return made
        if d < 4:
            return [
                rdma(yfs.at[r, side], yfr.at[r, arrival], slot, near[d]),
                rdma(ycs.at[r, side], ycr.at[r, arrival], slot + 1, near[d]),
            ]
        return [rdma(xs.at[r], xr.at[r, arrival], slot, near[d])]

    def start_round(r):
        for d in (2, 3, 4, 5, 0, 1):
            @pl.when(has[d])
            def _(d=d):
                for copy in round_copies(r, d):
                    copy.start()

    def end_round(r, directions):
        for d in directions:
            @pl.when(has[d ^ 1])
            def _(d=d):
                for copy in round_copies(r, d):
                    copy.wait_recv()

    def pack(r, fine, coarse, face_x, face_y):
        for i, c in enumerate(face_y):
            yfs[r, 0, i] = fine[c, 1 : zf + 1, PAD : PAD + 1, 0:xf]
            yfs[r, 1, i] = fine[c, 1 : zf + 1, PAD + yf - 1 : PAD + yf, 0:xf]
            ycs[r, 0, i] = coarse[c, 1 : zc + 1, PAD : PAD + 1, 0:xc]
            ycs[r, 1, i] = coarse[c, 1 : zc + 1, PAD + yc - 1 : PAD + yc, 0:xc]
        xs[r, 0:yf] = pack_x(fine, face_x, zf, yf, xf)
        xs[r, yf : yf + yc] = pack_x(coarse, face_x, zc, yc, xc)

    def unpack(r, fine, coarse, face_x, face_y):
        for i, c in enumerate(face_y):
            fine[c, 1 : zf + 1, PAD - 1 : PAD, 0:xf] = yfr[r, 0, i]
            fine[c, 1 : zf + 1, PAD + yf : PAD + yf + 1, 0:xf] = yfr[r, 1, i]
            coarse[c, 1 : zc + 1, PAD - 1 : PAD, 0:xc] = ycr[r, 0, i]
            coarse[c, 1 : zc + 1, PAD + yc : PAD + yc + 1, 0:xc] = ycr[r, 1, i]
        unpack_x(fine, face_x, zf, yf, xf, xr[r, 0, 0:yf], xr[r, 1, 0:yf])
        unpack_x(coarse, face_x, zc, yc, xc, xr[r, 0, yf : yf + yc], xr[r, 1, yf : yf + yc])

    loads[0].wait()
    loads[1].wait()
    pack(0, u, uc, (0, 1, 2), (0, 1, 2))
    pl.semaphore_wait(barrier, expected)
    start_round(0)
    for load in loads[2:]:
        load.wait()

    lane = lanes_of(yc)
    even = (2 * lane) % LANES

    def squeeze(left, right, odd):
        return jnp.where(lane < LANES // 2, pick(left, even + odd), pick(right, even + odd))

    ikf_copy = rdma(own.at[6:18], ikf_opp, 24, (opp, gy, gx))

    @pl.when(is_f)
    def _():
        for c in range(3):
            inverse = 1.0 / stiff[CH[c], zf - 1]
            for t in range(2):
                tiles[t] = inverse[:, t * LANES : (t + 1) * LANES]
            for py in range(2):
                rows = pl.ds(py, yc, stride=2)
                left, right = tiles[0, rows, :], tiles[1, rows, :]
                for px in range(2):
                    own[6 + c * 4 + py * 2 + px] = squeeze(left, right, px)
        ikf_copy.start()

    def stretch_of(z):
        return jnp.where(gz * zf + z < n_z * zf // 2, metric[z : z + 1], 1.0)

    zb = min(4, zc)
    fine_order = tuple(range(zf - 1, -1, -1))
    coarse_order = tuple(range(0, zc, zb))

    end_round(0, (0, 1, 4, 5, 2, 3))
    unpack(0, u, uc, (0, 1, 2), (0, 1, 2))
    for z in fine_order:
        stress_block(u, stiff, s, z, 1, yf, xf, 0.5, stretch_of(z))
    for z in coarse_order:
        stress_block(uc, cstiff, sc, z, zb, yc, xc, 0.25, 1.0)
    pack(1, s, sc, FACE_X, FACE_Y)
    start_round(1)
    end_round(1, (0, 1, 4, 5, 2, 3))
    unpack(1, s, sc, FACE_X, FACE_Y)

    def fine_step(z):
        step_block(u, s, fprev, dens, fout, z, 1, yf, xf, 0.5, stretch_of(z))

    def coarse_step(z):
        step_block(uc, sc, cprev, cdens, cout, z, zb, yc, xc, 0.25, 1.0)

    fine_step(zf - 1)
    fine_step(zf - 2)
    coarse_step(0)

    @pl.when(is_c)
    def _():
        for c in range(3):
            start, below = cout[c, 0], cout[c, 1]
            k = cstiff[CH[c], 0] * 0.25
            own[c] = k * (below - start)
            own[3 + c] = below - 0.5 * start
            own[6 + c] = k

    @pl.when(is_f)
    def _():
        for c in range(3):
            for i, z in enumerate((zf - 2, zf - 1)):
                plane = fout[c, z]
                sums = []
                for t in range(2):
                    tiles[t] = plane[:, t * LANES : (t + 1) * LANES]
                    pair = tiles[t, pl.ds(0, yc, stride=2), :] + tiles[t, pl.ds(1, yc, stride=2), :]
                    sums.append(pair + pltpu.roll(pair, LANES - 1, 1))
                own[3 * i + c] = squeeze(sums[0], sums[1], 0) * 0.25

    fields = 18
    lane4 = lane // 4
    own_copy = rdma(own.at[0:9], own_opp, 25, (opp, gy, gx))
    strips = []
    for i, a in enumerate((-1, 1)):
        strips.append((
            jnp.logical_and(active, has_y[a]), jnp.logical_and(active, has_y[-a]),
            rdma(ys3.at[i], yr3.at[1 - i], 26 + i, (gz, gy + a, gx)),
        ))
    for i, b in enumerate((-1, 1)):
        for a in (-1, 0, 1):
            strips.append((
                jnp.logical_and(active, jnp.logical_and(has_y[a], has_x[b])),
                jnp.logical_and(active, jnp.logical_and(has_y[-a], has_x[-b])),
                rdma(xs3, xr3.at[1 - i, pl.ds((1 - a) * 8, 8)], 28 + i * 3 + (a + 1), (gz, gy + a, gx + b)),
            ))

    @pl.when(active)
    def _():
        own_copy.start()
        ys3[0] = own[:, 0:2, :]
        ys3[1] = own[:, yc - 2 : yc, :]
        packed = jnp.zeros((yc, LANES), F32)
        for k in range(fields):
            packed = jnp.where(lane4 == k, pltpu.roll(own[k], 4 * k + 2, 1), packed)
        xs3[...] = packed

    for there, _, copy in strips:
        @pl.when(there)
        def _(copy=copy):
            copy.start()

    for z in fine_order[2:]:
        fine_step(z)
    for z in coarse_order[1:]:
        coarse_step(z)

    early = [
        pltpu.make_async_copy(fout.at[:, 0 : zf - 1], fo_hbm.at[:, 0 : zf - 1], out_sem.at[0]),
        pltpu.make_async_copy(cout.at[:, 1:zc], co_hbm.at[:, 1:zc], out_sem.at[1]),
    ]
    late = [
        pltpu.make_async_copy(fout.at[:, zf - 1], fo_hbm.at[:, zf - 1], out_sem.at[2]),
        pltpu.make_async_copy(cout.at[:, 0], co_hbm.at[:, 0], out_sem.at[3]),
    ]
    for copy in early:
        copy.start()

    for _, comes, copy in strips:
        @pl.when(comes)
        def _(copy=copy):
            copy.wait_recv()

    forward = [
        rdma(yr3.at[:, 0:9], yo3, 34, (opp, gy, gx)),
        rdma(xr3, xo3, 35, (opp, gy, gx)),
    ]
    lane24 = lax.broadcasted_iota(jnp.int32, (24, LANES), 1)
    wide_row = lax.broadcasted_iota(jnp.int32, (24, 2 * LANES), 0)
    wide_lane = lax.broadcasted_iota(jnp.int32, (24, 2 * LANES), 1)

    def extend(k, field, centre, rims, sides):
        ext[k, 8:16, 0:LANES] = centre
        ext[k, 6:8, 0:LANES] = rims[0, field]
        ext[k, 16:18, 0:LANES] = rims[1, field]
        ext[k, :, LANES : 2 * LANES] = pltpu.roll(sides, LANES - (4 * field + 2), 1)

    def clamp(t):
        t = jnp.where(jnp.logical_and(wide_row == 7, gy == 0), pltpu.roll(t, 23, 0), t)
        t = jnp.where(jnp.logical_and(wide_row == 16, gy == n_y - 1), pltpu.roll(t, 1, 0), t)
        t = jnp.where(jnp.logical_and(wide_lane == 2 * LANES - 1, gx == 0), pltpu.roll(t, 2 * LANES - 1, 1), t)
        return jnp.where(jnp.logical_and(wide_lane == LANES, gx == n_x - 1), pltpu.roll(t, 1, 1), t)

    def along_y(t):
        return (0.75 * t + 0.25 * pltpu.roll(t, 1, 0), 0.75 * t + 0.25 * pltpu.roll(t, 23, 0))

    def along_x(t):
        return (0.75 * t + 0.25 * pltpu.roll(t, 1, 1), 0.75 * t + 0.25 * pltpu.roll(t, 2 * LANES - 1, 1))

    @pl.when(active)
    def _():
        for copy in forward:
            copy.start()
        own_copy.wait_recv()

    @pl.when(is_c)
    def _():
        ikf_copy.wait_recv()
        sides = jnp.where(lane24 % 4 < 2, xr3[0], xr3[1])
        for k in range(3, 9):
            extend(k, k, own[k], yr3, sides)

    @pl.when(is_f)
    def _():
        sides = jnp.where(lane24 % 4 < 2, xr3[0], xr3[1])
        for k in range(3):
            extend(9 + k, k, own[k], yr3, sides)
        for k in range(12):
            extend(12 + k, 6 + k, own[6 + k], yr3, sides)

    @pl.when(active)
    def _():
        for copy in forward:
            copy.wait_recv()

    @pl.when(is_c)
    def _():
        sides = jnp.where(lane24 % 4 < 2, xo3[0], xo3[1])
        for c in range(3):
            extend(9 + c, 3 + c, own_opp[3 + c], yo3, sides)
            t1 = clamp(ext[6 + c] * (ext[3 + c] - 0.5 * ext[9 + c]))
            total = jnp.zeros((yc, LANES), F32)
            for py, part in enumerate(along_y(t1)):
                for px, full in enumerate(along_x(part[8:16])):
                    total += full[:, 0:LANES] * ikf_opp[c * 4 + py * 2 + px]
            cout[c, 0] = 0.5 * (cout[c, 0] + own_opp[c] + 0.25 * total)

    @pl.when(is_f)
    def _():
        sides = jnp.where(lane24 % 4 < 2, xo3[0], xo3[1])
        half = lane // 2
        for c in range(3):
            for k in (c, 3 + c, 6 + c):
                extend(k, k, own_opp[k], yo3, sides)
            total = jnp.zeros((24, 2 * LANES), F32)
            for py, part in enumerate(along_y(clamp(ext[c]))):
                for px, full in enumerate(along_x(part)):
                    total += full * ext[12 + c * 4 + py * 2 + px]
            t2 = clamp(ext[6 + c] * (ext[3 + c] - 0.5 * (ext[9 + c] + 0.25 * total)))
            for py, part in enumerate(along_y(t2)):
                evens, odds = along_x(part[8:16])
                evens, odds = evens[:, 0:LANES], odds[:, 0:LANES]
                for t in range(2):
                    index = half + t * (LANES // 2)
                    tiles[t, pl.ds(py, yc, stride=2), :] = jnp.where(
                        lane % 2 == 0, pick(evens, index), pick(odds, index)
                    )
            for t in range(2):
                cols = slice(t * LANES, (t + 1) * LANES)
                fout[c, zf - 1, :, cols] = fout[c, zf - 2, :, cols] + tiles[t] / stiff[CH[c], zf - 1, :, cols]

    for copy in late:
        copy.start()
    for r in range(2):
        for d in range(6):
            @pl.when(has[d])
            def _(r=r, d=d):
                for copy in round_copies(r, d):
                    copy.wait_send()
    for there, _, copy in strips:
        @pl.when(there)
        def _(copy=copy):
            copy.wait_send()

    @pl.when(is_f)
    def _():
        ikf_copy.wait_send()

    @pl.when(active)
    def _():
        own_copy.wait_send()
        for copy in forward:
            copy.wait_send()

    for copy in early + late:
        copy.wait()


def per_device(counts, *args):
    fine, coarse = args[0].shape, args[5].shape
    _, zf, yf, xf = fine
    _, zc, yc, xc = coarse
    vmem = lambda *shape: pltpu.VMEM(shape, F32)
    anywhere = pl.BlockSpec(memory_space=pl.ANY)
    return pl.pallas_call(
        functools.partial(kernel, counts),
        out_shape=(jax.ShapeDtypeStruct(fine, F32), jax.ShapeDtypeStruct(coarse, F32)),
        in_specs=[anywhere] * 9,
        out_specs=(anywhere, anywhere),
        scratch_shapes=[
            vmem(3, zf + 2, yf + 2 * PAD, xf + LANES),
            vmem(3, zc + 2, yc + 2 * PAD, xc + LANES),
            vmem(6, zf + 2, yf + 2 * PAD, xf + LANES),
            vmem(6, zc + 2, yc + 2 * PAD, xc + LANES),
            vmem(3, zf, yf, xf), vmem(9, zf, yf, xf), vmem(zf, yf, xf), vmem(zf, yf, xf),
            vmem(3, zc, yc, xc), vmem(9, zc, yc, xc), vmem(zc, yc, xc),
            vmem(3, zf, yf, xf), vmem(3, zc, yc, xc),
            vmem(2, yf + yc, LANES), vmem(2, 2, yf + yc, LANES),
            vmem(2, 2, 3, zf, 1, xf), vmem(2, 2, 3, zf, 1, xf),
            vmem(2, 2, 3, zc, 1, xc), vmem(2, 2, 3, zc, 1, xc),
            vmem(2, yf, LANES), vmem(18, yc, LANES), vmem(9, yc, LANES), vmem(12, yc, LANES),
            vmem(2, 18, 2, LANES), vmem(2, 18, 2, LANES), vmem(2, 9, 2, LANES),
            vmem(yc, LANES), vmem(2, 24, LANES), vmem(2, 24, LANES),
            vmem(24, 24, 2 * LANES),
            pltpu.SemaphoreType.DMA((9,)),
            pltpu.SemaphoreType.DMA((4,)),
            pltpu.SemaphoreType.DMA((36,)),
            pltpu.SemaphoreType.DMA((36,)),
        ],
        compiler_params=pltpu.CompilerParams(
            collective_id=0, has_side_effects=True, vmem_limit_bytes=60 * 1024 * 1024
        ),
        name="elastic_step",
    )(*args)


def solution(mesh):
    counts = tuple(mesh.shape[name] for name in ("gz", "gy", "gx"))
    volume, field = P(None, "gz", "gy", "gx"), P("gz", "gy", "gx")
    return jax.shard_map(
        functools.partial(per_device, counts),
        mesh=mesh,
        in_specs=(volume, volume, volume, field, field, volume, volume, volume, field),
        out_specs=(volume, volume),
        check_vma=False,
    )
```

```python
import functools

import jax
import jax.numpy as jnp
from jax import lax
from jax.experimental import pallas as pl
from jax.experimental.pallas import tpu as pltpu
from jax.sharding import PartitionSpec as P

TIME_STEP = 0.2
ITERS = 3
F32 = jnp.float32
XX, XY, YY, XZ, YZ, ZZ = range(6)
FACE_X = (XX, XY, XZ)
FACE_Y = (XY, YY, YZ)
WIDE_Y = (1, 3, 5, 6, 8)
WIDE_X = (0, 4, 5, 6, 7)
CH = (4, 3, 2)
PAD = 8
LANES = 128


def lanes_of(rows):
    return lax.broadcasted_iota(jnp.int32, (rows, LANES), 1)


def pack_x(ref, comps, z_count, y_count, width):
    lane = lanes_of(y_count)
    packed = jnp.zeros((y_count, LANES), F32)
    k = 0
    for c in comps:
        for z in range(z_count):
            rows = pl.ds(PAD, y_count)
            tile = ref[c, z + 1, rows, 0:LANES]
            if width > LANES:
                last = ref[c, z + 1, rows, width - LANES : width]
                tile = jnp.where(lane >= LANES // 2, last, tile)
            packed = jnp.where(lane // 2 == k, pltpu.roll(tile, 2 * k + 1, 1), packed)
            k += 1
    return packed


def unpack_x(ref, comps, z_count, y_count, width, from_left, from_right):
    lane = lanes_of(y_count)
    both = jnp.where(lane % 2 == 0, from_left, from_right)
    k = 0
    for c in comps:
        for z in range(z_count):
            ref[c, z + 1, pl.ds(PAD, y_count), width : width + LANES] = pltpu.roll(
                both, LANES - 1 - 2 * k, 1
            )
            k += 1


def diff_x(ref, c, z0, zn, y_count, width, scale):
    v = ref[c, z0 : z0 + zn, PAD : PAD + y_count, :]
    span = width + LANES
    return (pltpu.roll(v, span - 1, 2) - pltpu.roll(v, 1, 2))[:, :, :width] * scale


def diff_y(ref, c, z0, zn, y_count, width, scale):
    after = ref[c, z0 : z0 + zn, PAD + 1 : PAD + 1 + y_count, 0:width]
    before = ref[c, z0 : z0 + zn, PAD - 1 : PAD - 1 + y_count, 0:width]
    return (after - before) * scale


def diff_z(ref, c, z0, zn, y_count, width, scale):
    after = ref[c, z0 + 1 : z0 + 1 + zn, PAD : PAD + y_count, 0:width]
    before = ref[c, z0 - 1 : z0 - 1 + zn, PAD : PAD + y_count, 0:width]
    return (after - before) * scale


def stress_block(u, stiff, s, z, zn, y_count, width, inv, stretch):
    args = (z + 1, zn, y_count, width, inv)
    own = (slice(z + 1, z + 1 + zn), slice(PAD, PAD + y_count), slice(0, width))
    c = [stiff[i, z : z + zn] for i in range(9)]
    nx = diff_x(u, 0, *args)
    ny = diff_y(u, 1, *args)
    nz = diff_z(u, 2, *args) * stretch
    s[(XX,) + own] = c[0] * nx + c[6] * ny + c[7] * nz
    s[(YY,) + own] = c[6] * nx + c[1] * ny + c[8] * nz
    s[(ZZ,) + own] = c[7] * nx + c[8] * ny + c[2] * nz
    s[(YZ,) + own] = c[3] * (diff_z(u, 1, *args) * stretch + diff_y(u, 2, *args))
    s[(XZ,) + own] = c[4] * (diff_z(u, 0, *args) * stretch + diff_x(u, 2, *args))
    s[(XY,) + own] = c[5] * (diff_y(u, 0, *args) + diff_x(u, 1, *args))


def step_block(u, s, prev, dens, out, z, zn, y_count, width, inv, stretch):
    args = (z + 1, zn, y_count, width, inv)
    gain = (TIME_STEP * TIME_STEP) / dens[z : z + zn]
    for c, (sx, sy, sz) in enumerate(((XX, XY, XZ), (XY, YY, YZ), (XZ, YZ, ZZ))):
        total = diff_x(s, sx, *args) + diff_y(s, sy, *args) + diff_z(s, sz, *args) * stretch
        now = u[c, z + 1 : z + 1 + zn, PAD : PAD + y_count, 0:width]
        out[c, z : z + zn] = (2.0 * now - prev[c, z : z + zn]) + gain * total


def stress_ext(u, stiff, s, layer, slab, y_count, width, inv):
    z, first, rows, span = layer + 1, PAD - 1, y_count + 2, width + LANES

    def at(c, dz, dr):
        return u[c, z + dz, first + dr : first + dr + rows, :]

    def dx(c):
        v = at(c, 0, 0)
        return (pltpu.roll(v, span - 1, 1) - pltpu.roll(v, 1, 1)) * inv

    def dy(c):
        return (at(c, 0, 1) - at(c, 0, -1)) * inv

    def dz(c):
        return (at(c, 1, 0) - at(c, -1, 0)) * inv

    c = [stiff[i, slab, first : first + rows, :] for i in range(9)]
    nx, ny, nz = dx(0), dy(1), dz(2)
    values = {
        XX: c[0] * nx + c[6] * ny + c[7] * nz,
        YY: c[6] * nx + c[1] * ny + c[8] * nz,
        ZZ: c[7] * nx + c[8] * ny + c[2] * nz,
        YZ: c[3] * (dz(1) + dy(2)),
        XZ: c[4] * (dz(0) + dx(2)),
        XY: c[5] * (dy(0) + dx(1)),
    }
    for component, value in values.items():
        s[component, z, first : first + rows, :] = value


def pick(x, index):
    return jnp.take_along_axis(x, index, axis=1, mode="promise_in_bounds")


class Grid:
    def __init__(self, **fields):
        self.__dict__.update(fields)
        self.own = (slice(1, self.z + 1), slice(PAD, PAD + self.y), slice(0, self.x))


def kernel(
    counts,
    fn, fp, st, me, de, cn, cp, cst, cde,
    fout, cout,
    u, uc, s, sc, fprev, stiff, metric, dens, cprev, cstiff, cdens,
    xs, xr, yfs, yfr, ycs, ycr,
    fwide, cwide, yef_s, yef_r, yec_s, yec_r, xef_s, xef_r, xec_s, xec_r,
    tiles, own, own_opp, ikf_opp, yi_s, yi_r, ys3, yr3, yo3, xs3, xr3, xo3, ext,
    load_sem, send_sem, recv_sem,
):
    n_z, n_y, n_x = counts
    zf, yf, xf = me.shape
    zc, yc, xc = cde.shape
    fine = Grid(
        z=zf, y=yf, x=xf, u=u, s=s, wide=fwide, source=st, stiff=stiff, third=zf - 3, prev=fprev, dens=dens, out=fout, inv=0.5,
        layers=(zf - 2, zf - 1), near=(zf - 3, zf - 2, zf - 1), ye_s=yef_s, ye_r=yef_r, xe_s=xef_s, xe_r=xef_r,
    )
    coarse = Grid(
        z=zc, y=yc, x=xc, u=uc, s=sc, wide=cwide, source=cst, stiff=cstiff, third=2, prev=cprev, dens=cdens, out=cout, inv=0.25,
        layers=(0, 1), near=(0, 1, 2), ye_s=yec_s, ye_r=yec_r, xe_s=xec_s, xe_r=xec_r,
    )
    gz, gy, gx = lax.axis_index("gz"), lax.axis_index("gy"), lax.axis_index("gx")
    opp = n_z - 1 - gz
    is_c, is_f = gz == 0, gz == n_z - 1
    active = jnp.logical_or(is_c, is_f)
    has_y = {-1: gy > 0, 0: gy >= 0, 1: gy < n_y - 1}
    has_x = {-1: gx > 0, 0: gx >= 0, 1: gx < n_x - 1}
    has = (gz > 0, gz < n_z - 1, has_y[-1], has_y[1], has_x[-1], has_x[1])
    near = (
        (gz - 1, gy, gx), (gz + 1, gy, gx),
        (gz, gy - 1, gx), (gz, gy + 1, gx),
        (gz, gy, gx - 1), (gz, gy, gx + 1),
    )

    barrier = pltpu.get_barrier_semaphore()
    expected = jnp.int32(0)

    def greet(there, device):
        @pl.when(there)
        def _():
            pl.semaphore_signal(barrier, 1, device_id=device, device_id_type=pl.DeviceIdType.MESH)

        return there.astype(jnp.int32)

    for d in (2, 3, 4, 5, 0, 1):
        expected += greet(has[d], near[d])
    for a in (-1, 1):
        for b in (-1, 1):
            there = jnp.logical_and(active, jnp.logical_and(has_y[a], has_x[b]))
            expected += greet(there, (gz, gy + a, gx + b))
    expected += greet(active, (opp, gy, gx))

    loads = [
        pltpu.make_async_copy(src, dst, load_sem.at[i])
        for i, (src, dst) in enumerate((
            (fn, u.at[(slice(None),) + fine.own]),
            (cn, uc.at[(slice(None),) + coarse.own]),
            (st, stiff), (cst, cstiff), (me, metric),
            (fp, fprev), (cp, cprev), (de, dens), (cde, cdens),
        ))
    ]

    def wide_load(g):
        return pltpu.make_async_copy(
            g.source.at[:, g.layers[0] : g.layers[1] + 1], g.wide.at[(slice(None), slice(None)) + g.own[1:]], load_sem.at[9]
        )

    sides = ((is_f, fine), (is_c, coarse))
    for load in loads[:2]:
        load.start()
    for there, g in sides:
        @pl.when(there)
        def _(g=g):
            wide_load(g).start()
    for load in loads[2:]:
        load.start()

    def clear(part):
        part[...] = jnp.zeros(part.shape, F32)

    for d in range(6):
        @pl.when(jnp.logical_not(has[d]))
        def _(d=d):
            side = d % 2
            if d < 2:
                for g in (fine, coarse):
                    plane = 0 if side == 0 else g.z + 1
                    clear(g.u.at[:, plane])
                    clear(g.s.at[3:6, plane, g.own[1], g.own[2]])
            elif d < 4:
                for r in range(2):
                    for ref in (yfr, ycr):
                        clear(ref.at[r, side])
                for g in (fine, coarse):
                    clear(g.ye_r.at[side])
                    for b in range(2):
                        rows = pl.ds(0 if side == 0 else PAD + g.y, PAD)
                        clear(g.xe_r.at[b, rows])
            else:
                for r in range(2):
                    clear(xr.at[r, side])
                for g in (fine, coarse):
                    clear(g.xe_r.at[side])

    def rdma(src, dst, slot, device):
        return pltpu.make_async_remote_copy(
            src_ref=src, dst_ref=dst, send_sem=send_sem.at[slot], recv_sem=recv_sem.at[slot],
            device_id=device, device_id_type=pl.DeviceIdType.MESH,
        )

    def round_copies(r, d):
        side = d % 2
        arrival = 1 - side
        slot = (r * 6 + d) * 2
        if d < 2:
            comps = (slice(0, 3), slice(3, 6))[r]
            made = []
            for i, g in enumerate((fine, coarse)):
                ref = (g.u, g.s)[r]
                sent, landed = (1, g.z + 1) if side == 0 else (g.z, 0)
                made.append(rdma(
                    ref.at[comps, sent, g.own[1], g.own[2]], ref.at[comps, landed, g.own[1], g.own[2]], slot + i, near[d]
                ))
            return made
        if d < 4:
            return [
                rdma(yfs.at[r, side], yfr.at[r, arrival], slot, near[d]),
                rdma(ycs.at[r, side], ycr.at[r, arrival], slot + 1, near[d]),
            ]
        return [rdma(xs.at[r], xr.at[r, arrival], slot, near[d])]

    def start_round(r, directions):
        for d in directions:
            @pl.when(has[d])
            def _(d=d):
                for copy in round_copies(r, d):
                    copy.start()

    def end_round(r, directions):
        for d in directions:
            @pl.when(has[d ^ 1])
            def _(d=d):
                for copy in round_copies(r, d):
                    copy.wait_recv()

    def pack_rows(r, refs, face_y):
        for g, ref, out in ((fine, refs[0], yfs), (coarse, refs[1], ycs)):
            for i, c in enumerate(face_y):
                out[r, 0, i] = ref[c, 1 : g.z + 1, PAD : PAD + 1, 0 : g.x]
                out[r, 1, i] = ref[c, 1 : g.z + 1, PAD + g.y - 1 : PAD + g.y, 0 : g.x]

    def pack_columns(r, refs, face_x):
        xs[r, 0:yf] = pack_x(refs[0], face_x, zf, yf, xf)
        xs[r, yf : yf + yc] = pack_x(refs[1], face_x, zc, yc, xc)

    def unpack_rows(r, g, ref, landed, face_y):
        for i, c in enumerate(face_y):
            ref[c, 1 : g.z + 1, PAD - 1 : PAD, 0 : g.x] = landed[r, 0, i]
            ref[c, 1 : g.z + 1, PAD + g.y : PAD + g.y + 1, 0 : g.x] = landed[r, 1, i]

    def unpack(r, refs, face_x, face_y):
        unpack_rows(r, fine, refs[0], yfr, face_y)
        unpack_rows(r, coarse, refs[1], ycr, face_y)
        unpack_x(refs[0], face_x, zf, yf, xf, xr[r, 0, 0:yf], xr[r, 1, 0:yf])
        unpack_x(refs[1], face_x, zc, yc, xc, xr[r, 0, yf : yf + yc], xr[r, 1, yf : yf + yc])

    def pack_wide(g):
        first = g.layers[0]
        for side, (edge, second) in enumerate(((PAD, PAD + 1), (PAD + g.y - 1, PAD + g.y - 2))):
            for c in range(3):
                g.ye_s[side, c] = g.u[c, first + 1 : first + 3, second : second + 1, 0 : g.x]
            for i, c in enumerate(WIDE_Y):
                g.ye_s[side, 3 + i] = g.wide[c, :, edge : edge + 1, 0 : g.x]
        lane = lanes_of(g.y)
        packed = jnp.zeros((g.y, LANES), F32)
        for k, (ref, index) in enumerate(wide_blocks(g)):
            tile = ref[index + (g.own[1], slice(0, LANES))]
            if g.x > LANES:
                last = ref[index + (g.own[1], slice(g.x - LANES, g.x))]
                tile = jnp.where(lane >= LANES // 2, last, tile)
            packed = jnp.where(lane // 4 == k, pltpu.roll(tile, 4 * k + 2, 1), packed)
        g.xe_s[...] = packed

    def wide_blocks(g):
        blocks = [(g.u, (c, z + 1)) for c in range(3) for z in g.near]
        return blocks + [(g.wide, (c, l)) for c in WIDE_X for l in range(2)]

    def wide_rows(g):
        return [
            (has_y[a], has_y[-a], rdma(g.ye_s.at[i], g.ye_r.at[1 - i], 26 + i, (gz, gy + a, gx)))
            for i, a in enumerate((-1, 1))
        ]

    def wide_columns(g):
        made = []
        for i, b in enumerate((-1, 1)):
            for a in (-1, 0, 1):
                src, dst = {
                    -1: (slice(0, PAD), slice(PAD + g.y, 2 * PAD + g.y)),
                    0: (slice(0, g.y), slice(PAD, PAD + g.y)),
                    1: (slice(g.y - PAD, g.y), slice(0, PAD)),
                }[a]
                made.append((
                    jnp.logical_and(has_y[a], has_x[b]), jnp.logical_and(has_y[-a], has_x[-b]),
                    rdma(g.xe_s.at[src], g.xe_r.at[1 - i, dst], 28 + i * 3 + (a + 1), (gz, gy + a, gx + b)),
                ))
        return made

    def unpack_wide(g):
        first = g.layers[0]
        unpack_rows(0, g, g.u, yfr if g is fine else ycr, (0, 1, 2))
        for side, (edge, second) in enumerate(((PAD - 1, PAD - 2), (PAD + g.y, PAD + g.y + 1))):
            for c in range(3):
                g.u[c, first + 1 : first + 3, second : second + 1, 0 : g.x] = g.ye_r[side, c]
            for i, c in enumerate(WIDE_Y):
                g.wide[c, :, edge : edge + 1, 0 : g.x] = g.ye_r[side, 3 + i]
        rows = g.y + 2 * PAD
        both = jnp.where(lanes_of(rows) % 4 < 2, g.xe_r[0], g.xe_r[1])
        for k, (ref, index) in enumerate(wide_blocks(g)):
            ref[index + (slice(0, rows), slice(g.x, g.x + LANES))] = pltpu.roll(both, LANES - (4 * k + 2), 1)

    def start_all(copies):
        for there, _, copy in copies:
            @pl.when(there)
            def _(copy=copy):
                copy.start()

    def receive_all(copies):
        for _, comes, copy in copies:
            @pl.when(comes)
            def _(copy=copy):
                copy.wait_recv()

    def sent_all(copies):
        for there, _, copy in copies:
            @pl.when(there)
            def _(copy=copy):
                copy.wait_send()

    with jax.named_scope("load_pack"):
        loads[0].wait()
        loads[1].wait()
        pack_rows(0, (u, uc), (0, 1, 2))
        for there, g in sides:
            @pl.when(there)
            def _(g=g):
                wide_load(g).wait()
                pack_wide(g)
        pack_columns(0, (u, uc), (0, 1, 2))
    with jax.named_scope("barrier"):
        pl.semaphore_wait(barrier, expected)
    with jax.named_scope("send_0"):
        start_round(0, (2, 3))
        for there, g in sides:
            @pl.when(there)
            def _(g=g):
                start_all(wide_rows(g))
                start_all(wide_columns(g))
        start_round(0, (4, 5, 0, 1))
        for load in loads[2:]:
            load.wait()

    lane = lanes_of(yc)
    even = (2 * lane) % LANES

    def squeeze(left, right, odd):
        return jnp.where(lane < LANES // 2, pick(left, even + odd), pick(right, even + odd))

    ikf_copy = rdma(own.at[6:18], ikf_opp, 24, (opp, gy, gx))
    ikf_rows = [
        (has_y[a], has_y[-a], rdma(yi_s.at[i], yi_r.at[1 - i], 34 + i, (gz, gy + a, gx))) for i, a in enumerate((-1, 1))
    ]

    @pl.when(is_f)
    def _():
        for c in range(3):
            inverse = 1.0 / stiff[CH[c], zf - 1]
            for t in range(2):
                tiles[t] = inverse[:, t * LANES : (t + 1) * LANES]
            for py in range(2):
                rows = pl.ds(py, yc, stride=2)
                left, right = tiles[0, rows, :], tiles[1, rows, :]
                for px in range(2):
                    own[6 + c * 4 + py * 2 + px] = squeeze(left, right, px)
        yi_s[0] = own[6:18, 0:2, :]
        yi_s[1] = own[6:18, yc - 2 : yc, :]
        ikf_copy.start()
        start_all(ikf_rows)

    with jax.named_scope("wait_wide"):
        for there, g in sides:
            @pl.when(there)
            def _(g=g):
                receive_all(wide_rows(g))
                receive_all(wide_columns(g))
                for d in (2, 3):
                    @pl.when(has[d ^ 1])
                    def _(d=d):
                        round_copies(0, d)[0 if g is fine else 1].wait_recv()

    for there, g in sides:
        @pl.when(there)
        def _(g=g):
            unpack_wide(g)
            stress_block(g.u, g.stiff, g.s, g.third, 1, g.y, g.x, g.inv, 1.0)
            for l, z in enumerate(g.layers):
                stress_ext(g.u, g.wide, g.s, z, l, g.y, g.x, g.inv)
            for z in g.layers:
                step_block(g.u, g.s, g.prev, g.dens, g.out, z, 1, g.y, g.x, g.inv, 1.0)

    @pl.when(is_c)
    def _():
        for c in range(3):
            start, below = cout[c, 0], cout[c, 1]
            k = cstiff[CH[c], 0] * 0.25
            own[c] = k * (below - start)
            own[3 + c] = below - 0.5 * start
            own[6 + c] = k

    @pl.when(is_f)
    def _():
        for c in range(3):
            for i, z in enumerate((zf - 2, zf - 1)):
                plane = fout[c, z]
                sums = []
                for t in range(2):
                    tiles[t] = plane[:, t * LANES : (t + 1) * LANES]
                    pair = tiles[t, pl.ds(0, yc, stride=2), :] + tiles[t, pl.ds(1, yc, stride=2), :]
                    sums.append(pair + pltpu.roll(pair, LANES - 1, 1))
                own[3 * i + c] = squeeze(sums[0], sums[1], 0) * 0.25

    fields = 18
    lane4 = lane // 4
    own_copy = rdma(own.at[0:9], own_opp, 25, (opp, gy, gx))
    strips = []
    for level, rows_to, tile_to, slot in ((opp, yo3, xo3, 36), (gz, yr3, xr3, 44)):
        for i, a in enumerate((-1, 1)):
            strips.append((
                jnp.logical_and(active, has_y[a]), jnp.logical_and(active, has_y[-a]),
                rdma(ys3.at[i], rows_to.at[1 - i], slot + i, (level, gy + a, gx)),
            ))
        for i, b in enumerate((-1, 1)):
            for a in (-1, 0, 1):
                strips.append((
                    jnp.logical_and(active, jnp.logical_and(has_y[a], has_x[b])),
                    jnp.logical_and(active, jnp.logical_and(has_y[-a], has_x[-b])),
                    rdma(xs3, tile_to.at[1 - i, pl.ds((1 - a) * 8, 8)], slot + 2 + i * 3 + (a + 1), (level, gy + a, gx + b)),
                ))
    opp_strips, level_strips = strips[:8], strips[8:]

    @pl.when(active)
    def _():
        ys3[0] = own[0:9, 0:2, :]
        ys3[1] = own[0:9, yc - 2 : yc, :]
        packed = jnp.zeros((yc, LANES), F32)
        for k in range(fields):
            packed = jnp.where(lane4 == k, pltpu.roll(own[k], 4 * k + 2, 1), packed)
        xs3[...] = packed
        own_copy.start()

    start_all(strips)

    def stretch_of(z):
        return jnp.where(gz * zf + z < n_z * zf // 2, metric[z : z + 1], 1.0)

    zb = min(4, zc)

    with jax.named_scope("wait_0"):
        @pl.when(jnp.logical_not(is_f))
        def _():
            for d in (2, 3):
                @pl.when(has[d ^ 1])
                def _(d=d):
                    round_copies(0, d)[0].wait_recv()

        @pl.when(jnp.logical_not(is_c))
        def _():
            for d in (2, 3):
                @pl.when(has[d ^ 1])
                def _(d=d):
                    round_copies(0, d)[1].wait_recv()

        end_round(0, (0, 1, 4, 5))
    with jax.named_scope("stress"):
        unpack(0, (u, uc), (0, 1, 2), (0, 1, 2))
        for z in range(zf):
            stress_block(u, stiff, s, z, 1, yf, xf, 0.5, stretch_of(z))
        for z in range(0, zc, zb):
            stress_block(uc, cstiff, sc, z, zb, yc, xc, 0.25, 1.0)
    with jax.named_scope("pack_1"):
        pack_rows(1, (s, sc), FACE_Y)
        start_round(1, (2, 3))
        pack_columns(1, (s, sc), FACE_X)
        start_round(1, (4, 5, 0, 1))
    with jax.named_scope("wait_1"):
        end_round(1, (0, 1, 4, 5, 2, 3))
    with jax.named_scope("step"):
        unpack(1, (s, sc), FACE_X, FACE_Y)
        for z in range(zf):
            step_block(u, s, fprev, dens, fout, z, 1, yf, xf, 0.5, stretch_of(z))
        for z in range(0, zc, zb):
            step_block(uc, sc, cprev, cdens, cout, z, zb, yc, xc, 0.25, 1.0)

    lane24 = lax.broadcasted_iota(jnp.int32, (24, LANES), 1)
    wide_row = lax.broadcasted_iota(jnp.int32, (24, 2 * LANES), 0)
    wide_lane = lax.broadcasted_iota(jnp.int32, (24, 2 * LANES), 1)

    def extend(k, field, centre, rims, row, edges):
        ext[k, 8:16, 0:LANES] = centre
        ext[k, 6:8, 0:LANES] = rims[0, row]
        ext[k, 16:18, 0:LANES] = rims[1, row]
        ext[k, :, LANES : 2 * LANES] = pltpu.roll(edges, LANES - (4 * field + 2), 1)

    def clamp(t):
        t = jnp.where(jnp.logical_and(wide_row == 7, gy == 0), pltpu.roll(t, 23, 0), t)
        t = jnp.where(jnp.logical_and(wide_row == 16, gy == n_y - 1), pltpu.roll(t, 1, 0), t)
        t = jnp.where(jnp.logical_and(wide_lane == 2 * LANES - 1, gx == 0), pltpu.roll(t, 2 * LANES - 1, 1), t)
        return jnp.where(jnp.logical_and(wide_lane == LANES, gx == n_x - 1), pltpu.roll(t, 1, 1), t)

    def along_y(t):
        return (0.75 * t + 0.25 * pltpu.roll(t, 1, 0), 0.75 * t + 0.25 * pltpu.roll(t, 23, 0))

    def along_x(t):
        return (0.75 * t + 0.25 * pltpu.roll(t, 1, 1), 0.75 * t + 0.25 * pltpu.roll(t, 2 * LANES - 1, 1))

    with jax.named_scope("wait_level"):
        receive_all(level_strips)

        @pl.when(is_f)
        def _():
            receive_all(ikf_rows)

    @pl.when(is_c)
    def _():
        edges = jnp.where(lane24 % 4 < 2, xr3[0], xr3[1])
        for k in range(3, 9):
            extend(k, k, own[k], yr3, k, edges)
        ikf_copy.wait_recv()

    @pl.when(is_f)
    def _():
        edges = jnp.where(lane24 % 4 < 2, xr3[0], xr3[1])
        for k in range(3):
            extend(9 + k, k, own[k], yr3, k, edges)
        for k in range(12):
            extend(12 + k, 6 + k, own[6 + k], yi_r, k, edges)

    with jax.named_scope("wait_opp"):
        @pl.when(active)
        def _():
            own_copy.wait_recv()

        receive_all(opp_strips)

    @pl.when(is_c)
    def _():
        edges = jnp.where(lane24 % 4 < 2, xo3[0], xo3[1])
        for c in range(3):
            extend(9 + c, 3 + c, own_opp[3 + c], yo3, 3 + c, edges)
            t1 = clamp(ext[6 + c] * (ext[3 + c] - 0.5 * ext[9 + c]))
            total = jnp.zeros((yc, LANES), F32)
            for py, part in enumerate(along_y(t1)):
                for px, full in enumerate(along_x(part[8:16])):
                    total += full[:, 0:LANES] * ikf_opp[c * 4 + py * 2 + px]
            cout[c, 0] = 0.5 * (cout[c, 0] + own_opp[c] + 0.25 * total)

    @pl.when(is_f)
    def _():
        edges = jnp.where(lane24 % 4 < 2, xo3[0], xo3[1])
        half = lane // 2
        for c in range(3):
            for k in (c, 3 + c, 6 + c):
                extend(k, k, own_opp[k], yo3, k, edges)
            total = jnp.zeros((24, 2 * LANES), F32)
            for py, part in enumerate(along_y(clamp(ext[c]))):
                for px, full in enumerate(along_x(part)):
                    total += full * ext[12 + c * 4 + py * 2 + px]
            t2 = clamp(ext[6 + c] * (ext[3 + c] - 0.5 * (ext[9 + c] + 0.25 * total)))
            for py, part in enumerate(along_y(t2)):
                evens, odds = along_x(part[8:16])
                evens, odds = evens[:, 0:LANES], odds[:, 0:LANES]
                for t in range(2):
                    index = half + t * (LANES // 2)
                    tiles[t, pl.ds(py, yc, stride=2), :] = jnp.where(
                        lane % 2 == 0, pick(evens, index), pick(odds, index)
                    )
            for t in range(2):
                cols = slice(t * LANES, (t + 1) * LANES)
                fout[c, zf - 1, :, cols] = fout[c, zf - 2, :, cols] + tiles[t] / stiff[CH[c], zf - 1, :, cols]

    with jax.named_scope("drain"):
        for r in range(2):
            for d in range(6):
                @pl.when(has[d])
                def _(r=r, d=d):
                    for copy in round_copies(r, d):
                        copy.wait_send()
        sent_all(strips)
        for there, g in sides:
            @pl.when(there)
            def _(g=g):
                sent_all(wide_rows(g))
                sent_all(wide_columns(g))

        @pl.when(is_f)
        def _():
            ikf_copy.wait_send()
            sent_all(ikf_rows)

        @pl.when(active)
        def _():
            own_copy.wait_send()


def per_device(counts, *args):
    fine, coarse = args[0].shape, args[5].shape
    _, zf, yf, xf = fine
    _, zc, yc, xc = coarse
    vmem = lambda *shape: pltpu.VMEM(shape, F32)
    anywhere = pl.BlockSpec(memory_space=pl.ANY)
    in_vmem = pl.BlockSpec(memory_space=pltpu.VMEM)
    return pl.pallas_call(
        functools.partial(kernel, counts),
        out_shape=(pltpu.VMEM(fine, F32), pltpu.VMEM(coarse, F32)),
        in_specs=[anywhere] * 9,
        out_specs=(in_vmem, in_vmem),
        scratch_shapes=[
            vmem(3, zf + 2, yf + 2 * PAD, xf + LANES),
            vmem(3, zc + 2, yc + 2 * PAD, xc + LANES),
            vmem(6, zf + 2, yf + 2 * PAD, xf + LANES),
            vmem(6, zc + 2, yc + 2 * PAD, xc + LANES),
            vmem(3, zf, yf, xf), vmem(9, zf, yf, xf), vmem(zf, yf, xf), vmem(zf, yf, xf),
            vmem(3, zc, yc, xc), vmem(9, zc, yc, xc), vmem(zc, yc, xc),
            vmem(2, yf + yc, LANES), vmem(2, 2, yf + yc, LANES),
            vmem(2, 2, 3, zf, 1, xf), vmem(2, 2, 3, zf, 1, xf),
            vmem(2, 2, 3, zc, 1, xc), vmem(2, 2, 3, zc, 1, xc),
            vmem(9, 2, yf + 2 * PAD, xf + LANES), vmem(9, 2, yc + 2 * PAD, xc + LANES),
            vmem(2, 8, 2, 1, xf), vmem(2, 8, 2, 1, xf), vmem(2, 8, 2, 1, xc), vmem(2, 8, 2, 1, xc),
            vmem(yf, LANES), vmem(2, yf + 2 * PAD, LANES), vmem(yc, LANES), vmem(2, yc + 2 * PAD, LANES),
            vmem(2, yf, LANES), vmem(18, yc, LANES), vmem(9, yc, LANES), vmem(12, yc, LANES),
            vmem(2, 12, 2, LANES), vmem(2, 12, 2, LANES),
            vmem(2, 9, 2, LANES), vmem(2, 9, 2, LANES), vmem(2, 9, 2, LANES),
            vmem(yc, LANES), vmem(2, 24, LANES), vmem(2, 24, LANES),
            vmem(24, 24, 2 * LANES),
            pltpu.SemaphoreType.DMA((10,)),
            pltpu.SemaphoreType.DMA((52,)),
            pltpu.SemaphoreType.DMA((52,)),
        ],
        compiler_params=pltpu.CompilerParams(
            collective_id=0, has_side_effects=True, vmem_limit_bytes=56 * 1024 * 1024
        ),
        name="elastic_step",
    )(*args)


def solution(mesh):
    counts = tuple(mesh.shape[name] for name in ("gz", "gy", "gx"))
    volume, field = P(None, "gz", "gy", "gx"), P("gz", "gy", "gx")
    return jax.shard_map(
        functools.partial(per_device, counts),
        mesh=mesh,
        in_specs=(volume, volume, volume, field, field, volume, volume, volume, field),
        out_specs=(volume, volume),
        check_vma=False,
    )
```

```python
import functools

import jax
import jax.numpy as jnp
from jax import lax
from jax.experimental import pallas as pl
from jax.experimental.pallas import tpu as pltpu
from jax.sharding import PartitionSpec as P

TIME_STEP = 0.2
ITERS = 3
F32 = jnp.float32
XX, XY, YY, XZ, YZ, ZZ = range(6)
FACE_X = (XX, XY, XZ)
FACE_Y = (XY, YY, YZ)
WIDE_Y = (1, 3, 5, 6, 8)
WIDE_X = (0, 4, 5, 6, 7)
CH = (4, 3, 2)
PAD = 8
LANES = 128


def lanes_of(rows):
    return lax.broadcasted_iota(jnp.int32, (rows, LANES), 1)


def pack_x(ref, comps, z_count, y_count, width):
    lane = lanes_of(y_count)
    packed = jnp.zeros((y_count, LANES), F32)
    k = 0
    for c in comps:
        for z in range(z_count):
            rows = pl.ds(PAD, y_count)
            tile = ref[c, z + 1, rows, 0:LANES]
            if width > LANES:
                last = ref[c, z + 1, rows, width - LANES : width]
                tile = jnp.where(lane >= LANES // 2, last, tile)
            packed = jnp.where(lane // 2 == k, pltpu.roll(tile, 2 * k + 1, 1), packed)
            k += 1
    return packed


def unpack_x(ref, comps, z_count, y_count, width, from_left, from_right):
    lane = lanes_of(y_count)
    both = jnp.where(lane % 2 == 0, from_left, from_right)
    k = 0
    for c in comps:
        for z in range(z_count):
            ref[c, z + 1, pl.ds(PAD, y_count), width : width + LANES] = pltpu.roll(
                both, LANES - 1 - 2 * k, 1
            )
            k += 1


def diff_x(ref, c, z0, zn, y_count, width, scale):
    v = ref[c, z0 : z0 + zn, PAD : PAD + y_count, :]
    span = width + LANES
    return (pltpu.roll(v, span - 1, 2) - pltpu.roll(v, 1, 2))[:, :, :width] * scale


def diff_y(ref, c, z0, zn, y_count, width, scale):
    after = ref[c, z0 : z0 + zn, PAD + 1 : PAD + 1 + y_count, 0:width]
    before = ref[c, z0 : z0 + zn, PAD - 1 : PAD - 1 + y_count, 0:width]
    return (after - before) * scale


def diff_z(ref, c, z0, zn, y_count, width, scale):
    after = ref[c, z0 + 1 : z0 + 1 + zn, PAD : PAD + y_count, 0:width]
    before = ref[c, z0 - 1 : z0 - 1 + zn, PAD : PAD + y_count, 0:width]
    return (after - before) * scale


def stress_block(u, stiff, s, z, zn, y_count, width, inv, stretch):
    args = (z + 1, zn, y_count, width, inv)
    own = (slice(z + 1, z + 1 + zn), slice(PAD, PAD + y_count), slice(0, width))
    c = [stiff[i, z : z + zn] for i in range(9)]
    nx = diff_x(u, 0, *args)
    ny = diff_y(u, 1, *args)
    nz = diff_z(u, 2, *args) * stretch
    s[(XX,) + own] = c[0] * nx + c[6] * ny + c[7] * nz
    s[(YY,) + own] = c[6] * nx + c[1] * ny + c[8] * nz
    s[(ZZ,) + own] = c[7] * nx + c[8] * ny + c[2] * nz
    s[(YZ,) + own] = c[3] * (diff_z(u, 1, *args) * stretch + diff_y(u, 2, *args))
    s[(XZ,) + own] = c[4] * (diff_z(u, 0, *args) * stretch + diff_x(u, 2, *args))
    s[(XY,) + own] = c[5] * (diff_y(u, 0, *args) + diff_x(u, 1, *args))


def step_block(u, s, prev, dens, out, z, zn, y_count, width, inv, stretch):
    args = (z + 1, zn, y_count, width, inv)
    gain = (TIME_STEP * TIME_STEP) / dens[z : z + zn]
    for c, (sx, sy, sz) in enumerate(((XX, XY, XZ), (XY, YY, YZ), (XZ, YZ, ZZ))):
        total = diff_x(s, sx, *args) + diff_y(s, sy, *args) + diff_z(s, sz, *args) * stretch
        now = u[c, z + 1 : z + 1 + zn, PAD : PAD + y_count, 0:width]
        out[c, z : z + zn] = (2.0 * now - prev[c, z : z + zn]) + gain * total


def stress_ext(u, stiff, s, layer, slab, y_count, width, inv):
    z, first, rows, span = layer + 1, PAD - 1, y_count + 2, width + LANES

    def at(c, dz, dr):
        return u[c, z + dz, first + dr : first + dr + rows, :]

    def dx(c):
        v = at(c, 0, 0)
        return (pltpu.roll(v, span - 1, 1) - pltpu.roll(v, 1, 1)) * inv

    def dy(c):
        return (at(c, 0, 1) - at(c, 0, -1)) * inv

    def dz(c):
        return (at(c, 1, 0) - at(c, -1, 0)) * inv

    c = [stiff[i, slab, first : first + rows, :] for i in range(9)]
    nx, ny, nz = dx(0), dy(1), dz(2)
    values = {
        XX: c[0] * nx + c[6] * ny + c[7] * nz,
        YY: c[6] * nx + c[1] * ny + c[8] * nz,
        ZZ: c[7] * nx + c[8] * ny + c[2] * nz,
        YZ: c[3] * (dz(1) + dy(2)),
        XZ: c[4] * (dz(0) + dx(2)),
        XY: c[5] * (dy(0) + dx(1)),
    }
    for component, value in values.items():
        s[component, z, first : first + rows, :] = value


def pick(x, index):
    return jnp.take_along_axis(x, index, axis=1, mode="promise_in_bounds")


class Grid:
    def __init__(self, **fields):
        self.__dict__.update(fields)
        self.own = (slice(1, self.z + 1), slice(PAD, PAD + self.y), slice(0, self.x))


def kernel(
    counts,
    fn, fp, st, me, de, cn, cp, cst, cde,
    fout, cout,
    u, uc, s, sc, fprev, stiff, metric, dens, cprev, cstiff, cdens,
    xs, xr, ys, yr,
    fwide, cwide, yef_s, yef_r, yec_s, yec_r, xef_s, xef_r, xec_s, xec_r,
    npf_s, npf_r, npc_s, npc_r,
    tiles, sums, own, own_opp, ikf_opp, yi_s, yi_r, ys3, yo3, xs3, xr3, xo3, ext,
    load_sem, send_sem, recv_sem,
):
    n_z, n_y, n_x = counts
    zf, yf, xf = me.shape
    zc, yc, xc = cde.shape
    fine = Grid(
        z=zf, y=yf, x=xf, u=u, s=s, wide=fwide, source=st, stiff=stiff, third=0, prev=fprev, dens=dens, out=fout, inv=0.5,
        slabs=(1, 2), near=zf - 3, np_s=npf_s, np_r=npf_r, ye_s=yef_s, ye_r=yef_r, xe_s=xef_s, xe_r=xef_r,
    )
    coarse = Grid(
        z=zc, y=yc, x=xc, u=uc, s=sc, wide=cwide, source=cst, stiff=cstiff, third=2, prev=cprev, dens=cdens, out=cout, inv=0.25,
        slabs=(0, 1), near=0, np_s=npc_s, np_r=npc_r, ye_s=yec_s, ye_r=yec_r, xe_s=xec_s, xe_r=xec_r,
    )
    gz, gy, gx = lax.axis_index("gz"), lax.axis_index("gy"), lax.axis_index("gx")
    opp = n_z - 1 - gz
    is_c, is_f = gz == 0, gz == n_z - 1
    active = jnp.logical_or(is_c, is_f)
    has_y = {-1: gy > 0, 0: gy >= 0, 1: gy < n_y - 1}
    has_x = {-1: gx > 0, 0: gx >= 0, 1: gx < n_x - 1}
    has = (gz > 0, gz < n_z - 1, has_y[-1], has_y[1], has_x[-1], has_x[1])
    near = (
        (gz - 1, gy, gx), (gz + 1, gy, gx),
        (gz, gy - 1, gx), (gz, gy + 1, gx),
        (gz, gy, gx - 1), (gz, gy, gx + 1),
    )

    barrier = pltpu.get_barrier_semaphore()
    expected = jnp.int32(0)

    def greet(there, device):
        @pl.when(there)
        def _():
            pl.semaphore_signal(barrier, 1, device_id=device, device_id_type=pl.DeviceIdType.MESH)

        return there.astype(jnp.int32)

    for d in (2, 3, 4, 5, 0, 1):
        expected += greet(has[d], near[d])
    for a in (-1, 1):
        for b in (-1, 1):
            there = jnp.logical_and(active, jnp.logical_and(has_y[a], has_x[b]))
            expected += greet(there, (gz, gy + a, gx + b))
    expected += greet(active, (opp, gy, gx))

    loads = [
        pltpu.make_async_copy(src, dst, load_sem.at[i])
        for i, (src, dst) in enumerate((
            (fn, u.at[(slice(None),) + fine.own]),
            (cn, uc.at[(slice(None),) + coarse.own]),
            (de, dens), (cde, cdens), (fp, fprev), (cp, cprev),
            (st, stiff), (cst, cstiff), (me, metric),
        ))
    ]

    def wide_load(g):
        return pltpu.make_async_copy(
            g.source.at[:, g.near : g.near + 3], g.wide.at[(slice(None), slice(None)) + g.own[1:]], load_sem.at[9]
        )

    sides = ((is_f, fine), (is_c, coarse))
    for load in loads[:2]:
        load.start()
    for there, g in sides:
        @pl.when(there)
        def _(g=g):
            wide_load(g).start()
    for load in loads[2:]:
        load.start()

    def clear(part):
        part[...] = jnp.zeros(part.shape, F32)

    for there, g in sides:
        @pl.when(there)
        def _(g=g):
            for rows in (pl.ds(0, PAD), pl.ds(PAD + g.y, PAD)):
                clear(g.u.at[:, g.near + 1 : g.near + 4, rows])
                clear(g.wide.at[:, :, rows])

    for d in range(6):
        @pl.when(jnp.logical_not(has[d]))
        def _(d=d):
            side = d % 2
            if d < 2:
                for g in (fine, coarse):
                    plane = 0 if side == 0 else g.z + 1
                    clear(g.u.at[:, plane])
                    clear(g.s.at[3:6, plane, g.own[1], g.own[2]])
            elif d < 4:
                for r in range(2):
                    clear(yr.at[r, side])
                for g in (fine, coarse):
                    clear(g.ye_r.at[side])
                    clear(g.np_r.at[side])
                    for b in range(2):
                        clear(g.xe_r.at[b, pl.ds(0 if side == 0 else PAD + g.y, PAD)])
            else:
                for r in range(2):
                    clear(xr.at[r, side])
                for g in (fine, coarse):
                    clear(g.xe_r.at[side])

    def rdma(src, dst, out, into, device):
        return pltpu.make_async_remote_copy(
            src_ref=src, dst_ref=dst, send_sem=send_sem.at[out], recv_sem=recv_sem.at[into],
            device_id=device, device_id_type=pl.DeviceIdType.MESH,
        )

    def round_copies(r, d):
        side = d % 2
        arrival = 1 - side
        if d < 2:
            comps = (slice(0, 3), slice(3, 6))[r]
            made = []
            for i, g in enumerate((fine, coarse)):
                ref = (g.u, g.s)[r]
                sent, landed = (1, g.z + 1) if side == 0 else (g.z, 0)
                made.append(rdma(
                    ref.at[comps, sent, g.own[1], g.own[2]], ref.at[comps, landed, g.own[1], g.own[2]],
                    2 * d + i, 8 * r + 2 * d + i, near[d],
                ))
            return made
        if d < 4:
            return [rdma(ys.at[r, side], yr.at[r, arrival], d + 2, 8 * r + d + 2, near[d])]
        return [rdma(xs.at[r], xr.at[r, arrival], d + 2, 8 * r + d + 2, near[d])]

    def start_round(r, directions):
        for d in directions:
            @pl.when(has[d])
            def _(d=d):
                for copy in round_copies(r, d):
                    copy.start()

    def end_round(r, directions):
        for d in directions:
            @pl.when(has[d ^ 1])
            def _(d=d):
                for copy in round_copies(r, d):
                    copy.wait_recv()

    def row_parts(g, ref, c, row):
        if g is fine:
            return [(ref.at[c, 1 : zf + 1, row : row + 1, 0:xf], (c, slice(0, zf), slice(None), slice(0, xf)))]
        half = zc // 2
        return [
            (
                ref.at[c, 1 + i * half : 1 + (i + 1) * half, row : row + 1, 0:xc],
                (c, slice(zf, zf + half), slice(None), slice(i * xc, (i + 1) * xc)),
            )
            for i in range(2)
        ]

    def pack_rows(r, refs, face_y):
        for g, ref in ((fine, refs[0]), (coarse, refs[1])):
            for side, row in enumerate((PAD, PAD + g.y - 1)):
                for i, c in enumerate(face_y):
                    for part, place in row_parts(g, ref, c, row):
                        ys[(r, side, i) + place[1:]] = part[...]

    def pack_columns(r, refs, face_x):
        xs[r, 0:yf] = pack_x(refs[0], face_x, zf, yf, xf)
        xs[r, yf : yf + yc] = pack_x(refs[1], face_x, zc, yc, xc)

    def unpack_rows(r, g, ref, face_y):
        for side, row in enumerate((PAD - 1, PAD + g.y)):
            for i, c in enumerate(face_y):
                for part, place in row_parts(g, ref, c, row):
                    part[...] = yr[(r, side, i) + place[1:]]

    def unpack(r, refs, face_x, face_y):
        unpack_rows(r, fine, refs[0], face_y)
        unpack_rows(r, coarse, refs[1], face_y)
        unpack_x(refs[0], face_x, zf, yf, xf, xr[r, 0, 0:yf], xr[r, 1, 0:yf])
        unpack_x(refs[1], face_x, zc, yc, xc, xr[r, 0, yf : yf + yc], xr[r, 1, yf : yf + yc])

    def pack_wide_rows(g):
        first = g.near + g.slabs[0]
        for side, (edge, second) in enumerate(((PAD, PAD + 1), (PAD + g.y - 1, PAD + g.y - 2))):
            out = g.ye_s.at[side]
            for c in range(3):
                out[2 * c : 2 * c + 2] = g.u[c, first + 1 : first + 3, second : second + 1, 0 : g.x]
            for i, c in enumerate(WIDE_Y):
                out[6 + 3 * i : 9 + 3 * i] = g.wide[c, :, edge : edge + 1, 0 : g.x]
            for i, row in enumerate((edge, second)):
                out[21 + 2 * i : 23 + 2 * i] = g.dens[first : first + 2, row - PAD : row - PAD + 1, :]
                if g is coarse:
                    for c in range(3):
                        out[25 + 3 * i + c] = g.wide[CH[c], 0, row : row + 1, 0 : g.x]

    def pack_wide_columns(g):
        lane = lanes_of(g.y)
        packed = jnp.zeros((g.y, LANES), F32)
        for k, (ref, index) in enumerate(wide_blocks(g)):
            tile = ref[index + (g.own[1], slice(0, LANES))]
            if g.x > LANES:
                last = ref[index + (g.own[1], slice(g.x - LANES, g.x))]
                tile = jnp.where(lane >= LANES // 2, last, tile)
            packed = jnp.where(lane // 4 == k, pltpu.roll(tile, 4 * k + 2, 1), packed)
        g.xe_s[...] = packed

    def wide_blocks(g):
        blocks = [(g.u, (c, g.near + l + 1)) for c in range(3) for l in range(3)]
        return blocks + [(g.wide, (c, l)) for c in WIDE_X for l in g.slabs]

    def wide_rows(g):
        return [
            (has_y[a], has_y[-a], rdma(g.ye_s.at[i], g.ye_r.at[1 - i], 11 + i, 19 + i, (gz, gy + a, gx)))
            for i, a in enumerate((-1, 1))
        ]

    def wide_columns(g, ups):
        made = []
        for i, b in enumerate((-1, 1)):
            for a in ups:
                src, dst = {
                    -1: (slice(0, PAD), slice(PAD + g.y, 2 * PAD + g.y)),
                    0: (slice(0, g.y), slice(PAD, PAD + g.y)),
                    1: (slice(g.y - PAD, g.y), slice(0, PAD)),
                }[a]
                made.append((
                    jnp.logical_and(has_y[a], has_x[b]), jnp.logical_and(has_y[-a], has_x[-b]),
                    rdma(
                        g.xe_s.at[src], g.xe_r.at[1 - i, dst], 13 + i * 3 + (a + 1), 21 + i * 3 + (a + 1),
                        (gz, gy + a, gx + b),
                    ),
                ))
        return made

    def part_rows(g):
        return [
            (has_y[a], has_y[-a], rdma(g.np_s.at[i], g.np_r.at[1 - i], 19 + i, 27 + i, (gz, gy + a, gx)))
            for i, a in enumerate((-1, 1))
        ]

    def unpack_wide_rows(g):
        first = g.near + g.slabs[0]
        unpack_rows(0, g, g.u, (0, 1, 2))
        for side, (edge, second) in enumerate(((PAD - 1, PAD - 2), (PAD + g.y, PAD + g.y + 1))):
            landed = g.ye_r.at[side]
            for c in range(3):
                g.u[c, first + 1 : first + 3, second : second + 1, 0 : g.x] = landed[2 * c : 2 * c + 2]
            for i, c in enumerate(WIDE_Y):
                g.wide[c, :, edge : edge + 1, 0 : g.x] = landed[6 + 3 * i : 9 + 3 * i]

    def unpack_wide_columns(g, row, count):
        rows = slice(row, row + count)
        both = jnp.where(lanes_of(count) % 4 < 2, g.xe_r[0, rows], g.xe_r[1, rows])
        for k, (ref, index) in enumerate(wide_blocks(g)):
            ref[index + (rows, slice(g.x, g.x + LANES))] = pltpu.roll(both, LANES - (4 * k + 2), 1)

    def interface_step(g):
        stress_block(g.u, g.stiff, g.s, g.near + g.third, 1, g.y, g.x, g.inv, 1.0)
        for l in g.slabs:
            stress_ext(g.u, g.wide, g.s, g.near + l, l, g.y, g.x, g.inv)
        for l in g.slabs:
            step_block(g.u, g.s, g.prev, g.dens, g.out, g.near + l, 1, g.y, g.x, g.inv, 1.0)

    def beyond_edges(g):
        first = g.near + g.slabs[0]
        span = g.x + LANES
        result = []
        for side, (sign, edge, adjacent) in enumerate(((1.0, PAD, PAD - 1), (-1.0, PAD + g.y - 1, PAD + g.y))):
            scale = sign * g.inv
            d = [g.u[c, g.near + 1 : g.near + 4, edge : edge + 1, :] * scale for c in range(3)]
            w = {c: g.wide[c, :, adjacent : adjacent + 1, :] for c in WIDE_Y}
            s_xx, s_yy, s_zz, s_yz, s_xy = w[6] * d[1], w[1] * d[1], w[8] * d[1], w[3] * d[2], w[5] * d[0]

            def two(v):
                return v[g.slabs[0] : g.slabs[0] + 2, :, 0 : g.x]

            def along_x_of(v):
                v = v[g.slabs[0] : g.slabs[0] + 2]
                return (pltpu.roll(v, span - 1, 2) - pltpu.roll(v, 1, 2))[:, :, 0 : g.x] * g.inv

            def along_z_of(v):
                v = v[:, :, 0 : g.x]
                parts = []
                for l in g.slabs:
                    parts.append((v[l + 1 : l + 2] if l < 2 else 0.0) - (v[l - 1 : l] if l > 0 else 0.0))
                return jnp.concatenate(parts, 0) * g.inv

            def edge_stress(component):
                return g.s[component, first + 1 : first + 3, edge : edge + 1, 0 : g.x] * scale

            totals = (
                (
                    along_x_of(s_xx) + edge_stress(XY),
                    along_x_of(s_xy) + edge_stress(YY) + along_z_of(s_yz),
                    edge_stress(YZ) + along_z_of(s_zz),
                ),
                (two(s_xy) * scale, two(s_yy) * scale, two(s_yz) * scale),
            )
            rows = []
            for i in range(2):
                gain = (TIME_STEP * TIME_STEP) / g.ye_r[side, 21 + 2 * i : 23 + 2 * i]
                index = 1 - i if side == 0 else i
                rows.append([g.np_r[side, index, c] + gain * totals[i][c] for c in range(3)])
            result.append(rows)
        return result

    def start_all(copies):
        for there, _, copy in copies:
            @pl.when(there)
            def _(copy=copy):
                copy.start()

    def receive_all(copies):
        for _, comes, copy in copies:
            @pl.when(comes)
            def _(copy=copy):
                copy.wait_recv()

    def sent_all(copies):
        for there, _, copy in copies:
            @pl.when(there)
            def _(copy=copy):
                copy.wait_send()

    with jax.named_scope("load_pack"):
        loads[0].wait()
        loads[1].wait()
        for there, g in sides:
            @pl.when(there)
            def _(g=g):
                wide_load(g).wait()
                pack_wide_columns(g)
        pack_rows(0, (u, uc), (0, 1, 2))
        loads[2].wait()
        loads[3].wait()
        for there, g in sides:
            @pl.when(there)
            def _(g=g):
                pack_wide_rows(g)
        pack_columns(0, (u, uc), (0, 1, 2))
    with jax.named_scope("barrier"):
        pl.semaphore_wait(barrier, expected)
    with jax.named_scope("send_0"):
        for there, g in sides:
            @pl.when(there)
            def _(g=g):
                start_all(wide_columns(g, (0,)))
        start_round(0, (2, 3))
        for there, g in sides:
            @pl.when(there)
            def _(g=g):
                start_all(wide_rows(g))
                start_all(wide_columns(g, (-1, 1)))
        start_round(0, (4, 5, 0, 1))
        for load in loads[4:]:
            load.wait()

    lane = lanes_of(yc)
    even = (2 * lane) % LANES

    def squeeze(left, right, odd):
        return jnp.where(lane < LANES // 2, pick(left, even + odd), pick(right, even + odd))

    ikf_copy = rdma(own.at[6:18, 8:16], ikf_opp, 8, 16, (opp, gy, gx))
    ikf_rows = [
        (has_y[a], has_y[-a], rdma(yi_s.at[i], yi_r.at[1 - i], 9 + i, 17 + i, (gz, gy + a, gx))) for i, a in enumerate((-1, 1))
    ]

    @pl.when(is_f)
    def _():
        for c in range(3):
            inverse = 1.0 / stiff[CH[c], zf - 1]
            for t in range(2):
                tiles[t] = inverse[:, t * LANES : (t + 1) * LANES]
            for py in range(2):
                rows = pl.ds(py, yc, stride=2)
                left, right = tiles[0, rows, :], tiles[1, rows, :]
                for px in range(2):
                    own[6 + c * 4 + py * 2 + px, 8:16] = squeeze(left, right, px)
        yi_s[0] = own[6:18, 8:9, :]
        yi_s[1] = own[6:18, yc + 7 : yc + 8, :]
        ikf_copy.start()
        start_all(ikf_rows)

    with jax.named_scope("wait_part"):
        for there, g in sides:
            @pl.when(there)
            def _(g=g):
                receive_all(wide_columns(g, (0,)))

    for there, g in sides:
        @pl.when(there)
        def _(g=g):
            unpack_wide_columns(g, PAD, g.y)
            interface_step(g)
            first = g.near + g.slabs[0]
            for side, row in enumerate((0, g.y - 2)):
                for i in range(2):
                    for c in range(3):
                        g.np_s[side, i, c] = g.out[c, first : first + 2, row + i : row + i + 1, :]
            start_all(part_rows(g))

    with jax.named_scope("wait_wide"):
        for there, g in sides:
            @pl.when(there)
            def _(g=g):
                end_round(0, (2, 3))
                receive_all(wide_rows(g))
                receive_all(wide_columns(g, (-1, 1)))

    for there, g in sides:
        @pl.when(there)
        def _(g=g):
            unpack_wide_rows(g)
            unpack_wide_columns(g, 0, PAD)
            unpack_wide_columns(g, PAD + g.y, PAD)
            interface_step(g)

    @pl.when(is_c)
    def _():
        for c in range(3):
            start, below = cout[c, 0], cout[c, 1]
            k = cstiff[CH[c], 0] * 0.25
            own[c, 8:16] = k * (below - start)
            own[3 + c, 8:16] = below - 0.5 * start
            own[6 + c, 8:16] = k

    @pl.when(is_f)
    def _():
        for c in range(3):
            for i, z in enumerate((zf - 2, zf - 1)):
                plane = fout[c, z]
                pairs = []
                for t in range(2):
                    tiles[t] = plane[:, t * LANES : (t + 1) * LANES]
                    pair = tiles[t, pl.ds(0, yc, stride=2), :] + tiles[t, pl.ds(1, yc, stride=2), :]
                    pairs.append(pair + pltpu.roll(pair, LANES - 1, 1))
                own[3 * i + c, 8:16] = squeeze(pairs[0], pairs[1], 0) * 0.25

    with jax.named_scope("wait_beyond"):
        for there, g in sides:
            @pl.when(there)
            def _(g=g):
                receive_all(part_rows(g))

        @pl.when(is_f)
        def _():
            receive_all(ikf_rows)

    @pl.when(is_c)
    def _():
        for side, rows in enumerate(beyond_edges(coarse)):
            for i in range(2):
                place = (7 - i) if side == 0 else (16 + i)
                for c in range(3):
                    start, below = rows[i][c][0], rows[i][c][1]
                    k = yec_r[side, 25 + 3 * i + c] * 0.25
                    own[c, place : place + 1] = k * (below - start)
                    own[3 + c, place : place + 1] = below - 0.5 * start
                    own[6 + c, place : place + 1] = k

    @pl.when(is_f)
    def _():
        for side, rows in enumerate(beyond_edges(fine)):
            for c in range(3):
                both = rows[0][c] + rows[1][c]
                for i in range(2):
                    k = side * 6 + 3 * i + c
                    for t in range(2):
                        sums[t, k : k + 1] = both[i, :, t * LANES : (t + 1) * LANES]
        pairs = [sums[t] + pltpu.roll(sums[t], LANES - 1, 1) for t in range(2)]
        lane16 = lanes_of(16)
        index = (2 * lane16) % LANES
        tiles[0] = jnp.where(lane16 < LANES // 2, pick(pairs[0], index), pick(pairs[1], index)) * 0.25
        for side, place in enumerate((7, 16)):
            for k in range(6):
                own[k, place : place + 1] = tiles[0, side * 6 + k : side * 6 + k + 1]
            own[6:18, place : place + 1] = yi_r[side]

    fields = 18
    strips = [
        (active, active, rdma(own.at[0:9, 8:16], own_opp, 13, 29, (opp, gy, gx))),
        (active, active, rdma(ys3, yo3, 14, 30, (opp, gy, gx))),
    ]
    for level, tile_to, out, into in ((opp, xo3, 15, 33), (gz, xr3, 17, 31)):
        for i, b in enumerate((-1, 1)):
            strips.append((
                jnp.logical_and(active, has_x[b]), jnp.logical_and(active, has_x[-b]),
                rdma(xs3, tile_to.at[1 - i], out + i, into + i, (level, gy, gx + b)),
            ))
    opp_strips, level_strips = strips[:4], strips[4:]

    @pl.when(active)
    def _():
        ys3[0] = own[0:9, 6:8, :]
        ys3[1] = own[0:9, 16:18, :]
        packed = jnp.zeros((24, LANES), F32)
        lane4 = lanes_of(24) // 4
        for k in range(fields):
            packed = jnp.where(lane4 == k, pltpu.roll(own[k], 4 * k + 2, 1), packed)
        xs3[...] = packed

    for there, g in sides:
        @pl.when(there)
        def _(g=g):
            sent_all(wide_columns(g, (-1, 0, 1)))

    start_all(strips)

    def stretch_of(z):
        return jnp.where(gz * zf + z < n_z * zf // 2, metric[z : z + 1], 1.0)

    zb = min(4, zc)

    with jax.named_scope("wait_0"):
        @pl.when(jnp.logical_not(active))
        def _():
            end_round(0, (2, 3))

        end_round(0, (0, 1, 4, 5))
    with jax.named_scope("stress"):
        unpack(0, (u, uc), (0, 1, 2), (0, 1, 2))
        for z in range(zf):
            stress_block(u, stiff, s, z, 1, yf, xf, 0.5, stretch_of(z))
        for z in range(0, zc, zb):
            stress_block(uc, cstiff, sc, z, zb, yc, xc, 0.25, 1.0)
    with jax.named_scope("pack_1"):
        pack_rows(1, (s, sc), FACE_Y)
        for d in range(6):
            @pl.when(has[d])
            def _(d=d):
                for copy in round_copies(0, d):
                    copy.wait_send()
        start_round(1, (2, 3))
        pack_columns(1, (s, sc), FACE_X)
        start_round(1, (4, 5, 0, 1))
    with jax.named_scope("wait_1"):
        end_round(1, (0, 1, 4, 5, 2, 3))
    with jax.named_scope("step"):
        unpack(1, (s, sc), FACE_X, FACE_Y)
        for z in range(zf):
            step_block(u, s, fprev, dens, fout, z, 1, yf, xf, 0.5, stretch_of(z))
        for z in range(0, zc, zb):
            step_block(uc, sc, cprev, cdens, cout, z, zb, yc, xc, 0.25, 1.0)

    lane24 = lax.broadcasted_iota(jnp.int32, (24, LANES), 1)
    wide_row = lax.broadcasted_iota(jnp.int32, (24, 2 * LANES), 0)
    wide_lane = lax.broadcasted_iota(jnp.int32, (24, 2 * LANES), 1)

    def extend(k, field, centre, rims, row, edges):
        ext[k, 8:16, 0:LANES] = centre
        ext[k, 6:8, 0:LANES] = rims[0, row]
        ext[k, 16:18, 0:LANES] = rims[1, row]
        ext[k, :, LANES : 2 * LANES] = pltpu.roll(edges, LANES - (4 * field + 2), 1)

    def clamp(t):
        t = jnp.where(jnp.logical_and(wide_row == 7, gy == 0), pltpu.roll(t, 23, 0), t)
        t = jnp.where(jnp.logical_and(wide_row == 16, gy == n_y - 1), pltpu.roll(t, 1, 0), t)
        t = jnp.where(jnp.logical_and(wide_lane == 2 * LANES - 1, gx == 0), pltpu.roll(t, 2 * LANES - 1, 1), t)
        return jnp.where(jnp.logical_and(wide_lane == LANES, gx == n_x - 1), pltpu.roll(t, 1, 1), t)

    def along_y(t):
        return (0.75 * t + 0.25 * pltpu.roll(t, 1, 0), 0.75 * t + 0.25 * pltpu.roll(t, 23, 0))

    def along_x(t):
        return (0.75 * t + 0.25 * pltpu.roll(t, 1, 1), 0.75 * t + 0.25 * pltpu.roll(t, 2 * LANES - 1, 1))

    def extend_own(k, field, edges):
        ext[k, :, 0:LANES] = own[field]
        ext[k, :, LANES : 2 * LANES] = pltpu.roll(edges, LANES - (4 * field + 2), 1)

    with jax.named_scope("wait_level"):
        receive_all(level_strips)

    @pl.when(is_c)
    def _():
        edges = jnp.where(lane24 % 4 < 2, xr3[0], xr3[1])
        for k in range(3, 9):
            extend_own(k, k, edges)
        ikf_copy.wait_recv()

    @pl.when(is_f)
    def _():
        edges = jnp.where(lane24 % 4 < 2, xr3[0], xr3[1])
        for k in range(3):
            extend_own(9 + k, k, edges)
        for k in range(12):
            extend_own(12 + k, 6 + k, edges)

    with jax.named_scope("wait_opp"):
        receive_all(opp_strips)

    @pl.when(is_c)
    def _():
        edges = jnp.where(lane24 % 4 < 2, xo3[0], xo3[1])
        for c in range(3):
            extend(9 + c, 3 + c, own_opp[3 + c], yo3, 3 + c, edges)
            t1 = clamp(ext[6 + c] * (ext[3 + c] - 0.5 * ext[9 + c]))
            total = jnp.zeros((yc, LANES), F32)
            for py, part in enumerate(along_y(t1)):
                for px, full in enumerate(along_x(part[8:16])):
                    total += full[:, 0:LANES] * ikf_opp[c * 4 + py * 2 + px]
            cout[c, 0] = 0.5 * (cout[c, 0] + own_opp[c] + 0.25 * total)

    @pl.when(is_f)
    def _():
        edges = jnp.where(lane24 % 4 < 2, xo3[0], xo3[1])
        half = lane // 2
        for c in range(3):
            for k in (c, 3 + c, 6 + c):
                extend(k, k, own_opp[k], yo3, k, edges)
            total = jnp.zeros((24, 2 * LANES), F32)
            for py, part in enumerate(along_y(clamp(ext[c]))):
                for px, full in enumerate(along_x(part)):
                    total += full * ext[12 + c * 4 + py * 2 + px]
            t2 = clamp(ext[6 + c] * (ext[3 + c] - 0.5 * (ext[9 + c] + 0.25 * total)))
            for py, part in enumerate(along_y(t2)):
                evens, odds = along_x(part[8:16])
                evens, odds = evens[:, 0:LANES], odds[:, 0:LANES]
                for t in range(2):
                    index = half + t * (LANES // 2)
                    tiles[t, pl.ds(py, yc, stride=2), :] = jnp.where(
                        lane % 2 == 0, pick(evens, index), pick(odds, index)
                    )
            for t in range(2):
                cols = slice(t * LANES, (t + 1) * LANES)
                fout[c, zf - 1, :, cols] = fout[c, zf - 2, :, cols] + tiles[t] / stiff[CH[c], zf - 1, :, cols]

    with jax.named_scope("drain"):
        for d in range(6):
            @pl.when(has[d])
            def _(d=d):
                for copy in round_copies(1, d):
                    copy.wait_send()
        sent_all(strips)
        for there, g in sides:
            @pl.when(there)
            def _(g=g):
                sent_all(wide_rows(g))
                sent_all(part_rows(g))

        @pl.when(is_f)
        def _():
            ikf_copy.wait_send()
            sent_all(ikf_rows)


def per_device(counts, *args):
    fine, coarse = args[0].shape, args[5].shape
    _, zf, yf, xf = fine
    _, zc, yc, xc = coarse
    vmem = lambda *shape: pltpu.VMEM(shape, F32)
    anywhere = pl.BlockSpec(memory_space=pl.ANY)
    in_vmem = pl.BlockSpec(memory_space=pltpu.VMEM)
    return pl.pallas_call(
        functools.partial(kernel, counts),
        out_shape=(pltpu.VMEM(fine, F32), pltpu.VMEM(coarse, F32)),
        in_specs=[anywhere] * 9,
        out_specs=(in_vmem, in_vmem),
        scratch_shapes=[
            vmem(3, zf + 2, yf + 2 * PAD, xf + LANES),
            vmem(3, zc + 2, yc + 2 * PAD, xc + LANES),
            vmem(6, zf + 2, yf + 2 * PAD, xf + LANES),
            vmem(6, zc + 2, yc + 2 * PAD, xc + LANES),
            vmem(3, zf, yf, xf), vmem(9, zf, yf, xf), vmem(zf, yf, xf), vmem(zf, yf, xf),
            vmem(3, zc, yc, xc), vmem(9, zc, yc, xc), vmem(zc, yc, xc),
            vmem(2, yf + yc, LANES), vmem(2, 2, yf + yc, LANES),
            vmem(2, 2, 3, zf + zc // 2, 1, xf), vmem(2, 2, 3, zf + zc // 2, 1, xf),
            vmem(9, 3, yf + 2 * PAD, xf + LANES), vmem(9, 3, yc + 2 * PAD, xc + LANES),
            vmem(2, 31, 1, xf), vmem(2, 31, 1, xf), vmem(2, 31, 1, xc), vmem(2, 31, 1, xc),
            vmem(yf, LANES), vmem(2, yf + 2 * PAD, LANES), vmem(yc, LANES), vmem(2, yc + 2 * PAD, LANES),
            vmem(2, 2, 3, 2, 1, xf), vmem(2, 2, 3, 2, 1, xf), vmem(2, 2, 3, 2, 1, xc), vmem(2, 2, 3, 2, 1, xc),
            vmem(2, yf, LANES), vmem(2, yf, LANES), vmem(18, 24, LANES), vmem(9, yc, LANES), vmem(12, yc, LANES),
            vmem(2, 12, 1, LANES), vmem(2, 12, 1, LANES),
            vmem(2, 9, 2, LANES), vmem(2, 9, 2, LANES),
            vmem(24, LANES), vmem(2, 24, LANES), vmem(2, 24, LANES),
            vmem(24, 24, 2 * LANES),
            pltpu.SemaphoreType.DMA((10,)),
            pltpu.SemaphoreType.DMA((21,)),
            pltpu.SemaphoreType.DMA((35,)),
        ],
        compiler_params=pltpu.CompilerParams(
            collective_id=0, has_side_effects=True, vmem_limit_bytes=56 * 1024 * 1024
        ),
        name="elastic_step",
    )(*args)


def solution(mesh):
    counts = tuple(mesh.shape[name] for name in ("gz", "gy", "gx"))
    volume, field = P(None, "gz", "gy", "gx"), P("gz", "gy", "gx")
    return jax.shard_map(
        functools.partial(per_device, counts),
        mesh=mesh,
        in_specs=(volume, volume, volume, field, field, volume, volume, volume, field),
        out_specs=(volume, volume),
        check_vma=False,
    )
```

```python
import functools

import jax
import jax.numpy as jnp
from jax import lax
from jax.experimental import pallas as pl
from jax.experimental.pallas import tpu as pltpu
from jax.sharding import PartitionSpec as P

TIME_STEP = 0.2
ITERS = 3
SPLIT = False
F32 = jnp.float32
XX, XY, YY, XZ, YZ, ZZ = range(6)
FACE_X = (XX, XY, XZ)
FACE_Y = (XY, YY, YZ)
WIDE_Y = (1, 3, 5, 6, 8)
EDGE_Y = (5, 1, 3)
WIDE_X = (0, 4, 5, 6, 7)
CH = (4, 3, 2)
PAD = 8
LANES = 128


def lanes_of(rows):
    return lax.broadcasted_iota(jnp.int32, (rows, LANES), 1)


def pack_x(ref, comps, z_count, y_count, width):
    lane = lanes_of(y_count)
    packed = jnp.zeros((y_count, LANES), F32)
    k = 0
    for c in comps:
        for z in range(z_count):
            rows = pl.ds(PAD, y_count)
            tile = ref[c, z + 1, rows, 0:LANES]
            if width > LANES:
                last = ref[c, z + 1, rows, width - LANES : width]
                tile = jnp.where(lane >= LANES // 2, last, tile)
            packed = jnp.where(lane // 2 == k, pltpu.roll(tile, 2 * k + 1, 1), packed)
            k += 1
    return packed


def unpack_x(ref, comps, z_count, y_count, width, from_left, from_right):
    lane = lanes_of(y_count)
    both = jnp.where(lane % 2 == 0, from_left, from_right)
    k = 0
    for c in comps:
        for z in range(z_count):
            ref[c, z + 1, pl.ds(PAD, y_count), width : width + LANES] = pltpu.roll(
                both, LANES - 1 - 2 * k, 1
            )
            k += 1


def diff_x(ref, c, z0, zn, y_count, width, scale):
    v = ref[c, z0 : z0 + zn, PAD : PAD + y_count, :]
    span = width + LANES
    return (pltpu.roll(v, span - 1, 2) - pltpu.roll(v, 1, 2))[:, :, :width] * scale


def diff_y(ref, c, z0, zn, y_count, width, scale):
    after = ref[c, z0 : z0 + zn, PAD + 1 : PAD + 1 + y_count, 0:width]
    before = ref[c, z0 : z0 + zn, PAD - 1 : PAD - 1 + y_count, 0:width]
    return (after - before) * scale


def diff_z(ref, c, z0, zn, y_count, width, scale):
    after = ref[c, z0 + 1 : z0 + 1 + zn, PAD : PAD + y_count, 0:width]
    before = ref[c, z0 - 1 : z0 - 1 + zn, PAD : PAD + y_count, 0:width]
    return (after - before) * scale


def stress_block(u, stiff, s, z, zn, y_count, width, inv, stretch):
    args = (z + 1, zn, y_count, width, inv)
    own = (slice(z + 1, z + 1 + zn), slice(PAD, PAD + y_count), slice(0, width))
    c = [stiff[i, z : z + zn] for i in range(9)]
    nx = diff_x(u, 0, *args)
    ny = diff_y(u, 1, *args)
    nz = diff_z(u, 2, *args) * stretch
    s[(XX,) + own] = c[0] * nx + c[6] * ny + c[7] * nz
    s[(YY,) + own] = c[6] * nx + c[1] * ny + c[8] * nz
    s[(ZZ,) + own] = c[7] * nx + c[8] * ny + c[2] * nz
    s[(YZ,) + own] = c[3] * (diff_z(u, 1, *args) * stretch + diff_y(u, 2, *args))
    s[(XZ,) + own] = c[4] * (diff_z(u, 0, *args) * stretch + diff_x(u, 2, *args))
    s[(XY,) + own] = c[5] * (diff_y(u, 0, *args) + diff_x(u, 1, *args))


def step_block(u, s, prev, dens, out, z, zn, y_count, width, inv, stretch):
    args = (z + 1, zn, y_count, width, inv)
    gain = (TIME_STEP * TIME_STEP) / dens[z : z + zn]
    for c, (sx, sy, sz) in enumerate(((XX, XY, XZ), (XY, YY, YZ), (XZ, YZ, ZZ))):
        total = diff_x(s, sx, *args) + diff_y(s, sy, *args) + diff_z(s, sz, *args) * stretch
        now = u[c, z + 1 : z + 1 + zn, PAD : PAD + y_count, 0:width]
        out[c, z : z + zn] = (2.0 * now - prev[c, z : z + zn]) + gain * total


def stress_ext(u, stiff, s, layer, slab, y_count, width, inv):
    z, first, rows, span = layer + 1, PAD - 1, y_count + 2, width + LANES

    def at(c, dz, dr):
        return u[c, z + dz, first + dr : first + dr + rows, :]

    def dx(c):
        v = at(c, 0, 0)
        return (pltpu.roll(v, span - 1, 1) - pltpu.roll(v, 1, 1)) * inv

    def dy(c):
        return (at(c, 0, 1) - at(c, 0, -1)) * inv

    def dz(c):
        return (at(c, 1, 0) - at(c, -1, 0)) * inv

    c = [stiff[i, slab, first : first + rows, :] for i in range(9)]
    nx, ny, nz = dx(0), dy(1), dz(2)
    values = {
        XX: c[0] * nx + c[6] * ny + c[7] * nz,
        YY: c[6] * nx + c[1] * ny + c[8] * nz,
        ZZ: c[7] * nx + c[8] * ny + c[2] * nz,
        YZ: c[3] * (dz(1) + dy(2)),
        XZ: c[4] * (dz(0) + dx(2)),
        XY: c[5] * (dy(0) + dx(1)),
    }
    for component, value in values.items():
        s[component, z, first : first + rows, :] = value


def pick(x, index):
    return jnp.take_along_axis(x, index, axis=1, mode="promise_in_bounds")


class Grid:
    def __init__(self, **fields):
        self.__dict__.update(fields)
        self.own = (slice(1, self.z + 1), slice(PAD, PAD + self.y), slice(0, self.x))


def kernel(
    counts,
    fn, fp, st, me, de, cn, cp, cst, cde,
    fout, cout,
    u, uc, s, sc, fprev, stiff, metric, dens, cprev, cstiff, cdens,
    xs, xr, ys, yr,
    fwide, cwide, yef_s, yef_r, yec_s, yec_r, xef_s, xef_r, xec_s, xec_r,
    npf_s, npf_l, npf_o, npc_s, npc_l, npc_o, cs, cr,
    tiles, sums, own, own_opp, ikf_opp, ys3, yo3, xs3, xr3, xo3, ext,
    load_sem, send_sem, recv_sem,
):
    n_z, n_y, n_x = counts
    zf, yf, xf = me.shape
    zc, yc, xc = cde.shape
    fine = Grid(
        z=zf, y=yf, x=xf, u=u, s=s, wide=fwide, source=st, stiff=stiff, third=0, prev=fprev, dens=dens, out=fout, inv=0.5,
        slabs=(1, 2), near=zf - 3, np_s=npf_s, np_l=npf_l, np_o=npf_o, ye_s=yef_s, ye_r=yef_r, xe_s=xef_s, xe_r=xef_r,
    )
    coarse = Grid(
        z=zc, y=yc, x=xc, u=uc, s=sc, wide=cwide, source=cst, stiff=cstiff, third=2, prev=cprev, dens=cdens, out=cout, inv=0.25,
        slabs=(0, 1), near=0, np_s=npc_s, np_l=npc_l, np_o=npc_o, ye_s=yec_s, ye_r=yec_r, xe_s=xec_s, xe_r=xec_r,
    )
    gz, gy, gx = lax.axis_index("gz"), lax.axis_index("gy"), lax.axis_index("gx")
    opp = n_z - 1 - gz
    is_c, is_f = gz == 0, gz == n_z - 1
    active = jnp.logical_or(is_c, is_f)
    has_y = {-1: gy > 0, 0: gy >= 0, 1: gy < n_y - 1}
    has_x = {-1: gx > 0, 0: gx >= 0, 1: gx < n_x - 1}
    has = (gz > 0, gz < n_z - 1, has_y[-1], has_y[1], has_x[-1], has_x[1])
    near = (
        (gz - 1, gy, gx), (gz + 1, gy, gx),
        (gz, gy - 1, gx), (gz, gy + 1, gx),
        (gz, gy, gx - 1), (gz, gy, gx + 1),
    )

    barrier = pltpu.get_barrier_semaphore()
    expected = jnp.int32(0)

    def greet(there, device):
        @pl.when(there)
        def _():
            pl.semaphore_signal(barrier, 1, device_id=device, device_id_type=pl.DeviceIdType.MESH)

        return there.astype(jnp.int32)

    for d in (2, 3, 4, 5, 0, 1):
        expected += greet(has[d], near[d])
    for a in (-1, 1):
        for b in (-1, 1):
            there = jnp.logical_and(active, jnp.logical_and(has_y[a], has_x[b]))
            expected += greet(there, (gz, gy + a, gx + b))
    expected += greet(active, (opp, gy, gx))

    loads = [
        pltpu.make_async_copy(src, dst, load_sem.at[i])
        for i, (src, dst) in enumerate((
            (fn, u.at[(slice(None),) + fine.own]),
            (cn, uc.at[(slice(None),) + coarse.own]),
            (de, dens), (cde, cdens), (fp, fprev), (cp, cprev),
            (st, stiff), (cst, cstiff), (me, metric),
        ))
    ]

    def wide_load(g):
        return pltpu.make_async_copy(
            g.source.at[:, g.near : g.near + 3], g.wide.at[(slice(None), slice(None)) + g.own[1:]], load_sem.at[9]
        )

    sides = ((is_f, fine), (is_c, coarse))
    for load in loads[:2]:
        load.start()
    for there, g in sides:
        @pl.when(there)
        def _(g=g):
            wide_load(g).start()
    for load in loads[2:4]:
        load.start()

    def clear(part):
        part[...] = jnp.zeros(part.shape, F32)

    for there, g in sides:
        @pl.when(there)
        def _(g=g):
            for rows in (pl.ds(0, PAD), pl.ds(PAD + g.y, PAD)):
                clear(g.u.at[:, g.near + 1 : g.near + 4, rows])
                clear(g.wide.at[:, :, rows])

    for g in (fine, coarse):
        for row in (PAD - 1, PAD + g.y):
            clear(g.u.at[:, 1 : g.z + 1, row : row + 1, 0 : g.x])
    for d in range(6):
        @pl.when(jnp.logical_not(has[d]))
        def _(d=d):
            side = d % 2
            if d < 2:
                for g in (fine, coarse):
                    plane = 0 if side == 0 else g.z + 1
                    clear(g.u.at[:, plane])
                    clear(g.s.at[3:6, plane, g.own[1], g.own[2]])
            elif d < 4:
                for r in range(2):
                    clear(yr.at[r, side])
                clear(cr.at[side])
                for g in (fine, coarse):
                    clear(g.ye_r.at[side])
                    for b in range(2):
                        clear(g.xe_r.at[b, pl.ds(0 if side == 0 else PAD + g.y, PAD)])
            else:
                for r in range(2):
                    clear(xr.at[r, side])
                for g in (fine, coarse):
                    clear(g.xe_r.at[side])

    def rdma(src, dst, out, into, device):
        return pltpu.make_async_remote_copy(
            src_ref=src, dst_ref=dst, send_sem=send_sem.at[out], recv_sem=recv_sem.at[into],
            device_id=device, device_id_type=pl.DeviceIdType.MESH,
        )

    def round_copies(r, d):
        side = d % 2
        arrival = 1 - side
        if d < 2:
            comps = (slice(0, 3), slice(3, 6))[r]
            made = []
            for i, g in enumerate((fine, coarse)):
                ref = (g.u, g.s)[r]
                sent, landed = (1, g.z + 1) if side == 0 else (g.z, 0)
                made.append(rdma(
                    ref.at[comps, sent, g.own[1], g.own[2]], ref.at[comps, landed, g.own[1], g.own[2]],
                    (0, 31)[r] + 2 * d + i, 8 * r + 2 * d + i, near[d],
                ))
            return made
        if d < 4:
            return [rdma(ys.at[r, side], yr.at[r, arrival], (d + 2, d + 19)[r], 8 * r + d + 2, near[d])]
        return [rdma(xs.at[r], xr.at[r, arrival], (d + 2, d + 31)[r], 8 * r + d + 2, near[d])]

    def start_round(r, directions):
        for d in directions:
            @pl.when(has[d])
            def _(d=d):
                for copy in round_copies(r, d):
                    copy.start()

    def end_round(r, directions):
        for d in directions:
            @pl.when(has[d ^ 1])
            def _(d=d):
                for copy in round_copies(r, d):
                    copy.wait_recv()

    def row_parts(g, ref, c, row):
        if g is fine:
            return [(ref.at[c, 1 : zf + 1, row : row + 1, 0:xf], (c, slice(0, zf), slice(None), slice(0, xf)))]
        half = zc // 2
        return [
            (
                ref.at[c, 1 + i * half : 1 + (i + 1) * half, row : row + 1, 0:xc],
                (c, slice(zf, zf + half), slice(None), slice(i * xc, (i + 1) * xc)),
            )
            for i in range(2)
        ]

    def pack_rows(r, refs, face_y):
        for g, ref in ((fine, refs[0]), (coarse, refs[1])):
            for side, row in enumerate((PAD, PAD + g.y - 1)):
                for i, c in enumerate(face_y):
                    for part, place in row_parts(g, ref, c, row):
                        ys[(r, side, i) + place[1:]] = part[...]

    def pack_columns(r, refs, face_x):
        xs[r, 0:yf] = pack_x(refs[0], face_x, zf, yf, xf)
        xs[r, yf : yf + yc] = pack_x(refs[1], face_x, zc, yc, xc)

    stiff_rows = [
        (has_y[a], has_y[-a], rdma(cs.at[i], cr.at[1 - i], 23 + i, 35 + i, (gz, gy + a, gx))) for i, a in enumerate((-1, 1))
    ]

    def pack_stiff_rows():
        half = zc // 2
        for i, c in enumerate(EDGE_Y):
            for side in range(2):
                row = (0, yf - 1)[side]
                cs[side, i, 0:zf] = stiff[c, :, row : row + 1, :]
                row = (0, yc - 1)[side]
                for j in range(2):
                    cs[side, i, zf : zf + half, :, j * xc : (j + 1) * xc] = cstiff[
                        c, j * half : (j + 1) * half, row : row + 1, :
                    ]

    def complete_rows():
        for side, sign in enumerate((1.0, -1.0)):
            for g, part in ((fine, slice(0, zf)), (coarse, slice(zf, zf + zc // 2))):
                yr[1, side, :, part] = yr[1, side, :, part] + cr[side, :, part] * ys[0, side, :, part] * (sign * g.inv)

    def unpack_rows(r, g, ref, face_y):
        for side, row in enumerate((PAD - 1, PAD + g.y)):
            for i, c in enumerate(face_y):
                for part, place in row_parts(g, ref, c, row):
                    part[...] = yr[(r, side, i) + place[1:]]

    def unpack_columns(r, refs, face_x):
        unpack_x(refs[0], face_x, zf, yf, xf, xr[r, 0, 0:yf], xr[r, 1, 0:yf])
        unpack_x(refs[1], face_x, zc, yc, xc, xr[r, 0, yf : yf + yc], xr[r, 1, yf : yf + yc])

    def pack_wide_rows(g):
        first = g.near + g.slabs[0]
        for side, (edge, second) in enumerate(((PAD, PAD + 1), (PAD + g.y - 1, PAD + g.y - 2))):
            out = g.ye_s.at[side]
            for c in range(3):
                out[2 * c : 2 * c + 2] = g.u[c, first + 1 : first + 3, second : second + 1, 0 : g.x]
            for i, c in enumerate(WIDE_Y):
                out[6 + 3 * i : 9 + 3 * i] = g.wide[c, :, edge : edge + 1, 0 : g.x]
            for i, row in enumerate((edge, second)):
                out[21 + 2 * i : 23 + 2 * i] = g.dens[first : first + 2, row - PAD : row - PAD + 1, :]
                if g is coarse:
                    for c in range(3):
                        out[25 + 3 * i + c] = g.wide[CH[c], 0, row : row + 1, 0 : g.x]

    def pack_wide_columns(g):
        lane = lanes_of(g.y)
        packed = jnp.zeros((g.y, LANES), F32)
        for k, (ref, index) in enumerate(wide_blocks(g)):
            tile = ref[index + (g.own[1], slice(0, LANES))]
            if g.x > LANES:
                last = ref[index + (g.own[1], slice(g.x - LANES, g.x))]
                tile = jnp.where(lane >= LANES // 2, last, tile)
            packed = jnp.where(lane // 4 == k, pltpu.roll(tile, 4 * k + 2, 1), packed)
        g.xe_s[...] = packed

    def wide_blocks(g):
        blocks = [(g.u, (c, g.near + l + 1)) for c in range(3) for l in range(3)]
        return blocks + [(g.wide, (c, l)) for c in WIDE_X for l in g.slabs]

    def wide_rows(g):
        return [
            (has_y[a], has_y[-a], rdma(g.ye_s.at[i], g.ye_r.at[1 - i], 11 + i, 19 + i, (gz, gy + a, gx)))
            for i, a in enumerate((-1, 1))
        ]

    def wide_columns(g, ups):
        made = []
        for i, b in enumerate((-1, 1)):
            for a in ups:
                src, dst = {
                    -1: (slice(0, PAD), slice(PAD + g.y, 2 * PAD + g.y)),
                    0: (slice(0, g.y), slice(PAD, PAD + g.y)),
                    1: (slice(g.y - PAD, g.y), slice(0, PAD)),
                }[a]
                made.append((
                    jnp.logical_and(has_y[a], has_x[b]), jnp.logical_and(has_y[-a], has_x[-b]),
                    rdma(
                        g.xe_s.at[src], g.xe_r.at[1 - i, dst], 13 + i * 3 + (a + 1), 21 + i * 3 + (a + 1),
                        (gz, gy + a, gx + b),
                    ),
                ))
        return made

    def part_rows(g):
        made = []
        for i, a in enumerate((-1, 1)):
            for b in (-1, 0, 1):
                k = 3 * i + b + 1
                made.append((
                    jnp.logical_and(has_y[a], has_x[b]), jnp.logical_and(has_y[-a], has_x[-b]),
                    rdma(g.np_s.at[i], g.np_l.at[1 - i, 1 - b], 25 + k, 37 + k, (gz, gy + a, gx + b)),
                ))
        return made

    def passed_parts(g):
        source, target = (npf_l.at[:, :, 0:6], npc_o) if g is fine else (npc_l, npf_o)
        return rdma(source, target, 9, 17, (opp, gy, gx))

    def squeeze_rows(row_of):
        for side in range(2):
            for c in range(3):
                both = row_of(side, c)
                for i in range(2):
                    k = side * 6 + 3 * i + c
                    for t in range(2):
                        sums[t, k : k + 1] = both[i, :, t * LANES : (t + 1) * LANES]
        pairs = [sums[t] + pltpu.roll(sums[t], LANES - 1, 1) for t in range(2)]
        lane16 = lanes_of(16)
        index = (2 * lane16) % LANES
        return jnp.where(lane16 < LANES // 2, pick(pairs[0], index), pick(pairs[1], index)) * 0.25

    def unpack_wide_rows(g):
        first = g.near + g.slabs[0]
        for side, (edge, second) in enumerate(((PAD - 1, PAD - 2), (PAD + g.y, PAD + g.y + 1))):
            landed = g.ye_r.at[side]
            for c in range(3):
                g.u[c, first + 1 : first + 3, second : second + 1, 0 : g.x] = landed[2 * c : 2 * c + 2]
            for i, c in enumerate(WIDE_Y):
                g.wide[c, :, edge : edge + 1, 0 : g.x] = landed[6 + 3 * i : 9 + 3 * i]

    def unpack_wide_columns(g, row, count):
        rows = slice(row, row + count)
        both = jnp.where(lanes_of(count) % 4 < 2, g.xe_r[0, rows], g.xe_r[1, rows])
        for k, (ref, index) in enumerate(wide_blocks(g)):
            ref[index + (rows, slice(g.x, g.x + LANES))] = pltpu.roll(both, LANES - (4 * k + 2), 1)

    def interface_step(g):
        stress_block(g.u, g.stiff, g.s, g.near + g.third, 1, g.y, g.x, g.inv, 1.0)
        for l in g.slabs:
            stress_ext(g.u, g.wide, g.s, g.near + l, l, g.y, g.x, g.inv)
        for l in g.slabs:
            step_block(g.u, g.s, g.prev, g.dens, g.out, g.near + l, 1, g.y, g.x, g.inv, 1.0)

    def beyond_edges(g):
        first = g.near + g.slabs[0]
        span = g.x + LANES
        result = []
        for side, (sign, edge, adjacent) in enumerate(((1.0, PAD, PAD - 1), (-1.0, PAD + g.y - 1, PAD + g.y))):
            scale = sign * g.inv
            d = [g.u[c, g.near + 1 : g.near + 4, edge : edge + 1, :] * scale for c in range(3)]
            w = {c: g.wide[c, :, adjacent : adjacent + 1, :] for c in WIDE_Y}
            s_xx, s_yy, s_zz, s_yz, s_xy = w[6] * d[1], w[1] * d[1], w[8] * d[1], w[3] * d[2], w[5] * d[0]

            def two(v):
                return v[g.slabs[0] : g.slabs[0] + 2, :, 0 : g.x]

            def along_x_of(v):
                v = v[g.slabs[0] : g.slabs[0] + 2]
                return (pltpu.roll(v, span - 1, 2) - pltpu.roll(v, 1, 2))[:, :, 0 : g.x] * g.inv

            def along_z_of(v):
                v = v[:, :, 0 : g.x]
                parts = []
                for l in g.slabs:
                    parts.append((v[l + 1 : l + 2] if l < 2 else 0.0) - (v[l - 1 : l] if l > 0 else 0.0))
                return jnp.concatenate(parts, 0) * g.inv

            def edge_stress(component):
                return g.s[component, first + 1 : first + 3, edge : edge + 1, 0 : g.x] * scale

            totals = (
                (
                    along_x_of(s_xx) + edge_stress(XY),
                    along_x_of(s_xy) + edge_stress(YY) + along_z_of(s_yz),
                    edge_stress(YZ) + along_z_of(s_zz),
                ),
                (two(s_xy) * scale, two(s_yy) * scale, two(s_yz) * scale),
            )
            rows = []
            for i in range(2):
                gain = (TIME_STEP * TIME_STEP) / g.ye_r[side, 21 + 2 * i : 23 + 2 * i]
                rows.append([gain * totals[i][c] for c in range(3)])
            result.append(rows)
        return result

    def start_all(copies):
        for there, _, copy in copies:
            @pl.when(there)
            def _(copy=copy):
                copy.start()

    def receive_all(copies):
        for _, comes, copy in copies:
            @pl.when(comes)
            def _(copy=copy):
                copy.wait_recv()

    def sent_all(copies):
        for there, _, copy in copies:
            @pl.when(there)
            def _(copy=copy):
                copy.wait_send()

    with jax.named_scope("load_pack"):
        loads[0].wait()
        loads[1].wait()
        for load in loads[4:]:
            load.start()
        for there, g in sides:
            @pl.when(there)
            def _(g=g):
                wide_load(g).wait()
                pack_wide_columns(g)
        pack_rows(0, (u, uc), (0, 1, 2))
        loads[2].wait()
        loads[3].wait()
        for there, g in sides:
            @pl.when(there)
            def _(g=g):
                pack_wide_rows(g)
        pack_columns(0, (u, uc), (0, 1, 2))
    with jax.named_scope("barrier"):
        pl.semaphore_wait(barrier, expected)
    with jax.named_scope("send_0"):
        for there, g in sides:
            @pl.when(there)
            def _(g=g):
                start_all(wide_columns(g, (0,)))
        start_round(0, (2, 3))
        for there, g in sides:
            @pl.when(there)
            def _(g=g):
                start_all(wide_rows(g))
                start_all(wide_columns(g, (-1, 1)))
        start_round(0, (4, 5, 0, 1))
        for load in loads[4:]:
            load.wait()
        if SPLIT:
            pack_stiff_rows()

    lane = lanes_of(yc)
    even = (2 * lane) % LANES

    def squeeze(left, right, odd):
        return jnp.where(lane < LANES // 2, pick(left, even + odd), pick(right, even + odd))

    ikf_copy = rdma(own.at[6:18, 8:16], ikf_opp, 8, 16, (opp, gy, gx))
    @pl.when(is_f)
    def _():
        for c in range(3):
            inverse = 1.0 / stiff[CH[c], zf - 1]
            for t in range(2):
                tiles[t] = inverse[:, t * LANES : (t + 1) * LANES]
            for py in range(2):
                rows = pl.ds(py, yc, stride=2)
                left, right = tiles[0, rows, :], tiles[1, rows, :]
                for px in range(2):
                    own[6 + c * 4 + py * 2 + px, 8:16] = squeeze(left, right, px)

    k_copy = rdma(own.at[6:9, 8:16], own_opp.at[6:9], 8, 16, (opp, gy, gx))

    @pl.when(is_c)
    def _():
        for c in range(3):
            own[6 + c, 8:16] = cstiff[CH[c], 0] * 0.25

    with jax.named_scope("wait_part"):
        for there, g in sides:
            @pl.when(there)
            def _(g=g):
                receive_all(wide_columns(g, (0,)))

    for there, g in sides:
        @pl.when(there)
        def _(g=g):
            unpack_wide_columns(g, PAD, g.y)
            interface_step(g)

    @pl.when(is_f)
    def _():
        first = fine.near + fine.slabs[0]

        def two_rows(side, c):
            row = (0, yf - 2)[side]
            return fout[c, first : first + 2, row : row + 1, :] + fout[c, first : first + 2, row + 1 : row + 2, :]

        tiles[0] = squeeze_rows(two_rows)
        for side in range(2):
            for k in range(6):
                npf_s[side, k] = tiles[0, side * 6 + k : side * 6 + k + 1]
            npf_s[side, 6:18] = own[6:18, (8, yc + 7)[side] : (9, yc + 8)[side], :]
        start_all(part_rows(fine))
        ikf_copy.start()

    @pl.when(is_c)
    def _():
        for side in range(2):
            for i in range(2):
                row = (i, yc - 1 - i)[side]
                for c in range(3):
                    start, below = cout[c, 0, row : row + 1, :], cout[c, 1, row : row + 1, :]
                    npc_s[side, 6 * i + c] = own[6 + c, 8 + row : 9 + row] * (below - start)
                    npc_s[side, 6 * i + 3 + c] = below - 0.5 * start
        start_all(part_rows(coarse))
        k_copy.start()

    def stretch_of(z):
        return jnp.where(gz * zf + z < n_z * zf // 2, metric[z : z + 1], 1.0)

    zb = min(4, zc)

    def stress_all():
        for z in range(zf):
            stress_block(u, stiff, s, z, 1, yf, xf, 0.5, stretch_of(z))
        for z in range(0, zc, zb):
            stress_block(uc, cstiff, sc, z, zb, yc, xc, 0.25, 1.0)

    with jax.named_scope("wait_near"):
        end_round(0, (4, 5, 0, 1))
    with jax.named_scope("part_stress"):
        unpack_columns(0, (u, uc), (0, 1, 2))
        if SPLIT:
            stress_all()
            pack_rows(1, (s, sc), FACE_Y)
            start_round(1, (2, 3))
            start_all(stiff_rows)

    with jax.named_scope("wait_rows"):
        end_round(0, (2, 3))
        unpack_rows(0, fine, u, (0, 1, 2))
        unpack_rows(0, coarse, uc, (0, 1, 2))

    with jax.named_scope("stress"):
        stress_all()
        if not SPLIT:
            pack_rows(1, (s, sc), FACE_Y)
            start_round(1, (2, 3))
        pack_columns(1, (s, sc), FACE_X)
        start_round(1, (4, 5, 0, 1))

    with jax.named_scope("wait_wide"):
        for there, g in sides:
            @pl.when(there)
            def _(g=g):
                receive_all(wide_rows(g))
                receive_all(wide_columns(g, (-1, 1)))

    for there, g in sides:
        @pl.when(there)
        def _(g=g):
            unpack_wide_rows(g)
            unpack_wide_columns(g, 0, 2 * PAD + g.y)
            interface_step(g)

    @pl.when(is_c)
    def _():
        for c in range(3):
            start, below = cout[c, 0], cout[c, 1]
            own[c, 8:16] = own[6 + c, 8:16] * (below - start)
            own[3 + c, 8:16] = below - 0.5 * start

    @pl.when(is_f)
    def _():
        for c in range(3):
            for i, z in enumerate((zf - 2, zf - 1)):
                plane = fout[c, z]
                pairs = []
                for t in range(2):
                    tiles[t] = plane[:, t * LANES : (t + 1) * LANES]
                    pair = tiles[t, pl.ds(0, yc, stride=2), :] + tiles[t, pl.ds(1, yc, stride=2), :]
                    pairs.append(pair + pltpu.roll(pair, LANES - 1, 1))
                own[3 * i + c, 8:16] = squeeze(pairs[0], pairs[1], 0) * 0.25

    @pl.when(is_c)
    def _():
        for side, rows in enumerate(beyond_edges(coarse)):
            for i in range(2):
                place = (7 - i) if side == 0 else (16 + i)
                for c in range(3):
                    start, below = rows[i][c][0], rows[i][c][1]
                    k = yec_r[side, 25 + 3 * i + c] * 0.25
                    own[c, place : place + 1] = k * (below - start)
                    own[3 + c, place : place + 1] = below - 0.5 * start
                    own[6 + c, place : place + 1] = k

    @pl.when(is_f)
    def _():
        beyond = beyond_edges(fine)
        tiles[0] = squeeze_rows(lambda side, c: beyond[side][0][c] + beyond[side][1][c])
        for side, place in enumerate((7, 16)):
            for k in range(6):
                own[k, place : place + 1] = tiles[0, side * 6 + k : side * 6 + k + 1]

    fields = 18
    strips = [
        (active, active, rdma(own.at[0:6, 8:16], own_opp.at[0:6], 13, 29, (opp, gy, gx))),
        (active, active, rdma(ys3, yo3, 14, 30, (opp, gy, gx))),
    ]
    for level, tile_to, out, into in ((opp, xo3, 15, 33), (gz, xr3, 17, 31)):
        for i, b in enumerate((-1, 1)):
            strips.append((
                jnp.logical_and(active, has_x[b]), jnp.logical_and(active, has_x[-b]),
                rdma(xs3, tile_to.at[1 - i], out + i, into + i, (level, gy, gx + b)),
            ))
    opp_strips, level_strips = strips[:4], strips[4:]

    @pl.when(active)
    def _():
        ys3[0] = own[0:9, 6:8, :]
        ys3[1] = own[0:9, 16:18, :]
        packed = jnp.zeros((24, LANES), F32)
        lane4 = lanes_of(24) // 4
        for k in range(fields):
            packed = jnp.where(lane4 == k, pltpu.roll(own[k], 4 * k + 2, 1), packed)
        xs3[...] = packed

    for there, g in sides:
        @pl.when(there)
        def _(g=g):
            sent_all(wide_columns(g, (-1, 0, 1)))

    start_all(strips)

    with jax.named_scope("wait_parts"):
        for there, g in sides:
            @pl.when(there)
            def _(g=g):
                receive_all(part_rows(g))
                passed_parts(g).start()

    with jax.named_scope("wait_1"):
        end_round(1, (0, 1, 4, 5, 2, 3))
        if SPLIT:
            receive_all(stiff_rows)
            complete_rows()
    with jax.named_scope("step"):
        unpack_rows(1, fine, s, FACE_Y)
        unpack_rows(1, coarse, sc, FACE_Y)
        unpack_columns(1, (s, sc), FACE_X)
        for z in range(zf):
            step_block(u, s, fprev, dens, fout, z, 1, yf, xf, 0.5, stretch_of(z))
        for z in range(0, zc, zb):
            step_block(uc, sc, cprev, cdens, cout, z, zb, yc, xc, 0.25, 1.0)

    lane24 = lax.broadcasted_iota(jnp.int32, (24, LANES), 1)
    wide_row = lax.broadcasted_iota(jnp.int32, (24, 2 * LANES), 0)
    wide_lane = lax.broadcasted_iota(jnp.int32, (24, 2 * LANES), 1)

    def extend(k, field, centre, rims, row, edges):
        ext[k, 8:16, 0:LANES] = centre
        ext[k, 6:8, 0:LANES] = rims[0, row]
        ext[k, 16:18, 0:LANES] = rims[1, row]
        ext[k, :, LANES : 2 * LANES] = pltpu.roll(edges, LANES - (4 * field + 2), 1)

    def clamp(t):
        t = jnp.where(jnp.logical_and(wide_row == 7, gy == 0), pltpu.roll(t, 23, 0), t)
        t = jnp.where(jnp.logical_and(wide_row == 16, gy == n_y - 1), pltpu.roll(t, 1, 0), t)
        t = jnp.where(jnp.logical_and(wide_lane == 2 * LANES - 1, gx == 0), pltpu.roll(t, 2 * LANES - 1, 1), t)
        return jnp.where(jnp.logical_and(wide_lane == LANES, gx == n_x - 1), pltpu.roll(t, 1, 1), t)

    def along_y(t):
        return (0.75 * t + 0.25 * pltpu.roll(t, 1, 0), 0.75 * t + 0.25 * pltpu.roll(t, 23, 0))

    def along_x(t):
        return (0.75 * t + 0.25 * pltpu.roll(t, 1, 1), 0.75 * t + 0.25 * pltpu.roll(t, 2 * LANES - 1, 1))

    def extend_own(k, field, edges):
        ext[k, :, 0:LANES] = own[field]
        ext[k, :, LANES : 2 * LANES] = pltpu.roll(edges, LANES - (4 * field + 2), 1)

    with jax.named_scope("wait_level"):
        receive_all(level_strips)

    @pl.when(is_c)
    def _():
        edges = jnp.where(lane24 % 4 < 2, xr3[0], xr3[1])
        for k in range(3, 9):
            extend_own(k, k, edges)
        ikf_copy.wait_recv()

    @pl.when(is_f)
    def _():
        edges = jnp.where(lane24 % 4 < 2, xr3[0], xr3[1])
        for k in range(3):
            extend_own(9 + k, k, edges)
        for k in range(12):
            extend_own(12 + k, 6 + k, edges)

    with jax.named_scope("wait_opp"):
        receive_all(opp_strips)

    with jax.named_scope("wait_passed"):
        for there, g in sides:
            @pl.when(there)
            def _(g=g):
                passed_parts(coarse if g is fine else fine).wait_recv()

    def part_of(parts, side, field):
        edges = jnp.where(lanes_of(1) < LANES // 2, parts[side, 2, field], parts[side, 0, field])
        return jnp.concatenate([parts[side, 1, field], edges], 1)

    def add_part(k, parts, side, field, place):
        ext[k, place : place + 1] += part_of(parts, side, field)

    def set_part(k, parts, side, field, place):
        ext[k, place : place + 1] = part_of(parts, side, field)

    @pl.when(is_f)
    def _():
        k_copy.wait_recv()

    @pl.when(is_c)
    def _():
        edges = jnp.where(lane24 % 4 < 2, xo3[0], xo3[1])
        for c in range(3):
            extend(9 + c, 3 + c, own_opp[3 + c], yo3, 3 + c, edges)
            for side, place in enumerate((7, 16)):
                add_part(9 + c, npc_o, side, 3 + c, place)
                add_part(3 + c, npc_l, side, 3 + c, place)
            t1 = clamp(ext[6 + c] * (ext[3 + c] - 0.5 * ext[9 + c]))
            total = jnp.zeros((yc, LANES), F32)
            for py, part in enumerate(along_y(t1)):
                for px, full in enumerate(along_x(part[8:16])):
                    total += full[:, 0:LANES] * ikf_opp[c * 4 + py * 2 + px]
            cout[c, 0] = 0.5 * (cout[c, 0] + own_opp[c] + 0.25 * total)

    @pl.when(is_f)
    def _():
        edges = jnp.where(lane24 % 4 < 2, xo3[0], xo3[1])
        half = lane // 2
        for c in range(3):
            for k in (c, 3 + c, 6 + c):
                extend(k, k, own_opp[k], yo3, k, edges)
            for side, (place, after) in enumerate(((7, 6), (16, 17))):
                add_part(c, npf_o, side, c, place)
                add_part(c, npf_o, side, 6 + c, after)
                add_part(3 + c, npf_o, side, 3 + c, place)
                add_part(9 + c, npf_l, side, c, place)
                for k in range(4 * c, 4 * c + 4):
                    set_part(12 + k, npf_l, side, 6 + k, place)
            total = jnp.zeros((24, 2 * LANES), F32)
            for py, part in enumerate(along_y(clamp(ext[c]))):
                for px, full in enumerate(along_x(part)):
                    total += full * ext[12 + c * 4 + py * 2 + px]
            t2 = clamp(ext[6 + c] * (ext[3 + c] - 0.5 * (ext[9 + c] + 0.25 * total)))
            for py, part in enumerate(along_y(t2)):
                evens, odds = along_x(part[8:16])
                evens, odds = evens[:, 0:LANES], odds[:, 0:LANES]
                for t in range(2):
                    index = half + t * (LANES // 2)
                    tiles[t, pl.ds(py, yc, stride=2), :] = jnp.where(
                        lane % 2 == 0, pick(evens, index), pick(odds, index)
                    )
            for t in range(2):
                cols = slice(t * LANES, (t + 1) * LANES)
                fout[c, zf - 1, :, cols] = fout[c, zf - 2, :, cols] + tiles[t] / stiff[CH[c], zf - 1, :, cols]

    with jax.named_scope("drain"):
        for d in range(6):
            @pl.when(has[d])
            def _(d=d):
                for copy in round_copies(1, d):
                    copy.wait_send()
        for d in range(6):
            @pl.when(has[d])
            def _(d=d):
                for copy in round_copies(0, d):
                    copy.wait_send()
        if SPLIT:
            sent_all(stiff_rows)
        sent_all(strips)
        for there, g in sides:
            @pl.when(there)
            def _(g=g):
                sent_all(wide_rows(g))
                sent_all(part_rows(g))
                passed_parts(g).wait_send()

        @pl.when(is_f)
        def _():
            ikf_copy.wait_send()

        @pl.when(is_c)
        def _():
            k_copy.wait_send()


def write_out(fine, coarse, fine_out, coarse_out, sem):
    copies = [
        pltpu.make_async_copy(fine, fine_out, sem.at[0]),
        pltpu.make_async_copy(coarse, coarse_out, sem.at[1]),
    ]
    for copy in copies:
        copy.start()
    for copy in copies:
        copy.wait()


def per_device(counts, *args):
    fine, coarse = args[0].shape, args[5].shape
    _, zf, yf, xf = fine
    _, zc, yc, xc = coarse
    vmem = lambda *shape: pltpu.VMEM(shape, F32)
    anywhere = pl.BlockSpec(memory_space=pl.ANY)
    in_vmem = pl.BlockSpec(memory_space=pltpu.VMEM)
    made = pl.pallas_call(
        functools.partial(kernel, counts),
        out_shape=(pltpu.VMEM(fine, F32), pltpu.VMEM(coarse, F32)),
        in_specs=[anywhere] * 9,
        out_specs=(in_vmem, in_vmem),
        scratch_shapes=[
            vmem(3, zf + 2, yf + 2 * PAD, xf + LANES),
            vmem(3, zc + 2, yc + 2 * PAD, xc + LANES),
            vmem(6, zf + 2, yf + 2 * PAD, xf + LANES),
            vmem(6, zc + 2, yc + 2 * PAD, xc + LANES),
            vmem(3, zf, yf, xf), vmem(9, zf, yf, xf), vmem(zf, yf, xf), vmem(zf, yf, xf),
            vmem(3, zc, yc, xc), vmem(9, zc, yc, xc), vmem(zc, yc, xc),
            vmem(2, yf + yc, LANES), vmem(2, 2, yf + yc, LANES),
            vmem(2, 2, 3, zf + zc // 2, 1, xf), vmem(2, 2, 3, zf + zc // 2, 1, xf),
            vmem(9, 3, yf + 2 * PAD, xf + LANES), vmem(9, 3, yc + 2 * PAD, xc + LANES),
            vmem(2, 25, 1, xf), vmem(2, 25, 1, xf), vmem(2, 31, 1, xc), vmem(2, 31, 1, xc),
            vmem(yf, LANES), vmem(2, yf + 2 * PAD, LANES), vmem(yc, LANES), vmem(2, yc + 2 * PAD, LANES),
            vmem(2, 18, 1, LANES), vmem(2, 3, 18, 1, LANES), vmem(2, 3, 12, 1, LANES),
            vmem(2, 12, 1, LANES), vmem(2, 3, 12, 1, LANES), vmem(2, 3, 6, 1, LANES),
            vmem(2, 3, zf + zc // 2, 1, xf), vmem(2, 3, zf + zc // 2, 1, xf),
            vmem(2, yf, LANES), vmem(2, yf, LANES), vmem(18, 24, LANES), vmem(9, yc, LANES), vmem(12, yc, LANES),
            vmem(2, 9, 2, LANES), vmem(2, 9, 2, LANES),
            vmem(24, LANES), vmem(2, 24, LANES), vmem(2, 24, LANES),
            vmem(24, 24, 2 * LANES),
            pltpu.SemaphoreType.DMA((10,)),
            pltpu.SemaphoreType.DMA((37,)),
            pltpu.SemaphoreType.DMA((43,)),
        ],
        compiler_params=pltpu.CompilerParams(
            collective_id=0, has_side_effects=True, vmem_limit_bytes=56 * 1024 * 1024
        ),
        name="elastic_step",
    )(*args)
    made = [pltpu.with_memory_space_constraint(part, pltpu.VMEM) for part in made]
    return pl.pallas_call(
        write_out,
        out_shape=(jax.ShapeDtypeStruct(fine, F32), jax.ShapeDtypeStruct(coarse, F32)),
        in_specs=[in_vmem, in_vmem],
        out_specs=(anywhere, anywhere),
        scratch_shapes=[pltpu.SemaphoreType.DMA((2,))],
        name="write_out",
    )(*made)


def solution(mesh):
    counts = tuple(mesh.shape[name] for name in ("gz", "gy", "gx"))
    volume, field = P(None, "gz", "gy", "gx"), P("gz", "gy", "gx")
    return jax.shard_map(
        functools.partial(per_device, counts),
        mesh=mesh,
        in_specs=(volume, volume, volume, field, field, volume, volume, volume, field),
        out_specs=(volume, volume),
        check_vma=False,
    )
```

```python
import functools

import jax
import jax.numpy as jnp
from jax import lax
from jax.experimental import pallas as pl
from jax.experimental.pallas import tpu as pltpu
from jax.sharding import PartitionSpec as P

TIME_STEP = 0.2
ITERS = 3
F32 = jnp.float32
XX, XY, YY, XZ, YZ, ZZ = range(6)
FACE_X = (XX, XY, XZ)
FACE_Y = (XY, YY, YZ)
WIDE_Y = (1, 3, 5, 6, 8)
EDGE_Y = (5, 1, 3)
WIDE_X = (0, 4, 5, 6, 7)
CH = (4, 3, 2)
PAD = 8
LANES = 128


def lanes_of(rows):
    return lax.broadcasted_iota(jnp.int32, (rows, LANES), 1)


def pack_x(ref, comps, z_count, y_count, width):
    lane = lanes_of(y_count)
    packed = jnp.zeros((y_count, LANES), F32)
    k = 0
    for c in comps:
        for z in range(z_count):
            rows = pl.ds(PAD, y_count)
            tile = ref[c, z + 1, rows, 0:LANES]
            if width > LANES:
                last = ref[c, z + 1, rows, width - LANES : width]
                tile = jnp.where(lane >= LANES // 2, last, tile)
            packed = jnp.where(lane // 2 == k, pltpu.roll(tile, 2 * k + 1, 1), packed)
            k += 1
    return packed


def unpack_x(ref, comps, z_count, y_count, width, from_left, from_right):
    lane = lanes_of(y_count)
    both = jnp.where(lane % 2 == 0, from_left, from_right)
    k = 0
    for c in comps:
        for z in range(z_count):
            ref[c, z + 1, pl.ds(PAD, y_count), width : width + LANES] = pltpu.roll(
                both, LANES - 1 - 2 * k, 1
            )
            k += 1


def diff_x(ref, c, z0, zn, y_count, width, scale):
    v = ref[c, z0 : z0 + zn, PAD : PAD + y_count, :]
    span = width + LANES
    return (pltpu.roll(v, span - 1, 2) - pltpu.roll(v, 1, 2))[:, :, :width] * scale


def diff_y(ref, c, z0, zn, y_count, width, scale):
    after = ref[c, z0 : z0 + zn, PAD + 1 : PAD + 1 + y_count, 0:width]
    before = ref[c, z0 : z0 + zn, PAD - 1 : PAD - 1 + y_count, 0:width]
    return (after - before) * scale


def diff_z(ref, c, z0, zn, y_count, width, scale):
    after = ref[c, z0 + 1 : z0 + 1 + zn, PAD : PAD + y_count, 0:width]
    before = ref[c, z0 - 1 : z0 - 1 + zn, PAD : PAD + y_count, 0:width]
    return (after - before) * scale


def stress_block(u, stiff, s, z, zn, y_count, width, inv, stretch):
    args = (z + 1, zn, y_count, width, inv)
    own = (slice(z + 1, z + 1 + zn), slice(PAD, PAD + y_count), slice(0, width))
    c = [stiff[i, z : z + zn] for i in range(9)]
    nx = diff_x(u, 0, *args)
    ny = diff_y(u, 1, *args)
    nz = diff_z(u, 2, *args) * stretch
    s[(XX,) + own] = c[0] * nx + c[6] * ny + c[7] * nz
    s[(YY,) + own] = c[6] * nx + c[1] * ny + c[8] * nz
    s[(ZZ,) + own] = c[7] * nx + c[8] * ny + c[2] * nz
    s[(YZ,) + own] = c[3] * (diff_z(u, 1, *args) * stretch + diff_y(u, 2, *args))
    s[(XZ,) + own] = c[4] * (diff_z(u, 0, *args) * stretch + diff_x(u, 2, *args))
    s[(XY,) + own] = c[5] * (diff_y(u, 0, *args) + diff_x(u, 1, *args))


def step_block(u, s, prev, dens, out, z, zn, y_count, width, inv, stretch):
    args = (z + 1, zn, y_count, width, inv)
    gain = (TIME_STEP * TIME_STEP) / dens[z : z + zn]
    for c, (sx, sy, sz) in enumerate(((XX, XY, XZ), (XY, YY, YZ), (XZ, YZ, ZZ))):
        total = diff_x(s, sx, *args) + diff_y(s, sy, *args) + diff_z(s, sz, *args) * stretch
        now = u[c, z + 1 : z + 1 + zn, PAD : PAD + y_count, 0:width]
        out[c, z : z + zn] = (2.0 * now - prev[c, z : z + zn]) + gain * total


def stress_ext(u, stiff, s, layer, slab, y_count, width, inv):
    z, first, rows, span = layer + 1, PAD - 1, y_count + 2, width + LANES

    def at(c, dz, dr):
        return u[c, z + dz, first + dr : first + dr + rows, :]

    def dx(c):
        v = at(c, 0, 0)
        return (pltpu.roll(v, span - 1, 1) - pltpu.roll(v, 1, 1)) * inv

    def dy(c):
        return (at(c, 0, 1) - at(c, 0, -1)) * inv

    def dz(c):
        return (at(c, 1, 0) - at(c, -1, 0)) * inv

    c = [stiff[i, slab, first : first + rows, :] for i in range(9)]
    nx, ny, nz = dx(0), dy(1), dz(2)
    values = {
        XX: c[0] * nx + c[6] * ny + c[7] * nz,
        YY: c[6] * nx + c[1] * ny + c[8] * nz,
        ZZ: c[7] * nx + c[8] * ny + c[2] * nz,
        YZ: c[3] * (dz(1) + dy(2)),
        XZ: c[4] * (dz(0) + dx(2)),
        XY: c[5] * (dy(0) + dx(1)),
    }
    for component, value in values.items():
        s[component, z, first : first + rows, :] = value


def pick(x, index):
    return jnp.take_along_axis(x, index, axis=1, mode="promise_in_bounds")


class Grid:
    def __init__(self, **fields):
        self.__dict__.update(fields)
        self.own = (slice(1, self.z + 1), slice(PAD, PAD + self.y), slice(0, self.x))


def kernel(
    counts,
    fn, fp, st, me, de, cn, cp, cst, cde,
    fout, cout,
    u, uc, s, sc, fprev, stiff, metric, dens, cprev, cstiff, cdens,
    xs, xr, ys, yr,
    fwide, cwide, yef_s, yef_r, yec_s, yec_r, xef_s, xef_r, xec_s, xec_r,
    npf_s, npf_l, npf_o, npc_s, npc_l, npc_o, pe_s, pe_l, pe_o, cs, xd_s, xd_r,
    tiles, sums, own, own_opp, ikf_opp, ys3, yo3, xs3, xr3, xo3, ext,
    load_sem, send_sem, recv_sem,
):
    n_z, n_y, n_x = counts
    zf, yf, xf = me.shape
    zc, yc, xc = cde.shape
    fine = Grid(
        z=zf, y=yf, x=xf, u=u, s=s, wide=fwide, source=st, stiff=stiff, third=0, prev=fprev, dens=dens, out=fout, inv=0.5,
        slabs=(1, 2), near=zf - 3, np_s=npf_s, np_l=npf_l, np_o=npf_o, ye_s=yef_s, ye_r=yef_r, xe_s=xef_s, xe_r=xef_r,
    )
    coarse = Grid(
        z=zc, y=yc, x=xc, u=uc, s=sc, wide=cwide, source=cst, stiff=cstiff, third=2, prev=cprev, dens=cdens, out=cout, inv=0.25,
        slabs=(0, 1), near=0, np_s=npc_s, np_l=npc_l, np_o=npc_o, ye_s=yec_s, ye_r=yec_r, xe_s=xec_s, xe_r=xec_r,
    )
    gz, gy, gx = lax.axis_index("gz"), lax.axis_index("gy"), lax.axis_index("gx")
    opp = n_z - 1 - gz
    is_c, is_f = gz == 0, gz == n_z - 1
    active = jnp.logical_or(is_c, is_f)
    has_y = {-1: gy > 0, 0: gy >= 0, 1: gy < n_y - 1}
    has_x = {-1: gx > 0, 0: gx >= 0, 1: gx < n_x - 1}
    has = (gz > 0, gz < n_z - 1, has_y[-1], has_y[1], has_x[-1], has_x[1])
    near = (
        (gz - 1, gy, gx), (gz + 1, gy, gx),
        (gz, gy - 1, gx), (gz, gy + 1, gx),
        (gz, gy, gx - 1), (gz, gy, gx + 1),
    )

    barrier = pltpu.get_barrier_semaphore()
    expected = jnp.int32(0)

    def greet(there, device):
        @pl.when(there)
        def _():
            pl.semaphore_signal(barrier, 1, device_id=device, device_id_type=pl.DeviceIdType.MESH)

        return there.astype(jnp.int32)

    for d in (2, 3, 4, 5, 0, 1):
        expected += greet(has[d], near[d])
    for a in (-1, 1):
        for b in (-1, 1):
            there = jnp.logical_and(active, jnp.logical_and(has_y[a], has_x[b]))
            expected += greet(there, (gz, gy + a, gx + b))
    expected += greet(active, (opp, gy, gx))

    loads = [
        pltpu.make_async_copy(src, dst, load_sem.at[i])
        for i, (src, dst) in enumerate((
            (fn, u.at[(slice(None),) + fine.own]),
            (cn, uc.at[(slice(None),) + coarse.own]),
            (de, dens), (cde, cdens), (fp, fprev), (cp, cprev),
            (st, stiff), (cst, cstiff), (me, metric),
        ))
    ]

    def wide_load(g):
        return pltpu.make_async_copy(
            g.source.at[:, g.near : g.near + 3], g.wide.at[(slice(None), slice(None)) + g.own[1:]], load_sem.at[9]
        )

    sides = ((is_f, fine), (is_c, coarse))
    for load in loads[:2]:
        load.start()
    for there, g in sides:
        @pl.when(there)
        def _(g=g):
            wide_load(g).start()
    for load in loads[2:4]:
        load.start()

    def clear(part):
        part[...] = jnp.zeros(part.shape, F32)

    for there, g in sides:
        @pl.when(there)
        def _(g=g):
            for rows in (pl.ds(0, PAD), pl.ds(PAD + g.y, PAD)):
                clear(g.u.at[:, g.near + 1 : g.near + 4, rows])
                clear(g.wide.at[:, :, rows])

    for g in (fine, coarse):
        for row in (PAD - 1, PAD + g.y):
            clear(g.u.at[:, 1 : g.z + 1, row : row + 1, 0 : g.x])
    for d in range(6):
        @pl.when(jnp.logical_not(has[d]))
        def _(d=d):
            side = d % 2
            if d < 2:
                for g in (fine, coarse):
                    plane = 0 if side == 0 else g.z + 1
                    clear(g.u.at[:, plane])
                    clear(g.s.at[3:6, plane, g.own[1], g.own[2]])
            elif d < 4:
                for r in range(2):
                    clear(yr.at[r, side])
                for g in (fine, coarse):
                    clear(g.ye_r.at[side])
                for b in range(2):
                    clear(xd_r.at[b, side])
            else:
                for r in range(2):
                    clear(xr.at[r, side])
                for g in (fine, coarse):
                    clear(g.xe_r.at[side])
                for b in range(2):
                    clear(xd_r.at[side, b])

    def rdma(src, dst, out, into, device):
        return pltpu.make_async_remote_copy(
            src_ref=src, dst_ref=dst, send_sem=send_sem.at[out], recv_sem=recv_sem.at[into],
            device_id=device, device_id_type=pl.DeviceIdType.MESH,
        )

    def round_copies(r, d):
        side = d % 2
        arrival = 1 - side
        if d < 2:
            comps = (slice(0, 3), slice(3, 6))[r]
            made = []
            for i, g in enumerate((fine, coarse)):
                ref = (g.u, g.s)[r]
                sent, landed = (1, g.z + 1) if side == 0 else (g.z, 0)
                made.append(rdma(
                    ref.at[comps, sent, g.own[1], g.own[2]], ref.at[comps, landed, g.own[1], g.own[2]],
                    (0, 31)[r] + 2 * d + i, 8 * r + 2 * d + i, near[d],
                ))
            return made
        if d < 4:
            return [rdma(ys.at[r, side], yr.at[r, arrival], (d + 2, d + 19)[r], 8 * r + d + 2, near[d])]
        return [rdma(xs.at[r], xr.at[r, arrival], (d + 2, d + 31)[r], 8 * r + d + 2, near[d])]

    def start_round(r, directions):
        for d in directions:
            @pl.when(has[d])
            def _(d=d):
                for copy in round_copies(r, d):
                    copy.start()

    def end_round(r, directions):
        for d in directions:
            @pl.when(has[d ^ 1])
            def _(d=d):
                for copy in round_copies(r, d):
                    copy.wait_recv()

    def row_parts(g, ref, c, row):
        if g is fine:
            return [(ref.at[c, 1 : zf + 1, row : row + 1, 0:xf], (c, slice(0, zf), slice(None), slice(0, xf)))]
        half = zc // 2
        return [
            (
                ref.at[c, 1 + i * half : 1 + (i + 1) * half, row : row + 1, 0:xc],
                (c, slice(zf, zf + half), slice(None), slice(i * xc, (i + 1) * xc)),
            )
            for i in range(2)
        ]

    def pack_rows(r, refs, face_y):
        for g, ref in ((fine, refs[0]), (coarse, refs[1])):
            for side, row in enumerate((PAD, PAD + g.y - 1)):
                for i, c in enumerate(face_y):
                    for part, place in row_parts(g, ref, c, row):
                        ys[(r, side, i) + place[1:]] = part[...]

    def pack_columns(r, refs, face_x):
        xs[r, 0:yf] = pack_x(refs[0], face_x, zf, yf, xf)
        xs[r, yf : yf + yc] = pack_x(refs[1], face_x, zc, yc, xc)

    def pack_stiff_rows():
        half = zc // 2
        for i, c in enumerate(EDGE_Y):
            for side in range(2):
                row = (0, yf - 1)[side]
                cs[side, i, 0:zf] = stiff[c, :, row : row + 1, :]
                row = (0, yc - 1)[side]
                for j in range(2):
                    cs[side, i, zf : zf + half, :, j * xc : (j + 1) * xc] = cstiff[
                        c, j * half : (j + 1) * half, row : row + 1, :
                    ]

    def complete_rows():
        for side, sign in enumerate((-1.0, 1.0)):
            for g, part in ((fine, slice(0, zf)), (coarse, slice(zf, zf + zc // 2))):
                ys[1, side, :, part] = ys[1, side, :, part] + cs[side, :, part] * yr[0, side, :, part] * (sign * g.inv)

    def unpack_rows(r, g, ref, face_y):
        for side, row in enumerate((PAD - 1, PAD + g.y)):
            for i, c in enumerate(face_y):
                for part, place in row_parts(g, ref, c, row):
                    part[...] = yr[(r, side, i) + place[1:]]

    def unpack_columns(r, refs, face_x):
        unpack_x(refs[0], face_x, zf, yf, xf, xr[r, 0, 0:yf], xr[r, 1, 0:yf])
        unpack_x(refs[1], face_x, zc, yc, xc, xr[r, 0, yf : yf + yc], xr[r, 1, yf : yf + yc])

    def pack_wide_rows(g):
        first = g.near + g.slabs[0]
        for side, (edge, second) in enumerate(((PAD, PAD + 1), (PAD + g.y - 1, PAD + g.y - 2))):
            out = g.ye_s.at[side]
            for c in range(3):
                out[2 * c : 2 * c + 2] = g.u[c, first + 1 : first + 3, second : second + 1, 0 : g.x]
            for i, c in enumerate(WIDE_Y):
                out[6 + 3 * i : 9 + 3 * i] = g.wide[c, :, edge : edge + 1, 0 : g.x]
            for i, row in enumerate((edge, second)):
                out[21 + 2 * i : 23 + 2 * i] = g.dens[first : first + 2, row - PAD : row - PAD + 1, :]
                if g is coarse:
                    for c in range(3):
                        out[25 + 3 * i + c] = g.wide[CH[c], 0, row : row + 1, 0 : g.x]

    def pack_wide_columns(g):
        lane = lanes_of(g.y)
        packed = jnp.zeros((g.y, LANES), F32)
        for k, (ref, index) in enumerate(wide_blocks(g)):
            tile = ref[index + (g.own[1], slice(0, LANES))]
            if g.x > LANES:
                last = ref[index + (g.own[1], slice(g.x - LANES, g.x))]
                tile = jnp.where(lane >= LANES // 2, last, tile)
            packed = jnp.where(lane // 4 == k, pltpu.roll(tile, 4 * k + 2, 1), packed)
        g.xe_s[...] = packed
        xd_s[0] = packed[0:1]
        xd_s[1] = packed[g.y - 1 : g.y]

    def wide_blocks(g):
        blocks = [(g.u, (c, g.near + l + 1)) for c in range(3) for l in range(3)]
        return blocks + [(g.wide, (c, l)) for c in WIDE_X for l in g.slabs]

    def wide_rows(g):
        return [
            (has_y[a], has_y[-a], rdma(g.ye_s.at[i], g.ye_r.at[1 - i], 11 + i, 19 + i, (gz, gy + a, gx)))
            for i, a in enumerate((-1, 1))
        ]

    def wide_columns(g, ups):
        made = []
        for i, b in enumerate((-1, 1)):
            for a in ups:
                if a == 0:
                    src, dst = g.xe_s, g.xe_r.at[1 - i]
                else:
                    src, dst = xd_s.at[(a + 1) // 2], xd_r.at[1 - i, (1 - a) // 2]
                made.append((
                    jnp.logical_and(has_y[a], has_x[b]), jnp.logical_and(has_y[-a], has_x[-b]),
                    rdma(src, dst, 13 + i * 3 + (a + 1), 21 + i * 3 + (a + 1), (gz, gy + a, gx + b)),
                ))
        return made

    def part_rows(g):
        made = []
        for i, a in enumerate((-1, 1)):
            for b in (-1, 0, 1):
                k = 3 * i + b + 1
                if b == 0:
                    src, dst = g.np_s.at[i], g.np_l.at[1 - i]
                else:
                    src, dst = pe_s.at[i], pe_l.at[1 - i, (1 - b) // 2]
                made.append((
                    jnp.logical_and(has_y[a], has_x[b]), jnp.logical_and(has_y[-a], has_x[-b]),
                    rdma(src, dst, 25 + k, 35 + k, (gz, gy + a, gx + b)),
                ))
        return made

    def pack_parts(g, count):
        lane1 = lanes_of(1)
        for side in range(2):
            packed = jnp.zeros((1, LANES), F32)
            for k in range(count):
                packed = jnp.where(lane1 // 4 == k, pltpu.roll(g.np_s[side, k], 4 * k + 2, 1), packed)
            pe_s[side] = packed

    def passed_parts(g):
        source, target = (npf_l.at[:, 0:6], npc_o) if g is fine else (npc_l, npf_o)
        return [(active, active, rdma(source, target, 9, 17, (opp, gy, gx))), (active, active, rdma(pe_l, pe_o, 10, 18, (opp, gy, gx)))]

    def squeeze_rows(row_of):
        for side in range(2):
            for c in range(3):
                both = row_of(side, c)
                for i in range(2):
                    k = side * 6 + 3 * i + c
                    for t in range(2):
                        sums[t, k : k + 1] = both[i, :, t * LANES : (t + 1) * LANES]
        pairs = [sums[t] + pltpu.roll(sums[t], LANES - 1, 1) for t in range(2)]
        lane16 = lanes_of(16)
        index = (2 * lane16) % LANES
        return jnp.where(lane16 < LANES // 2, pick(pairs[0], index), pick(pairs[1], index)) * 0.25

    def unpack_wide_rows(g):
        first = g.near + g.slabs[0]
        for side, (edge, second) in enumerate(((PAD - 1, PAD - 2), (PAD + g.y, PAD + g.y + 1))):
            landed = g.ye_r.at[side]
            for c in range(3):
                g.u[c, first + 1 : first + 3, second : second + 1, 0 : g.x] = landed[2 * c : 2 * c + 2]
            for i, c in enumerate(WIDE_Y):
                g.wide[c, :, edge : edge + 1, 0 : g.x] = landed[6 + 3 * i : 9 + 3 * i]

    def unpack_wide_columns(g, corners):
        own_rows = (slice(PAD, PAD + g.y), jnp.where(lanes_of(g.y) % 4 < 2, g.xe_r[0], g.xe_r[1]))
        rows = [own_rows]
        if corners:
            for side, row in enumerate((PAD - 1, PAD + g.y)):
                rows.append((slice(row, row + 1), jnp.where(lanes_of(1) % 4 < 2, xd_r[0, side], xd_r[1, side])))
        for k, (ref, index) in enumerate(wide_blocks(g)):
            for where, both in rows:
                ref[index + (where, slice(g.x, g.x + LANES))] = pltpu.roll(both, LANES - (4 * k + 2), 1)

    def interface_step(g):
        stress_block(g.u, g.stiff, g.s, g.near + g.third, 1, g.y, g.x, g.inv, 1.0)
        for l in g.slabs:
            stress_ext(g.u, g.wide, g.s, g.near + l, l, g.y, g.x, g.inv)
        for l in g.slabs:
            step_block(g.u, g.s, g.prev, g.dens, g.out, g.near + l, 1, g.y, g.x, g.inv, 1.0)

    def beyond_edges(g):
        first = g.near + g.slabs[0]
        span = g.x + LANES
        result = []
        for side, (sign, edge, adjacent) in enumerate(((1.0, PAD, PAD - 1), (-1.0, PAD + g.y - 1, PAD + g.y))):
            scale = sign * g.inv
            d = [g.u[c, g.near + 1 : g.near + 4, edge : edge + 1, :] * scale for c in range(3)]
            w = {c: g.wide[c, :, adjacent : adjacent + 1, :] for c in WIDE_Y}
            s_xx, s_yy, s_zz, s_yz, s_xy = w[6] * d[1], w[1] * d[1], w[8] * d[1], w[3] * d[2], w[5] * d[0]

            def two(v):
                return v[g.slabs[0] : g.slabs[0] + 2, :, 0 : g.x]

            def along_x_of(v):
                v = v[g.slabs[0] : g.slabs[0] + 2]
                return (pltpu.roll(v, span - 1, 2) - pltpu.roll(v, 1, 2))[:, :, 0 : g.x] * g.inv

            def along_z_of(v):
                v = v[:, :, 0 : g.x]
                parts = []
                for l in g.slabs:
                    parts.append((v[l + 1 : l + 2] if l < 2 else 0.0) - (v[l - 1 : l] if l > 0 else 0.0))
                return jnp.concatenate(parts, 0) * g.inv

            def edge_stress(component):
                return g.s[component, first + 1 : first + 3, edge : edge + 1, 0 : g.x] * scale

            totals = (
                (
                    along_x_of(s_xx) + edge_stress(XY),
                    along_x_of(s_xy) + edge_stress(YY) + along_z_of(s_yz),
                    edge_stress(YZ) + along_z_of(s_zz),
                ),
                (two(s_xy) * scale, two(s_yy) * scale, two(s_yz) * scale),
            )
            rows = []
            for i in range(2):
                gain = (TIME_STEP * TIME_STEP) / g.ye_r[side, 21 + 2 * i : 23 + 2 * i]
                rows.append([gain * totals[i][c] for c in range(3)])
            result.append(rows)
        return result

    def start_all(copies):
        for there, _, copy in copies:
            @pl.when(there)
            def _(copy=copy):
                copy.start()

    def receive_all(copies):
        for _, comes, copy in copies:
            @pl.when(comes)
            def _(copy=copy):
                copy.wait_recv()

    def sent_all(copies):
        for there, _, copy in copies:
            @pl.when(there)
            def _(copy=copy):
                copy.wait_send()

    with jax.named_scope("load_pack"):
        loads[0].wait()
        loads[1].wait()
        for load in loads[4:]:
            load.start()
        for there, g in sides:
            @pl.when(there)
            def _(g=g):
                wide_load(g).wait()
                pack_wide_columns(g)
        pack_rows(0, (u, uc), (0, 1, 2))
        loads[2].wait()
        loads[3].wait()
        for there, g in sides:
            @pl.when(there)
            def _(g=g):
                pack_wide_rows(g)
        pack_columns(0, (u, uc), (0, 1, 2))
    with jax.named_scope("barrier"):
        pl.semaphore_wait(barrier, expected)
    with jax.named_scope("send_0"):
        for there, g in sides:
            @pl.when(there)
            def _(g=g):
                start_all(wide_columns(g, (0,)))
        start_round(0, (2, 3))
        for there, g in sides:
            @pl.when(there)
            def _(g=g):
                start_all(wide_rows(g))
                start_all(wide_columns(g, (-1, 1)))
        start_round(0, (4, 5, 0, 1))
        for load in loads[4:]:
            load.wait()
        pack_stiff_rows()

    lane = lanes_of(yc)
    even = (2 * lane) % LANES

    def squeeze(left, right, odd):
        return jnp.where(lane < LANES // 2, pick(left, even + odd), pick(right, even + odd))

    ikf_copy = rdma(own.at[6:18, 0:8], ikf_opp, 8, 16, (opp, gy, gx))
    @pl.when(is_f)
    def _():
        for c in range(3):
            inverse = 1.0 / stiff[CH[c], zf - 1]
            for t in range(2):
                tiles[c, t] = inverse[:, t * LANES : (t + 1) * LANES]
            for py in range(2):
                rows = pl.ds(py, yc, stride=2)
                left, right = tiles[c, 0, rows, :], tiles[c, 1, rows, :]
                for px in range(2):
                    own[6 + c * 4 + py * 2 + px, 0:8] = squeeze(left, right, px)

    k_copy = rdma(own.at[6:9, 0:8], own_opp.at[6:9], 8, 16, (opp, gy, gx))

    @pl.when(is_c)
    def _():
        for c in range(3):
            own[6 + c, 0:8] = cstiff[CH[c], 0] * 0.25

    def pack_own(first, last):
        lane4 = lanes_of(16) // 4
        packed = xs3[...]
        for k in range(first, last):
            packed = jnp.where(lane4 == k, pltpu.roll(own[k], 4 * k + 2, 1), packed)
        xs3[...] = packed

    @pl.when(is_f)
    def _():
        pack_own(6, 18)

    with jax.named_scope("wait_part"):
        for there, g in sides:
            @pl.when(there)
            def _(g=g):
                receive_all(wide_columns(g, (0,)))

    for there, g in sides:
        @pl.when(there)
        def _(g=g):
            unpack_wide_columns(g, False)
            interface_step(g)

    @pl.when(is_f)
    def _():
        first = fine.near + fine.slabs[0]

        def two_rows(side, c):
            row = (0, yf - 2)[side]
            return fout[c, first : first + 2, row : row + 1, :] + fout[c, first : first + 2, row + 1 : row + 2, :]

        squeezed = squeeze_rows(two_rows)
        for side in range(2):
            for k in range(6):
                npf_s[side, k] = squeezed[side * 6 + k : side * 6 + k + 1]
            npf_s[side, 6:18] = own[6:18, (0, yc - 1)[side] : (1, yc)[side], :]
        pack_parts(fine, 18)
        start_all(part_rows(fine))
        ikf_copy.start()

    @pl.when(is_c)
    def _():
        for side in range(2):
            for i in range(2):
                row = (i, yc - 1 - i)[side]
                for c in range(3):
                    start, below = cout[c, 0, row : row + 1, :], cout[c, 1, row : row + 1, :]
                    npc_s[side, 6 * i + c] = own[6 + c, row : row + 1] * (below - start)
                    npc_s[side, 6 * i + 3 + c] = below - 0.5 * start
        pack_parts(coarse, 12)
        start_all(part_rows(coarse))
        k_copy.start()

    def stretch_of(z):
        return jnp.where(gz * zf + z < n_z * zf // 2, metric[z : z + 1], 1.0)

    zb = min(4, zc)

    def stress_all():
        for z in range(zf):
            stress_block(u, stiff, s, z, 1, yf, xf, 0.5, stretch_of(z))
        for z in range(0, zc, zb):
            stress_block(uc, cstiff, sc, z, zb, yc, xc, 0.25, 1.0)

    with jax.named_scope("wait_near"):
        end_round(0, (4, 5, 0, 1))
    with jax.named_scope("part_stress"):
        unpack_columns(0, (u, uc), (0, 1, 2))
        stress_all()
        pack_rows(1, (s, sc), FACE_Y)

    with jax.named_scope("wait_rows"):
        end_round(0, (2, 3))
        complete_rows()
        start_round(1, (2, 3))
        unpack_rows(0, fine, u, (0, 1, 2))
        unpack_rows(0, coarse, uc, (0, 1, 2))

    with jax.named_scope("stress"):
        stress_all()
        pack_columns(1, (s, sc), FACE_X)
        start_round(1, (4, 5, 0, 1))

    with jax.named_scope("wait_wide"):
        for there, g in sides:
            @pl.when(there)
            def _(g=g):
                receive_all(wide_rows(g))
                receive_all(wide_columns(g, (-1, 1)))

    for there, g in sides:
        @pl.when(there)
        def _(g=g):
            unpack_wide_rows(g)
            unpack_wide_columns(g, True)
            interface_step(g)

    @pl.when(is_c)
    def _():
        for c in range(3):
            start, below = cout[c, 0], cout[c, 1]
            own[c, 0:8] = own[6 + c, 0:8] * (below - start)
            own[3 + c, 0:8] = below - 0.5 * start

    @pl.when(is_f)
    def _():
        for c in range(3):
            for i, z in enumerate((zf - 2, zf - 1)):
                plane = fout[c, z]
                pairs = []
                k = 3 * i + c
                for t in range(2):
                    tiles[k, t] = plane[:, t * LANES : (t + 1) * LANES]
                    pair = tiles[k, t, pl.ds(0, yc, stride=2), :] + tiles[k, t, pl.ds(1, yc, stride=2), :]
                    pairs.append(pair + pltpu.roll(pair, LANES - 1, 1))
                own[3 * i + c, 0:8] = squeeze(pairs[0], pairs[1], 0) * 0.25

    @pl.when(is_c)
    def _():
        for side, rows in enumerate(beyond_edges(coarse)):
            for i in range(2):
                place = (15 - i) if side == 0 else (8 + i)
                for c in range(3):
                    start, below = rows[i][c][0], rows[i][c][1]
                    k = yec_r[side, 25 + 3 * i + c] * 0.25
                    own[c, place : place + 1] = k * (below - start)
                    own[3 + c, place : place + 1] = below - 0.5 * start
                    own[6 + c, place : place + 1] = k

    @pl.when(is_f)
    def _():
        beyond = beyond_edges(fine)
        squeezed = squeeze_rows(lambda side, c: beyond[side][0][c] + beyond[side][1][c])
        for side, place in enumerate((15, 8)):
            for k in range(6):
                own[k, place : place + 1] = squeezed[side * 6 + k : side * 6 + k + 1]

    strips = [
        (active, active, rdma(own.at[0:6, 0:8], own_opp.at[0:6], 13, 29, (opp, gy, gx))),
        (is_f, is_c, rdma(ys3.at[:, 3:6], yo3.at[:, 3:6], 14, 30, (opp, gy, gx))),
        (is_c, is_f, rdma(ys3, yo3, 14, 30, (opp, gy, gx))),
    ]
    for level, tile_to, out, into in ((opp, xo3, 15, 33), (gz, xr3, 17, 31)):
        for i, b in enumerate((-1, 1)):
            strips.append((
                jnp.logical_and(active, has_x[b]), jnp.logical_and(active, has_x[-b]),
                rdma(xs3, tile_to.at[1 - i], out + i, into + i, (level, gy, gx + b)),
            ))
    opp_strips, level_strips = strips[:5], strips[5:]

    for there, first, last in ((is_f, 0, 6), (is_c, 0, 9)):
        @pl.when(there)
        def _(first=first, last=last):
            pack_own(first, last)

    @pl.when(active)
    def _():
        ys3[0] = own[0:9, 14:16, :]
        ys3[1] = own[0:9, 8:10, :]

    for there, g in sides:
        @pl.when(there)
        def _(g=g):
            sent_all(wide_columns(g, (-1, 0, 1)))

    start_all(strips)

    with jax.named_scope("wait_parts"):
        for there, g in sides:
            @pl.when(there)
            def _(g=g):
                receive_all(part_rows(g))
                start_all(passed_parts(g))

    with jax.named_scope("wait_1"):
        end_round(1, (4, 5, 0, 1))
    with jax.named_scope("step"):
        for g in (fine, coarse):
            for row in (PAD - 1, PAD + g.y):
                for c in FACE_Y:
                    clear(g.s.at[c, 1 : g.z + 1, row : row + 1, 0 : g.x])
        unpack_columns(1, (s, sc), FACE_X)
        for z in range(zf):
            step_block(u, s, fprev, dens, fout, z, 1, yf, xf, 0.5, stretch_of(z))
        for z in range(0, zc, zb):
            step_block(uc, sc, cprev, cdens, cout, z, zb, yc, xc, 0.25, 1.0)
    with jax.named_scope("wait_rows_1"):
        end_round(1, (2, 3))
        half = zc // 2
        for side, sign in enumerate((-1.0, 1.0)):
            row = (0, yf - 1)[side]
            gain = (sign * 0.5 * TIME_STEP * TIME_STEP) / dens[:, row : row + 1, :]
            for c in range(3):
                fout[c, :, row : row + 1, :] += gain * yr[1, side, c, 0:zf]
            row = (0, yc - 1)[side]
            gain = (sign * 0.25 * TIME_STEP * TIME_STEP) / cdens[:, row : row + 1, :]
            for j in range(2):
                part, cols = slice(j * half, (j + 1) * half), slice(j * xc, (j + 1) * xc)
                for c in range(3):
                    cout[c, part, row : row + 1, :] += gain[part] * yr[1, side, c, zf : zf + half, :, cols]

    lane16 = lanes_of(16)
    wide_row = lax.broadcasted_iota(jnp.int32, (16, 2 * LANES), 0)
    wide_lane = lax.broadcasted_iota(jnp.int32, (16, 2 * LANES), 1)

    def extend(k, field, centre, rims, row, edges):
        ext[k, 0:8, 0:LANES] = centre
        ext[k, 14:16, 0:LANES] = rims[0, row]
        ext[k, 8:10, 0:LANES] = rims[1, row]
        ext[k, :, LANES : 2 * LANES] = pltpu.roll(edges, LANES - (4 * field + 2), 1)

    def clamp(t):
        t = jnp.where(jnp.logical_and(wide_row == 15, gy == 0), pltpu.roll(t, 15, 0), t)
        t = jnp.where(jnp.logical_and(wide_row == 8, gy == n_y - 1), pltpu.roll(t, 1, 0), t)
        t = jnp.where(jnp.logical_and(wide_lane == 2 * LANES - 1, gx == 0), pltpu.roll(t, 2 * LANES - 1, 1), t)
        return jnp.where(jnp.logical_and(wide_lane == LANES, gx == n_x - 1), pltpu.roll(t, 1, 1), t)

    def along_y(t):
        return (0.75 * t + 0.25 * pltpu.roll(t, 1, 0), 0.75 * t + 0.25 * pltpu.roll(t, 15, 0))

    def along_x(t):
        return (0.75 * t + 0.25 * pltpu.roll(t, 1, 1), 0.75 * t + 0.25 * pltpu.roll(t, 2 * LANES - 1, 1))

    def extend_own(k, field, edges):
        ext[k, :, 0:LANES] = own[field]
        ext[k, :, LANES : 2 * LANES] = pltpu.roll(edges, LANES - (4 * field + 2), 1)

    with jax.named_scope("wait_level"):
        receive_all(level_strips)

    @pl.when(is_c)
    def _():
        edges = jnp.where(lane16 % 4 < 2, xr3[0], xr3[1])
        for k in range(3, 9):
            extend_own(k, k, edges)
        ikf_copy.wait_recv()

    @pl.when(is_f)
    def _():
        edges = jnp.where(lane16 % 4 < 2, xr3[0], xr3[1])
        for k in range(3):
            extend_own(9 + k, k, edges)
        for k in range(12):
            extend_own(12 + k, 6 + k, edges)

    with jax.named_scope("wait_opp"):
        receive_all(opp_strips)

    with jax.named_scope("wait_passed"):
        for there, g in sides:
            @pl.when(there)
            def _(g=g):
                receive_all(passed_parts(coarse if g is fine else fine))

    def part_of(parts, rims, side, field):
        edges = jnp.where(lanes_of(1) % 4 < 2, rims[side, 0], rims[side, 1])
        return jnp.concatenate([parts[side, field], pltpu.roll(edges, LANES - (4 * field + 2), 1)], 1)

    def add_part(k, parts, rims, side, field, place):
        ext[k, place : place + 1] += part_of(parts, rims, side, field)

    def set_part(k, parts, rims, side, field, place):
        ext[k, place : place + 1] = part_of(parts, rims, side, field)

    @pl.when(is_f)
    def _():
        k_copy.wait_recv()

    @pl.when(is_c)
    def _():
        edges = jnp.where(lane16 % 4 < 2, xo3[0], xo3[1])
        for c in range(3):
            extend(9 + c, 3 + c, own_opp[3 + c], yo3, 3 + c, edges)
            for side, place in enumerate((15, 8)):
                add_part(9 + c, npc_o, pe_o, side, 3 + c, place)
                add_part(3 + c, npc_l, pe_l, side, 3 + c, place)
            t1 = clamp(ext[6 + c] * (ext[3 + c] - 0.5 * ext[9 + c]))
            total = jnp.zeros((yc, LANES), F32)
            for py, part in enumerate(along_y(t1)):
                for px, full in enumerate(along_x(part[0:8])):
                    total += full[:, 0:LANES] * ikf_opp[c * 4 + py * 2 + px]
            cout[c, 0] = 0.5 * (cout[c, 0] + own_opp[c] + 0.25 * total)

    @pl.when(is_f)
    def _():
        edges = jnp.where(lane16 % 4 < 2, xo3[0], xo3[1])
        half = lane // 2
        for c in range(3):
            for k in (c, 3 + c, 6 + c):
                extend(k, k, own_opp[k], yo3, k, edges)
            for side, (place, after) in enumerate(((15, 14), (8, 9))):
                add_part(c, npf_o, pe_o, side, c, place)
                add_part(c, npf_o, pe_o, side, 6 + c, after)
                add_part(3 + c, npf_o, pe_o, side, 3 + c, place)
                add_part(9 + c, npf_l, pe_l, side, c, place)
                for k in range(4 * c, 4 * c + 4):
                    set_part(12 + k, npf_l, pe_l, side, 6 + k, place)
            total = jnp.zeros((16, 2 * LANES), F32)
            for py, part in enumerate(along_y(clamp(ext[c]))):
                for px, full in enumerate(along_x(part)):
                    total += full * ext[12 + c * 4 + py * 2 + px]
            t2 = clamp(ext[6 + c] * (ext[3 + c] - 0.5 * (ext[9 + c] + 0.25 * total)))
            for py, part in enumerate(along_y(t2)):
                evens, odds = along_x(part[0:8])
                evens, odds = evens[:, 0:LANES], odds[:, 0:LANES]
                for t in range(2):
                    index = half + t * (LANES // 2)
                    tiles[c, t, pl.ds(py, yc, stride=2), :] = jnp.where(
                        lane % 2 == 0, pick(evens, index), pick(odds, index)
                    )
            for t in range(2):
                cols = slice(t * LANES, (t + 1) * LANES)
                fout[c, zf - 1, :, cols] = fout[c, zf - 2, :, cols] + tiles[c, t] / stiff[CH[c], zf - 1, :, cols]

    with jax.named_scope("drain"):
        for d in range(6):
            @pl.when(has[d])
            def _(d=d):
                for copy in round_copies(1, d):
                    copy.wait_send()
        for d in range(6):
            @pl.when(has[d])
            def _(d=d):
                for copy in round_copies(0, d):
                    copy.wait_send()
        sent_all(strips)
        for there, g in sides:
            @pl.when(there)
            def _(g=g):
                sent_all(wide_rows(g))
                sent_all(part_rows(g))
                sent_all(passed_parts(g))

        @pl.when(is_f)
        def _():
            ikf_copy.wait_send()

        @pl.when(is_c)
        def _():
            k_copy.wait_send()


def write_out(fine, coarse, fine_out, coarse_out, sem):
    copies = [
        pltpu.make_async_copy(fine, fine_out, sem.at[0]),
        pltpu.make_async_copy(coarse, coarse_out, sem.at[1]),
    ]
    for copy in copies:
        copy.start()
    for copy in copies:
        copy.wait()


def per_device(counts, *args):
    fine, coarse = args[0].shape, args[5].shape
    _, zf, yf, xf = fine
    _, zc, yc, xc = coarse
    vmem = lambda *shape: pltpu.VMEM(shape, F32)
    anywhere = pl.BlockSpec(memory_space=pl.ANY)
    in_vmem = pl.BlockSpec(memory_space=pltpu.VMEM)
    made = pl.pallas_call(
        functools.partial(kernel, counts),
        out_shape=(pltpu.VMEM(fine, F32), pltpu.VMEM(coarse, F32)),
        in_specs=[anywhere] * 9,
        out_specs=(in_vmem, in_vmem),
        scratch_shapes=[
            vmem(3, zf + 2, yf + 2 * PAD, xf + LANES),
            vmem(3, zc + 2, yc + 2 * PAD, xc + LANES),
            vmem(6, zf + 2, yf + 2 * PAD, xf + LANES),
            vmem(6, zc + 2, yc + 2 * PAD, xc + LANES),
            vmem(3, zf, yf, xf), vmem(9, zf, yf, xf), vmem(zf, yf, xf), vmem(zf, yf, xf),
            vmem(3, zc, yc, xc), vmem(9, zc, yc, xc), vmem(zc, yc, xc),
            vmem(2, yf + yc, LANES), vmem(2, 2, yf + yc, LANES),
            vmem(2, 2, 3, zf + zc // 2, 1, xf), vmem(2, 2, 3, zf + zc // 2, 1, xf),
            vmem(9, 3, yf + 2 * PAD, xf + LANES), vmem(9, 3, yc + 2 * PAD, xc + LANES),
            vmem(2, 25, 1, xf), vmem(2, 25, 1, xf), vmem(2, 31, 1, xc), vmem(2, 31, 1, xc),
            vmem(yf, LANES), vmem(2, yf, LANES), vmem(yc, LANES), vmem(2, yc, LANES),
            vmem(2, 18, 1, LANES), vmem(2, 18, 1, LANES), vmem(2, 12, 1, LANES),
            vmem(2, 12, 1, LANES), vmem(2, 12, 1, LANES), vmem(2, 6, 1, LANES),
            vmem(2, 1, LANES), vmem(2, 2, 1, LANES), vmem(2, 2, 1, LANES),
            vmem(2, 3, zf + zc // 2, 1, xf), vmem(2, 1, LANES), vmem(2, 2, 1, LANES),
            vmem(6, 2, yf, LANES), vmem(2, 16, LANES), vmem(18, 16, LANES), vmem(9, yc, LANES), vmem(12, yc, LANES),
            vmem(2, 9, 2, LANES), vmem(2, 9, 2, LANES),
            vmem(16, LANES), vmem(2, 16, LANES), vmem(2, 16, LANES),
            vmem(24, 16, 2 * LANES),
            pltpu.SemaphoreType.DMA((10,)),
            pltpu.SemaphoreType.DMA((37,)),
            pltpu.SemaphoreType.DMA((41,)),
        ],
        compiler_params=pltpu.CompilerParams(
            collective_id=0, has_side_effects=True, vmem_limit_bytes=56 * 1024 * 1024
        ),
        name="elastic_step",
    )(*args)
    made = [pltpu.with_memory_space_constraint(part, pltpu.VMEM) for part in made]
    return pl.pallas_call(
        write_out,
        out_shape=(jax.ShapeDtypeStruct(fine, F32), jax.ShapeDtypeStruct(coarse, F32)),
        in_specs=[in_vmem, in_vmem],
        out_specs=(anywhere, anywhere),
        scratch_shapes=[pltpu.SemaphoreType.DMA((2,))],
        name="write_out",
    )(*made)


def solution(mesh):
    counts = tuple(mesh.shape[name] for name in ("gz", "gy", "gx"))
    volume, field = P(None, "gz", "gy", "gx"), P("gz", "gy", "gx")
    return jax.shard_map(
        functools.partial(per_device, counts),
        mesh=mesh,
        in_specs=(volume, volume, volume, field, field, volume, volume, volume, field),
        out_specs=(volume, volume),
        check_vma=False,
    )
```

```python
import functools

import jax
import jax.numpy as jnp
from jax import lax
from jax.experimental import pallas as pl
from jax.experimental.pallas import tpu as pltpu
from jax.sharding import PartitionSpec as P

TIME_STEP = 0.2
ITERS = 3
F32 = jnp.float32
XX, XY, YY, XZ, YZ, ZZ = range(6)
FACE_X = (XX, XY, XZ)
FACE_Y = (XY, YY, YZ)
WIDE_Y = (1, 3, 5, 6, 8)
EDGE_Y = (5, 1, 3)
WIDE_X = (0, 4, 5, 6, 7)
CH = (4, 3, 2)
PAD = 8
LANES = 128


def lanes_of(rows):
    return lax.broadcasted_iota(jnp.int32, (rows, LANES), 1)


def pack_x(ref, comps, z_count, y_count, width):
    lane = lanes_of(y_count)
    packed = jnp.zeros((y_count, LANES), F32)
    k = 0
    for c in comps:
        for z in range(z_count):
            rows = pl.ds(PAD, y_count)
            tile = ref[c, z + 1, rows, 0:LANES]
            if width > LANES:
                last = ref[c, z + 1, rows, width - LANES : width]
                tile = jnp.where(lane >= LANES // 2, last, tile)
            packed = jnp.where(lane // 2 == k, pltpu.roll(tile, 2 * k + 1, 1), packed)
            k += 1
    return packed


def unpack_x(ref, comps, z_count, y_count, width, from_left, from_right):
    lane = lanes_of(y_count)
    both = jnp.where(lane % 2 == 0, from_left, from_right)
    k = 0
    for c in comps:
        for z in range(z_count):
            ref[c, z + 1, pl.ds(PAD, y_count), width : width + LANES] = pltpu.roll(
                both, LANES - 1 - 2 * k, 1
            )
            k += 1


def diff_x(ref, c, z0, zn, y_count, width, scale):
    v = ref[c, z0 : z0 + zn, PAD : PAD + y_count, :]
    span = width + LANES
    return (pltpu.roll(v, span - 1, 2) - pltpu.roll(v, 1, 2))[:, :, :width] * scale


def diff_y(ref, c, z0, zn, y_count, width, scale):
    after = ref[c, z0 : z0 + zn, PAD + 1 : PAD + 1 + y_count, 0:width]
    before = ref[c, z0 : z0 + zn, PAD - 1 : PAD - 1 + y_count, 0:width]
    return (after - before) * scale


def diff_z(ref, c, z0, zn, y_count, width, scale):
    after = ref[c, z0 + 1 : z0 + 1 + zn, PAD : PAD + y_count, 0:width]
    before = ref[c, z0 - 1 : z0 - 1 + zn, PAD : PAD + y_count, 0:width]
    return (after - before) * scale


def stress_block(u, stiff, s, z, zn, y_count, width, inv, stretch):
    args = (z + 1, zn, y_count, width, inv)
    own = (slice(z + 1, z + 1 + zn), slice(PAD, PAD + y_count), slice(0, width))
    c = [stiff[i, z : z + zn] for i in range(9)]
    nx = diff_x(u, 0, *args)
    ny = diff_y(u, 1, *args)
    nz = diff_z(u, 2, *args) * stretch
    s[(XX,) + own] = c[0] * nx + c[6] * ny + c[7] * nz
    s[(YY,) + own] = c[6] * nx + c[1] * ny + c[8] * nz
    s[(ZZ,) + own] = c[7] * nx + c[8] * ny + c[2] * nz
    s[(YZ,) + own] = c[3] * (diff_z(u, 1, *args) * stretch + diff_y(u, 2, *args))
    s[(XZ,) + own] = c[4] * (diff_z(u, 0, *args) * stretch + diff_x(u, 2, *args))
    s[(XY,) + own] = c[5] * (diff_y(u, 0, *args) + diff_x(u, 1, *args))


def step_block(u, s, prev, dens, out, z, zn, y_count, width, inv, stretch):
    args = (z + 1, zn, y_count, width, inv)
    gain = (TIME_STEP * TIME_STEP) / dens[z : z + zn]
    for c, (sx, sy, sz) in enumerate(((XX, XY, XZ), (XY, YY, YZ), (XZ, YZ, ZZ))):
        total = diff_x(s, sx, *args) + diff_y(s, sy, *args) + diff_z(s, sz, *args) * stretch
        now = u[c, z + 1 : z + 1 + zn, PAD : PAD + y_count, 0:width]
        out[c, z : z + zn] = (2.0 * now - prev[c, z : z + zn]) + gain * total


def stress_ext(u, stiff, s, layer, slab, y_count, width, inv):
    z, first, rows, span = layer + 1, PAD - 1, y_count + 2, width + LANES

    def at(c, dz, dr):
        return u[c, z + dz, first + dr : first + dr + rows, :]

    def dx(c):
        v = at(c, 0, 0)
        return (pltpu.roll(v, span - 1, 1) - pltpu.roll(v, 1, 1)) * inv

    def dy(c):
        return (at(c, 0, 1) - at(c, 0, -1)) * inv

    def dz(c):
        return (at(c, 1, 0) - at(c, -1, 0)) * inv

    c = [stiff[i, slab, first : first + rows, :] for i in range(9)]
    nx, ny, nz = dx(0), dy(1), dz(2)
    values = {
        XX: c[0] * nx + c[6] * ny + c[7] * nz,
        YY: c[6] * nx + c[1] * ny + c[8] * nz,
        ZZ: c[7] * nx + c[8] * ny + c[2] * nz,
        YZ: c[3] * (dz(1) + dy(2)),
        XZ: c[4] * (dz(0) + dx(2)),
        XY: c[5] * (dy(0) + dx(1)),
    }
    for component, value in values.items():
        s[component, z, first : first + rows, :] = value


def pick(x, index):
    return jnp.take_along_axis(x, index, axis=1, mode="promise_in_bounds")


class Grid:
    def __init__(self, **fields):
        self.__dict__.update(fields)
        self.own = (slice(1, self.z + 1), slice(PAD, PAD + self.y), slice(0, self.x))


def kernel(
    counts,
    fn, fp, st, me, de, cn, cp, cst, cde,
    fout, cout,
    u, uc, s, sc, fprev, stiff, metric, dens, cprev, cstiff, cdens,
    xs, xr, ys, yr,
    fwide, cwide, yef_s, yef_r, yec_s, yec_r, xef_s, xef_r, xec_s, xec_r,
    npf_s, npf_l, npf_o, npc_s, npc_l, npc_o, pe_s, pe_l, pe_o, cs, xd_s, xd_r,
    tiles, sums, own, own_opp, ikf_opp, ys3, yo3, xs3, xr3, xo3, ext,
    load_sem, send_sem, recv_sem,
):
    n_z, n_y, n_x = counts
    zf, yf, xf = me.shape
    zc, yc, xc = cde.shape
    fine = Grid(
        z=zf, y=yf, x=xf, u=u, s=s, wide=fwide, source=st, stiff=stiff, third=0, prev=fprev, dens=dens, out=fout, inv=0.5,
        slabs=(1, 2), near=zf - 3, np_s=npf_s, np_l=npf_l, np_o=npf_o, ye_s=yef_s, ye_r=yef_r, xe_s=xef_s, xe_r=xef_r,
    )
    coarse = Grid(
        z=zc, y=yc, x=xc, u=uc, s=sc, wide=cwide, source=cst, stiff=cstiff, third=2, prev=cprev, dens=cdens, out=cout, inv=0.25,
        slabs=(0, 1), near=0, np_s=npc_s, np_l=npc_l, np_o=npc_o, ye_s=yec_s, ye_r=yec_r, xe_s=xec_s, xe_r=xec_r,
    )
    gz, gy, gx = lax.axis_index("gz"), lax.axis_index("gy"), lax.axis_index("gx")
    opp = n_z - 1 - gz
    is_c, is_f = gz == 0, gz == n_z - 1
    active = jnp.logical_or(is_c, is_f)
    has_y = {-1: gy > 0, 0: gy >= 0, 1: gy < n_y - 1}
    has_x = {-1: gx > 0, 0: gx >= 0, 1: gx < n_x - 1}
    has = (gz > 0, gz < n_z - 1, has_y[-1], has_y[1], has_x[-1], has_x[1])
    near = (
        (gz - 1, gy, gx), (gz + 1, gy, gx),
        (gz, gy - 1, gx), (gz, gy + 1, gx),
        (gz, gy, gx - 1), (gz, gy, gx + 1),
    )

    barrier = pltpu.get_barrier_semaphore()
    expected = jnp.int32(0)

    def greet(there, device):
        @pl.when(there)
        def _():
            pl.semaphore_signal(barrier, 1, device_id=device, device_id_type=pl.DeviceIdType.MESH)

        return there.astype(jnp.int32)

    for d in (2, 3, 4, 5, 0, 1):
        expected += greet(has[d], near[d])
    for a in (-1, 1):
        for b in (-1, 1):
            there = jnp.logical_and(active, jnp.logical_and(has_y[a], has_x[b]))
            expected += greet(there, (gz, gy + a, gx + b))
    expected += greet(active, (opp, gy, gx))

    loads = [
        pltpu.make_async_copy(src, dst, load_sem.at[i])
        for i, (src, dst) in enumerate((
            (fn, u.at[(slice(None),) + fine.own]),
            (cn, uc.at[(slice(None),) + coarse.own]),
            (de, dens), (cde, cdens), (fp, fprev), (cp, cprev),
            (st, stiff), (cst, cstiff), (me, metric),
        ))
    ]

    def wide_load(g):
        return pltpu.make_async_copy(
            g.source.at[:, g.near : g.near + 3], g.wide.at[(slice(None), slice(None)) + g.own[1:]], load_sem.at[9]
        )

    sides = ((is_f, fine), (is_c, coarse))
    for load in loads[:2]:
        load.start()
    for there, g in sides:
        @pl.when(there)
        def _(g=g):
            wide_load(g).start()
    for load in loads[2:4]:
        load.start()

    def clear(part):
        part[...] = jnp.zeros(part.shape, F32)

    for there, g in sides:
        @pl.when(there)
        def _(g=g):
            for rows in (pl.ds(0, PAD), pl.ds(PAD + g.y, PAD)):
                clear(g.u.at[:, g.near + 1 : g.near + 4, rows])
                clear(g.wide.at[:, :, rows])

    for g in (fine, coarse):
        for row in (PAD - 1, PAD + g.y):
            clear(g.u.at[:, 1 : g.z + 1, row : row + 1, 0 : g.x])
    for d in range(6):
        @pl.when(jnp.logical_not(has[d]))
        def _(d=d):
            side = d % 2
            if d < 2:
                for g in (fine, coarse):
                    plane = 0 if side == 0 else g.z + 1
                    clear(g.u.at[:, plane])
                    clear(g.s.at[3:6, plane, g.own[1], g.own[2]])
            elif d < 4:
                for r in range(2):
                    clear(yr.at[r, side])
                for g in (fine, coarse):
                    clear(g.ye_r.at[side])
                for b in range(2):
                    clear(xd_r.at[b, side])
            else:
                for r in range(2):
                    clear(xr.at[r, side])
                for g in (fine, coarse):
                    clear(g.xe_r.at[side])
                for b in range(2):
                    clear(xd_r.at[side, b])

    def rdma(src, dst, out, into, device):
        return pltpu.make_async_remote_copy(
            src_ref=src, dst_ref=dst, send_sem=send_sem.at[out], recv_sem=recv_sem.at[into],
            device_id=device, device_id_type=pl.DeviceIdType.MESH,
        )

    def round_copies(r, d):
        side = d % 2
        arrival = 1 - side
        if d < 2:
            comps = (slice(0, 3), slice(3, 6))[r]
            made = []
            for i, g in enumerate((fine, coarse)):
                ref = (g.u, g.s)[r]
                sent, landed = (1, g.z + 1) if side == 0 else (g.z, 0)
                made.append(rdma(
                    ref.at[comps, sent, g.own[1], g.own[2]], ref.at[comps, landed, g.own[1], g.own[2]],
                    (0, 29)[r] + 2 * d + i, 8 * r + 2 * d + i, near[d],
                ))
            return made
        if d < 4:
            return [rdma(ys.at[r, side], yr.at[r, arrival], (d + 2, d + 19)[r], 8 * r + d + 2, near[d])]
        return [rdma(xs.at[r], xr.at[r, arrival], (d + 2, d + 29)[r], 8 * r + d + 2, near[d])]

    def start_round(r, directions):
        for d in directions:
            @pl.when(has[d])
            def _(d=d):
                for copy in round_copies(r, d):
                    copy.start()

    def end_round(r, directions):
        for d in directions:
            @pl.when(has[d ^ 1])
            def _(d=d):
                for copy in round_copies(r, d):
                    copy.wait_recv()

    def row_parts(g, ref, c, row):
        if g is fine:
            return [(ref.at[c, 1 : zf + 1, row : row + 1, 0:xf], (c, slice(0, zf), slice(None), slice(0, xf)))]
        half = zc // 2
        return [
            (
                ref.at[c, 1 + i * half : 1 + (i + 1) * half, row : row + 1, 0:xc],
                (c, slice(zf, zf + half), slice(None), slice(i * xc, (i + 1) * xc)),
            )
            for i in range(2)
        ]

    def pack_rows(r, refs, face_y):
        for g, ref in ((fine, refs[0]), (coarse, refs[1])):
            for side, row in enumerate((PAD, PAD + g.y - 1)):
                for i, c in enumerate(face_y):
                    for part, place in row_parts(g, ref, c, row):
                        ys[(r, side, i) + place[1:]] = part[...]

    def pack_columns(r, refs, face_x):
        xs[r, 0:yf] = pack_x(refs[0], face_x, zf, yf, xf)
        xs[r, yf : yf + yc] = pack_x(refs[1], face_x, zc, yc, xc)

    def pack_stiff_rows():
        half = zc // 2
        for i, c in enumerate(EDGE_Y):
            for side in range(2):
                row = (0, yf - 1)[side]
                cs[side, i, 0:zf] = stiff[c, :, row : row + 1, :]
                row = (0, yc - 1)[side]
                for j in range(2):
                    cs[side, i, zf : zf + half, :, j * xc : (j + 1) * xc] = cstiff[
                        c, j * half : (j + 1) * half, row : row + 1, :
                    ]

    def complete_rows():
        for side, sign in enumerate((-1.0, 1.0)):
            for g, part in ((fine, slice(0, zf)), (coarse, slice(zf, zf + zc // 2))):
                ys[1, side, :, part] = ys[1, side, :, part] + cs[side, :, part] * yr[0, side, :, part] * (sign * g.inv)

    def unpack_rows(r, g, ref, face_y):
        for side, row in enumerate((PAD - 1, PAD + g.y)):
            for i, c in enumerate(face_y):
                for part, place in row_parts(g, ref, c, row):
                    part[...] = yr[(r, side, i) + place[1:]]

    def unpack_columns(r, refs, face_x):
        unpack_x(refs[0], face_x, zf, yf, xf, xr[r, 0, 0:yf], xr[r, 1, 0:yf])
        unpack_x(refs[1], face_x, zc, yc, xc, xr[r, 0, yf : yf + yc], xr[r, 1, yf : yf + yc])

    def pack_wide_rows(g):
        first = g.near + g.slabs[0]
        for side, (edge, second) in enumerate(((PAD, PAD + 1), (PAD + g.y - 1, PAD + g.y - 2))):
            out = g.ye_s.at[side]
            for c in range(3):
                out[2 * c : 2 * c + 2] = g.u[c, first + 1 : first + 3, second : second + 1, 0 : g.x]
            for i, c in enumerate(WIDE_Y):
                out[6 + 3 * i : 9 + 3 * i] = g.wide[c, :, edge : edge + 1, 0 : g.x]
            for i, row in enumerate((edge, second)):
                out[21 + 2 * i : 23 + 2 * i] = g.dens[first : first + 2, row - PAD : row - PAD + 1, :]
                if g is coarse:
                    for c in range(3):
                        out[25 + 3 * i + c] = g.wide[CH[c], 0, row : row + 1, 0 : g.x]

    def pack_wide_columns(g):
        lane = lanes_of(g.y)
        packed = jnp.zeros((g.y, LANES), F32)
        for k, (ref, index) in enumerate(wide_blocks(g)):
            tile = ref[index + (g.own[1], slice(0, LANES))]
            if g.x > LANES:
                last = ref[index + (g.own[1], slice(g.x - LANES, g.x))]
                tile = jnp.where(lane >= LANES // 2, last, tile)
            packed = jnp.where(lane // 4 == k, pltpu.roll(tile, 4 * k + 2, 1), packed)
        g.xe_s[...] = packed
        xd_s[0] = packed[0:1]
        xd_s[1] = packed[g.y - 1 : g.y]

    def wide_blocks(g):
        blocks = [(g.u, (c, g.near + l + 1)) for c in range(3) for l in range(3)]
        return blocks + [(g.wide, (c, l)) for c in WIDE_X for l in g.slabs]

    def wide_rows(g):
        return [
            (has_y[a], has_y[-a], rdma(g.ye_s.at[i], g.ye_r.at[1 - i], 11 + i, 19 + i, (gz, gy + a, gx)))
            for i, a in enumerate((-1, 1))
        ]

    def wide_columns(g, ups):
        made = []
        for i, b in enumerate((-1, 1)):
            for a in ups:
                if a == 0:
                    src, dst = g.xe_s, g.xe_r.at[1 - i]
                else:
                    src, dst = xd_s.at[(a + 1) // 2], xd_r.at[1 - i, (1 - a) // 2]
                made.append((
                    jnp.logical_and(has_y[a], has_x[b]), jnp.logical_and(has_y[-a], has_x[-b]),
                    rdma(src, dst, 13 + i * 3 + (a + 1), 21 + i * 3 + (a + 1), (gz, gy + a, gx + b)),
                ))
        return made

    def part_rows(g):
        made = []
        for i, a in enumerate((-1, 1)):
            for b in (-1, 0, 1):
                k = 3 * i + b + 1
                if b == 0:
                    src, dst = g.np_s.at[i], g.np_l.at[1 - i]
                else:
                    src, dst = pe_s.at[i], pe_l.at[1 - i, (1 - b) // 2]
                made.append((
                    jnp.logical_and(has_y[a], has_x[b]), jnp.logical_and(has_y[-a], has_x[-b]),
                    rdma(src, dst, 23 + k, 33 + k, (gz, gy + a, gx + b)),
                ))
        return made

    def pack_parts(g, count):
        lane1 = lanes_of(1)
        for side in range(2):
            packed = jnp.zeros((1, LANES), F32)
            for k in range(count):
                packed = jnp.where(lane1 // 4 == k, pltpu.roll(g.np_s[side, k], 4 * k + 2, 1), packed)
            pe_s[side] = packed

    def passed_parts(g):
        source, target = (npf_l.at[:, 0:6], npc_o) if g is fine else (npc_l, npf_o)
        return [(active, active, rdma(source, target, 9, 17, (opp, gy, gx))), (active, active, rdma(pe_l, pe_o, 10, 18, (opp, gy, gx)))]

    def squeeze_rows(row_of):
        for side in range(2):
            for c in range(3):
                both = row_of(side, c)
                for i in range(2):
                    k = side * 6 + 3 * i + c
                    for t in range(2):
                        sums[t, k : k + 1] = both[i, :, t * LANES : (t + 1) * LANES]
        pairs = [sums[t] + pltpu.roll(sums[t], LANES - 1, 1) for t in range(2)]
        lane16 = lanes_of(16)
        index = (2 * lane16) % LANES
        return jnp.where(lane16 < LANES // 2, pick(pairs[0], index), pick(pairs[1], index)) * 0.25

    def unpack_wide_rows(g):
        first = g.near + g.slabs[0]
        for side, (edge, second) in enumerate(((PAD - 1, PAD - 2), (PAD + g.y, PAD + g.y + 1))):
            landed = g.ye_r.at[side]
            for c in range(3):
                g.u[c, first + 1 : first + 3, second : second + 1, 0 : g.x] = landed[2 * c : 2 * c + 2]
            for i, c in enumerate(WIDE_Y):
                g.wide[c, :, edge : edge + 1, 0 : g.x] = landed[6 + 3 * i : 9 + 3 * i]

    def unpack_wide_columns(g, corners):
        own_rows = (slice(PAD, PAD + g.y), jnp.where(lanes_of(g.y) % 4 < 2, g.xe_r[0], g.xe_r[1]))
        rows = [own_rows]
        if corners:
            for side, row in enumerate((PAD - 1, PAD + g.y)):
                rows.append((slice(row, row + 1), jnp.where(lanes_of(1) % 4 < 2, xd_r[0, side], xd_r[1, side])))
        for k, (ref, index) in enumerate(wide_blocks(g)):
            for where, both in rows:
                ref[index + (where, slice(g.x, g.x + LANES))] = pltpu.roll(both, LANES - (4 * k + 2), 1)

    def interface_step(g, whole):
        if whole:
            stress_block(g.u, g.stiff, g.s, g.near + g.third, 1, g.y, g.x, g.inv, 1.0)
        for l in g.slabs:
            stress_ext(g.u, g.wide, g.s, g.near + l, l, g.y, g.x, g.inv)
        for l in g.slabs:
            step_block(g.u, g.s, g.prev, g.dens, g.out, g.near + l, 1, g.y, g.x, g.inv, 1.0)

    def beyond_edges(g):
        first = g.near + g.slabs[0]
        span = g.x + LANES
        result = []
        for side, (sign, edge, adjacent) in enumerate(((1.0, PAD, PAD - 1), (-1.0, PAD + g.y - 1, PAD + g.y))):
            scale = sign * g.inv
            d = [g.u[c, g.near + 1 : g.near + 4, edge : edge + 1, :] * scale for c in range(3)]
            w = {c: g.wide[c, :, adjacent : adjacent + 1, :] for c in WIDE_Y}
            s_xx, s_yy, s_zz, s_yz, s_xy = w[6] * d[1], w[1] * d[1], w[8] * d[1], w[3] * d[2], w[5] * d[0]

            def two(v):
                return v[g.slabs[0] : g.slabs[0] + 2, :, 0 : g.x]

            def along_x_of(v):
                v = v[g.slabs[0] : g.slabs[0] + 2]
                return (pltpu.roll(v, span - 1, 2) - pltpu.roll(v, 1, 2))[:, :, 0 : g.x] * g.inv

            def along_z_of(v):
                v = v[:, :, 0 : g.x]
                parts = []
                for l in g.slabs:
                    parts.append((v[l + 1 : l + 2] if l < 2 else 0.0) - (v[l - 1 : l] if l > 0 else 0.0))
                return jnp.concatenate(parts, 0) * g.inv

            def edge_stress(component):
                return g.s[component, first + 1 : first + 3, edge : edge + 1, 0 : g.x] * scale

            totals = (
                (
                    along_x_of(s_xx) + edge_stress(XY),
                    along_x_of(s_xy) + edge_stress(YY) + along_z_of(s_yz),
                    edge_stress(YZ) + along_z_of(s_zz),
                ),
                (two(s_xy) * scale, two(s_yy) * scale, two(s_yz) * scale),
            )
            rows = []
            for i in range(2):
                gain = (TIME_STEP * TIME_STEP) / g.ye_r[side, 21 + 2 * i : 23 + 2 * i]
                rows.append([gain * totals[i][c] for c in range(3)])
            result.append(rows)
        return result

    def start_all(copies):
        for there, _, copy in copies:
            @pl.when(there)
            def _(copy=copy):
                copy.start()

    def receive_all(copies):
        for _, comes, copy in copies:
            @pl.when(comes)
            def _(copy=copy):
                copy.wait_recv()

    def sent_all(copies):
        for there, _, copy in copies:
            @pl.when(there)
            def _(copy=copy):
                copy.wait_send()

    with jax.named_scope("load_pack"):
        loads[0].wait()
        loads[1].wait()
        for load in loads[4:]:
            load.start()
        for there, g in sides:
            @pl.when(there)
            def _(g=g):
                wide_load(g).wait()
                pack_wide_columns(g)
        pack_rows(0, (u, uc), (0, 1, 2))
        loads[2].wait()
        loads[3].wait()
        for there, g in sides:
            @pl.when(there)
            def _(g=g):
                pack_wide_rows(g)
        pack_columns(0, (u, uc), (0, 1, 2))
    with jax.named_scope("barrier"):
        pl.semaphore_wait(barrier, expected)
    with jax.named_scope("send_0"):
        for there, g in sides:
            @pl.when(there)
            def _(g=g):
                start_all(wide_columns(g, (0,)))
        start_round(0, (2, 3))
        for there, g in sides:
            @pl.when(there)
            def _(g=g):
                start_all(wide_rows(g))
                start_all(wide_columns(g, (-1, 1)))
        start_round(0, (4, 5, 0, 1))
        for load in loads[4:]:
            load.wait()
        pack_stiff_rows()

    lane = lanes_of(yc)
    even = (2 * lane) % LANES

    def squeeze(left, right, odd):
        return jnp.where(lane < LANES // 2, pick(left, even + odd), pick(right, even + odd))

    ikf_copy = rdma(own.at[6:18, 0:8], ikf_opp, 8, 16, (opp, gy, gx))
    @pl.when(is_f)
    def _():
        for c in range(3):
            inverse = 1.0 / stiff[CH[c], zf - 1]
            for t in range(2):
                tiles[c, t] = inverse[:, t * LANES : (t + 1) * LANES]
            for py in range(2):
                rows = pl.ds(py, yc, stride=2)
                left, right = tiles[c, 0, rows, :], tiles[c, 1, rows, :]
                for px in range(2):
                    own[6 + c * 4 + py * 2 + px, 0:8] = squeeze(left, right, px)

    k_copy = rdma(own.at[6:9, 0:8], own_opp.at[6:9], 8, 16, (opp, gy, gx))

    @pl.when(is_c)
    def _():
        for c in range(3):
            own[6 + c, 0:8] = cstiff[CH[c], 0] * 0.25

    def pack_own(first, last):
        lane4 = lanes_of(16) // 4
        packed = xs3[...]
        for k in range(first, last):
            packed = jnp.where(lane4 == k, pltpu.roll(own[k], 4 * k + 2, 1), packed)
        xs3[...] = packed

    @pl.when(is_f)
    def _():
        pack_own(6, 18)

    with jax.named_scope("wait_part"):
        for there, g in sides:
            @pl.when(there)
            def _(g=g):
                receive_all(wide_columns(g, (0,)))

    @pl.when(is_f)
    def _():
        unpack_wide_columns(fine, False)
        interface_step(fine, True)
        first = fine.near + fine.slabs[0]

        def two_rows(side, c):
            row = (0, yf - 2)[side]
            return fout[c, first : first + 2, row : row + 1, :] + fout[c, first : first + 2, row + 1 : row + 2, :]

        squeezed = squeeze_rows(two_rows)
        for side in range(2):
            for k in range(6):
                npf_s[side, k] = squeezed[side * 6 + k : side * 6 + k + 1]
            npf_s[side, 6:18] = own[6:18, (0, yc - 1)[side] : (1, yc)[side], :]
        pack_parts(fine, 18)
        start_all(part_rows(fine))
        ikf_copy.start()

    @pl.when(is_c)
    def _():
        unpack_wide_columns(coarse, False)
        interface_step(coarse, True)
        for side in range(2):
            for i in range(2):
                row = (i, yc - 1 - i)[side]
                for c in range(3):
                    start, below = cout[c, 0, row : row + 1, :], cout[c, 1, row : row + 1, :]
                    npc_s[side, 6 * i + c] = own[6 + c, row : row + 1] * (below - start)
                    npc_s[side, 6 * i + 3 + c] = below - 0.5 * start
        pack_parts(coarse, 12)
        start_all(part_rows(coarse))
        k_copy.start()

    def stretch_of(z):
        return jnp.where(gz * zf + z < n_z * zf // 2, metric[z : z + 1], 1.0)

    zb = min(4, zc)

    def stress_all():
        for z in range(zf):
            stress_block(u, stiff, s, z, 1, yf, xf, 0.5, stretch_of(z))
        for z in range(0, zc, zb):
            stress_block(uc, cstiff, sc, z, zb, yc, xc, 0.25, 1.0)

    def complete_stress():
        for g in (fine, coarse):
            for row, beyond, sign in ((0, PAD - 1, -1.0), (g.y - 1, PAD + g.y, 1.0)):
                d = [g.u[c, 1 : g.z + 1, beyond : beyond + 1, 0 : g.x] * (sign * g.inv) for c in range(3)]
                for component, channel, c in ((XX, 6, 1), (YY, 1, 1), (ZZ, 8, 1), (YZ, 3, 2), (XY, 5, 0)):
                    g.s[component, 1 : g.z + 1, PAD + row : PAD + row + 1, 0 : g.x] += (
                        g.stiff[channel, :, row : row + 1, :] * d[c]
                    )

    with jax.named_scope("wait_near"):
        end_round(0, (4, 5, 0, 1))
    with jax.named_scope("part_stress"):
        unpack_columns(0, (u, uc), (0, 1, 2))
        stress_all()
        pack_rows(1, (s, sc), FACE_Y)

    with jax.named_scope("wait_rows"):
        end_round(0, (2, 3))
        complete_rows()
        start_round(1, (2, 3))
        unpack_rows(0, fine, u, (0, 1, 2))
        unpack_rows(0, coarse, uc, (0, 1, 2))

    with jax.named_scope("stress"):
        complete_stress()
        pack_columns(1, (s, sc), FACE_X)
        start_round(1, (4, 5, 0, 1))

    with jax.named_scope("wait_wide"):
        for there, g in sides:
            @pl.when(there)
            def _(g=g):
                receive_all(wide_rows(g))
                receive_all(wide_columns(g, (-1, 1)))

    def pack_strips(first, last):
        pack_own(first, last)
        ys3[0] = own[0:9, 14:16, :]
        ys3[1] = own[0:9, 8:10, :]

    @pl.when(is_c)
    def _():
        unpack_wide_rows(coarse)
        unpack_wide_columns(coarse, True)
        interface_step(coarse, False)
        for c in range(3):
            start, below = cout[c, 0], cout[c, 1]
            own[c, 0:8] = own[6 + c, 0:8] * (below - start)
            own[3 + c, 0:8] = below - 0.5 * start
        for side, rows in enumerate(beyond_edges(coarse)):
            for i in range(2):
                place = (15 - i) if side == 0 else (8 + i)
                for c in range(3):
                    start, below = rows[i][c][0], rows[i][c][1]
                    k = yec_r[side, 25 + 3 * i + c] * 0.25
                    own[c, place : place + 1] = k * (below - start)
                    own[3 + c, place : place + 1] = below - 0.5 * start
                    own[6 + c, place : place + 1] = k
        pack_strips(0, 9)

    @pl.when(is_f)
    def _():
        unpack_wide_rows(fine)
        unpack_wide_columns(fine, True)
        interface_step(fine, False)
        beyond = beyond_edges(fine)
        squeezed = squeeze_rows(lambda side, c: beyond[side][0][c] + beyond[side][1][c])
        for c in range(3):
            for i, z in enumerate((zf - 2, zf - 1)):
                pairs = []
                k = 3 * i + c
                for t in range(2):
                    tiles[k, t] = fout[c, z, :, t * LANES : (t + 1) * LANES]
                    pair = tiles[k, t, pl.ds(0, yc, stride=2), :] + tiles[k, t, pl.ds(1, yc, stride=2), :]
                    pairs.append(pair + pltpu.roll(pair, LANES - 1, 1))
                own[k, 0:8] = squeeze(pairs[0], pairs[1], 0) * 0.25
        for side, place in enumerate((15, 8)):
            for k in range(6):
                own[k, place : place + 1] = squeezed[side * 6 + k : side * 6 + k + 1]
        pack_strips(0, 6)

    strips = [
        (active, active, rdma(own.at[0:6, 0:8], own_opp.at[0:6], 13, 27, (opp, gy, gx))),
        (is_f, is_c, rdma(ys3.at[:, 3:6], yo3.at[:, 3:6], 14, 28, (opp, gy, gx))),
        (is_c, is_f, rdma(ys3, yo3, 14, 28, (opp, gy, gx))),
    ]
    for level, tile_to, out, into in ((opp, xo3, 15, 31), (gz, xr3, 17, 29)):
        for i, b in enumerate((-1, 1)):
            strips.append((
                jnp.logical_and(active, has_x[b]), jnp.logical_and(active, has_x[-b]),
                rdma(xs3, tile_to.at[1 - i], out + i, into + i, (level, gy, gx + b)),
            ))
    opp_strips, level_strips = strips[:5], strips[5:]

    for there, g in sides:
        @pl.when(there)
        def _(g=g):
            sent_all(wide_columns(g, (-1, 0, 1)))

    start_all(strips)

    with jax.named_scope("wait_parts"):
        for there, g in sides:
            @pl.when(there)
            def _(g=g):
                receive_all(part_rows(g))
                start_all(passed_parts(g))

    with jax.named_scope("wait_1"):
        end_round(1, (4, 5, 0, 1))
    with jax.named_scope("step"):
        for g in (fine, coarse):
            for row in (PAD - 1, PAD + g.y):
                for c in FACE_Y:
                    clear(g.s.at[c, 1 : g.z + 1, row : row + 1, 0 : g.x])
        unpack_columns(1, (s, sc), FACE_X)
        for z in range(zf):
            step_block(u, s, fprev, dens, fout, z, 1, yf, xf, 0.5, stretch_of(z))
        for z in range(0, zc, zb):
            step_block(uc, sc, cprev, cdens, cout, z, zb, yc, xc, 0.25, 1.0)
    with jax.named_scope("wait_rows_1"):
        end_round(1, (2, 3))
        half = zc // 2
        for side, sign in enumerate((-1.0, 1.0)):
            row = (0, yf - 1)[side]
            gain = (sign * 0.5 * TIME_STEP * TIME_STEP) / dens[:, row : row + 1, :]
            for c in range(3):
                fout[c, :, row : row + 1, :] += gain * yr[1, side, c, 0:zf]
            row = (0, yc - 1)[side]
            gain = (sign * 0.25 * TIME_STEP * TIME_STEP) / cdens[:, row : row + 1, :]
            for j in range(2):
                part, cols = slice(j * half, (j + 1) * half), slice(j * xc, (j + 1) * xc)
                for c in range(3):
                    cout[c, part, row : row + 1, :] += gain[part] * yr[1, side, c, zf : zf + half, :, cols]

    lane16 = lanes_of(16)
    wide_row = lax.broadcasted_iota(jnp.int32, (16, 2 * LANES), 0)
    wide_lane = lax.broadcasted_iota(jnp.int32, (16, 2 * LANES), 1)

    def extend(k, field, centre, rims, row, edges):
        ext[k, 0:8, 0:LANES] = centre
        ext[k, 14:16, 0:LANES] = rims[0, row]
        ext[k, 8:10, 0:LANES] = rims[1, row]
        ext[k, :, LANES : 2 * LANES] = pltpu.roll(edges, LANES - (4 * field + 2), 1)

    def clamp(t):
        t = jnp.where(jnp.logical_and(wide_row == 15, gy == 0), pltpu.roll(t, 15, 0), t)
        t = jnp.where(jnp.logical_and(wide_row == 8, gy == n_y - 1), pltpu.roll(t, 1, 0), t)
        t = jnp.where(jnp.logical_and(wide_lane == 2 * LANES - 1, gx == 0), pltpu.roll(t, 2 * LANES - 1, 1), t)
        return jnp.where(jnp.logical_and(wide_lane == LANES, gx == n_x - 1), pltpu.roll(t, 1, 1), t)

    def along_y(t):
        return (0.75 * t + 0.25 * pltpu.roll(t, 1, 0), 0.75 * t + 0.25 * pltpu.roll(t, 15, 0))

    def along_x(t):
        return (0.75 * t + 0.25 * pltpu.roll(t, 1, 1), 0.75 * t + 0.25 * pltpu.roll(t, 2 * LANES - 1, 1))

    def extend_own(k, field, edges):
        ext[k, :, 0:LANES] = own[field]
        ext[k, :, LANES : 2 * LANES] = pltpu.roll(edges, LANES - (4 * field + 2), 1)

    with jax.named_scope("wait_level"):
        receive_all(level_strips)

    @pl.when(is_c)
    def _():
        edges = jnp.where(lane16 % 4 < 2, xr3[0], xr3[1])
        for k in range(3, 9):
            extend_own(k, k, edges)
        ikf_copy.wait_recv()

    @pl.when(is_f)
    def _():
        edges = jnp.where(lane16 % 4 < 2, xr3[0], xr3[1])
        for k in range(3):
            extend_own(9 + k, k, edges)
        for k in range(12):
            extend_own(12 + k, 6 + k, edges)

    with jax.named_scope("wait_opp"):
        receive_all(opp_strips)

    with jax.named_scope("wait_passed"):
        for there, g in sides:
            @pl.when(there)
            def _(g=g):
                receive_all(passed_parts(coarse if g is fine else fine))

    def part_of(parts, rims, side, field):
        edges = jnp.where(lanes_of(1) % 4 < 2, rims[side, 0], rims[side, 1])
        return jnp.concatenate([parts[side, field], pltpu.roll(edges, LANES - (4 * field + 2), 1)], 1)

    def add_part(k, parts, rims, side, field, place):
        ext[k, place : place + 1] += part_of(parts, rims, side, field)

    def set_part(k, parts, rims, side, field, place):
        ext[k, place : place + 1] = part_of(parts, rims, side, field)

    @pl.when(is_f)
    def _():
        k_copy.wait_recv()

    @pl.when(is_c)
    def _():
        edges = jnp.where(lane16 % 4 < 2, xo3[0], xo3[1])
        for c in range(3):
            extend(9 + c, 3 + c, own_opp[3 + c], yo3, 3 + c, edges)
            for side, place in enumerate((15, 8)):
                add_part(9 + c, npc_o, pe_o, side, 3 + c, place)
                add_part(3 + c, npc_l, pe_l, side, 3 + c, place)
            t1 = clamp(ext[6 + c] * (ext[3 + c] - 0.5 * ext[9 + c]))
            total = jnp.zeros((yc, LANES), F32)
            for py, part in enumerate(along_y(t1)):
                for px, full in enumerate(along_x(part[0:8])):
                    total += full[:, 0:LANES] * ikf_opp[c * 4 + py * 2 + px]
            cout[c, 0] = 0.5 * (cout[c, 0] + own_opp[c] + 0.25 * total)

    @pl.when(is_f)
    def _():
        edges = jnp.where(lane16 % 4 < 2, xo3[0], xo3[1])
        half = lane // 2
        for c in range(3):
            for k in (c, 3 + c, 6 + c):
                extend(k, k, own_opp[k], yo3, k, edges)
            for side, (place, after) in enumerate(((15, 14), (8, 9))):
                add_part(c, npf_o, pe_o, side, c, place)
                add_part(c, npf_o, pe_o, side, 6 + c, after)
                add_part(3 + c, npf_o, pe_o, side, 3 + c, place)
                add_part(9 + c, npf_l, pe_l, side, c, place)
                for k in range(4 * c, 4 * c + 4):
                    set_part(12 + k, npf_l, pe_l, side, 6 + k, place)
            total = jnp.zeros((16, 2 * LANES), F32)
            for py, part in enumerate(along_y(clamp(ext[c]))):
                for px, full in enumerate(along_x(part)):
                    total += full * ext[12 + c * 4 + py * 2 + px]
            t2 = clamp(ext[6 + c] * (ext[3 + c] - 0.5 * (ext[9 + c] + 0.25 * total)))
            for py, part in enumerate(along_y(t2)):
                evens, odds = along_x(part[0:8])
                evens, odds = evens[:, 0:LANES], odds[:, 0:LANES]
                for t in range(2):
                    index = half + t * (LANES // 2)
                    tiles[c, t, pl.ds(py, yc, stride=2), :] = jnp.where(
                        lane % 2 == 0, pick(evens, index), pick(odds, index)
                    )
            for t in range(2):
                cols = slice(t * LANES, (t + 1) * LANES)
                fout[c, zf - 1, :, cols] = fout[c, zf - 2, :, cols] + tiles[c, t] / stiff[CH[c], zf - 1, :, cols]

    with jax.named_scope("drain"):
        for d in range(6):
            @pl.when(has[d])
            def _(d=d):
                for copy in round_copies(1, d):
                    copy.wait_send()
        for d in range(6):
            @pl.when(has[d])
            def _(d=d):
                for copy in round_copies(0, d):
                    copy.wait_send()
        sent_all(strips)
        for there, g in sides:
            @pl.when(there)
            def _(g=g):
                sent_all(wide_rows(g))
                sent_all(part_rows(g))
                sent_all(passed_parts(g))

        @pl.when(is_f)
        def _():
            ikf_copy.wait_send()

        @pl.when(is_c)
        def _():
            k_copy.wait_send()


def write_out(fine, coarse, fine_out, coarse_out, sem):
    copies = [
        pltpu.make_async_copy(fine, fine_out, sem.at[0]),
        pltpu.make_async_copy(coarse, coarse_out, sem.at[1]),
    ]
    for copy in copies:
        copy.start()
    for copy in copies:
        copy.wait()


def per_device(counts, *args):
    fine, coarse = args[0].shape, args[5].shape
    _, zf, yf, xf = fine
    _, zc, yc, xc = coarse
    vmem = lambda *shape: pltpu.VMEM(shape, F32)
    anywhere = pl.BlockSpec(memory_space=pl.ANY)
    in_vmem = pl.BlockSpec(memory_space=pltpu.VMEM)
    made = pl.pallas_call(
        functools.partial(kernel, counts),
        out_shape=(pltpu.VMEM(fine, F32), pltpu.VMEM(coarse, F32)),
        in_specs=[anywhere] * 9,
        out_specs=(in_vmem, in_vmem),
        scratch_shapes=[
            vmem(3, zf + 2, yf + 2 * PAD, xf + LANES),
            vmem(3, zc + 2, yc + 2 * PAD, xc + LANES),
            vmem(6, zf + 2, yf + 2 * PAD, xf + LANES),
            vmem(6, zc + 2, yc + 2 * PAD, xc + LANES),
            vmem(3, zf, yf, xf), vmem(9, zf, yf, xf), vmem(zf, yf, xf), vmem(zf, yf, xf),
            vmem(3, zc, yc, xc), vmem(9, zc, yc, xc), vmem(zc, yc, xc),
            vmem(2, yf + yc, LANES), vmem(2, 2, yf + yc, LANES),
            vmem(2, 2, 3, zf + zc // 2, 1, xf), vmem(2, 2, 3, zf + zc // 2, 1, xf),
            vmem(9, 3, yf + 2 * PAD, xf + LANES), vmem(9, 3, yc + 2 * PAD, xc + LANES),
            vmem(2, 25, 1, xf), vmem(2, 25, 1, xf), vmem(2, 31, 1, xc), vmem(2, 31, 1, xc),
            vmem(yf, LANES), vmem(2, yf, LANES), vmem(yc, LANES), vmem(2, yc, LANES),
            vmem(2, 18, 1, LANES), vmem(2, 18, 1, LANES), vmem(2, 12, 1, LANES),
            vmem(2, 12, 1, LANES), vmem(2, 12, 1, LANES), vmem(2, 6, 1, LANES),
            vmem(2, 1, LANES), vmem(2, 2, 1, LANES), vmem(2, 2, 1, LANES),
            vmem(2, 3, zf + zc // 2, 1, xf), vmem(2, 1, LANES), vmem(2, 2, 1, LANES),
            vmem(6, 2, yf, LANES), vmem(2, 16, LANES), vmem(18, 16, LANES), vmem(9, yc, LANES), vmem(12, yc, LANES),
            vmem(2, 9, 2, LANES), vmem(2, 9, 2, LANES),
            vmem(16, LANES), vmem(2, 16, LANES), vmem(2, 16, LANES),
            vmem(24, 16, 2 * LANES),
            pltpu.SemaphoreType.DMA((10,)),
            pltpu.SemaphoreType.DMA((35,)),
            pltpu.SemaphoreType.DMA((39,)),
        ],
        compiler_params=pltpu.CompilerParams(
            collective_id=0, has_side_effects=True, vmem_limit_bytes=56 * 1024 * 1024
        ),
        name="elastic_step",
    )(*args)
    made = [pltpu.with_memory_space_constraint(part, pltpu.VMEM) for part in made]
    return pl.pallas_call(
        write_out,
        out_shape=(jax.ShapeDtypeStruct(fine, F32), jax.ShapeDtypeStruct(coarse, F32)),
        in_specs=[in_vmem, in_vmem],
        out_specs=(anywhere, anywhere),
        scratch_shapes=[pltpu.SemaphoreType.DMA((2,))],
        name="write_out",
    )(*made)


def solution(mesh):
    counts = tuple(mesh.shape[name] for name in ("gz", "gy", "gx"))
    volume, field = P(None, "gz", "gy", "gx"), P("gz", "gy", "gx")
    return jax.shard_map(
        functools.partial(per_device, counts),
        mesh=mesh,
        in_specs=(volume, volume, volume, field, field, volume, volume, volume, field),
        out_specs=(volume, volume),
        check_vma=False,
    )
```

```python
import functools

import jax
import jax.numpy as jnp
from jax import lax
from jax.experimental import pallas as pl
from jax.experimental.pallas import tpu as pltpu
from jax.sharding import PartitionSpec as P

TIME_STEP = 0.2
ITERS = 3
F32 = jnp.float32
XX, XY, YY, XZ, YZ, ZZ = range(6)
FACE_X = (XX, XY, XZ)
FACE_Y = (XY, YY, YZ)
WIDE_Y = (1, 3, 5, 6, 8)
EDGE_Y = (5, 1, 3)
WIDE_X = (0, 4, 5, 6, 7)
CH = (4, 3, 2)
PAD = 8
LANES = 128


def lanes_of(rows):
    return lax.broadcasted_iota(jnp.int32, (rows, LANES), 1)


def pack_x(ref, comps, z_count, y_count, width):
    lane = lanes_of(y_count)
    packed = jnp.zeros((y_count, LANES), F32)
    k = 0
    for c in comps:
        for z in range(z_count):
            rows = pl.ds(PAD, y_count)
            tile = ref[c, z + 1, rows, 0:LANES]
            if width > LANES:
                last = ref[c, z + 1, rows, width - LANES : width]
                tile = jnp.where(lane >= LANES // 2, last, tile)
            packed = jnp.where(lane // 2 == k, pltpu.roll(tile, 2 * k + 1, 1), packed)
            k += 1
    return packed


def unpack_x(ref, comps, z_count, y_count, width, from_left, from_right):
    lane = lanes_of(y_count)
    both = jnp.where(lane % 2 == 0, from_left, from_right)
    k = 0
    for c in comps:
        for z in range(z_count):
            ref[c, z + 1, pl.ds(PAD, y_count), width : width + LANES] = pltpu.roll(
                both, LANES - 1 - 2 * k, 1
            )
            k += 1


def diff_x(ref, c, z0, zn, y_count, width, scale):
    v = ref[c, z0 : z0 + zn, PAD : PAD + y_count, :]
    span = width + LANES
    return (pltpu.roll(v, span - 1, 2) - pltpu.roll(v, 1, 2))[:, :, :width] * scale


def diff_y(ref, c, z0, zn, y_count, width, scale):
    after = ref[c, z0 : z0 + zn, PAD + 1 : PAD + 1 + y_count, 0:width]
    before = ref[c, z0 : z0 + zn, PAD - 1 : PAD - 1 + y_count, 0:width]
    return (after - before) * scale


def diff_z(ref, c, z0, zn, y_count, width, scale):
    after = ref[c, z0 + 1 : z0 + 1 + zn, PAD : PAD + y_count, 0:width]
    before = ref[c, z0 - 1 : z0 - 1 + zn, PAD : PAD + y_count, 0:width]
    return (after - before) * scale


def stress_block(u, stiff, s, z, zn, y_count, width, inv, stretch):
    args = (z + 1, zn, y_count, width, inv)
    own = (slice(z + 1, z + 1 + zn), slice(PAD, PAD + y_count), slice(0, width))
    c = [stiff[i, z : z + zn] for i in range(9)]
    nx = diff_x(u, 0, *args)
    ny = diff_y(u, 1, *args)
    nz = diff_z(u, 2, *args) * stretch
    s[(XX,) + own] = c[0] * nx + c[6] * ny + c[7] * nz
    s[(YY,) + own] = c[6] * nx + c[1] * ny + c[8] * nz
    s[(ZZ,) + own] = c[7] * nx + c[8] * ny + c[2] * nz
    s[(YZ,) + own] = c[3] * (diff_z(u, 1, *args) * stretch + diff_y(u, 2, *args))
    s[(XZ,) + own] = c[4] * (diff_z(u, 0, *args) * stretch + diff_x(u, 2, *args))
    s[(XY,) + own] = c[5] * (diff_y(u, 0, *args) + diff_x(u, 1, *args))


def step_block(u, s, prev, dens, out, z, zn, y_count, width, inv, stretch):
    args = (z + 1, zn, y_count, width, inv)
    gain = (TIME_STEP * TIME_STEP) / dens[z : z + zn]
    for c, (sx, sy, sz) in enumerate(((XX, XY, XZ), (XY, YY, YZ), (XZ, YZ, ZZ))):
        total = diff_x(s, sx, *args) + diff_y(s, sy, *args) + diff_z(s, sz, *args) * stretch
        now = u[c, z + 1 : z + 1 + zn, PAD : PAD + y_count, 0:width]
        out[c, z : z + zn] = (2.0 * now - prev[c, z : z + zn]) + gain * total


def stress_ext(u, stiff, s, layer, slab, y_count, width, inv):
    z, first, rows, span = layer + 1, PAD - 1, y_count + 2, width + LANES

    def at(c, dz, dr):
        return u[c, z + dz, first + dr : first + dr + rows, :]

    def dx(c):
        v = at(c, 0, 0)
        return (pltpu.roll(v, span - 1, 1) - pltpu.roll(v, 1, 1)) * inv

    def dy(c):
        return (at(c, 0, 1) - at(c, 0, -1)) * inv

    def dz(c):
        return (at(c, 1, 0) - at(c, -1, 0)) * inv

    c = [stiff[i, slab, first : first + rows, :] for i in range(9)]
    nx, ny, nz = dx(0), dy(1), dz(2)
    values = {
        XX: c[0] * nx + c[6] * ny + c[7] * nz,
        YY: c[6] * nx + c[1] * ny + c[8] * nz,
        ZZ: c[7] * nx + c[8] * ny + c[2] * nz,
        YZ: c[3] * (dz(1) + dy(2)),
        XZ: c[4] * (dz(0) + dx(2)),
        XY: c[5] * (dy(0) + dx(1)),
    }
    for component, value in values.items():
        s[component, z, first : first + rows, :] = value


def pick(x, index):
    return jnp.take_along_axis(x, index, axis=1, mode="promise_in_bounds")


class Grid:
    def __init__(self, **fields):
        self.__dict__.update(fields)
        self.own = (slice(1, self.z + 1), slice(PAD, PAD + self.y), slice(0, self.x))


def kernel(
    counts,
    fn, fp, st, me, de, cn, cp, cst, cde,
    fout, cout,
    u, uc, s, sc, fprev, stiff, metric, dens, cprev, cstiff, cdens,
    xs, xr, ys, yr,
    fwide, cwide, yef_s, yef_r, yec_s, yec_r, xef_s, xef_r, xec_s, xec_r,
    npf_s, npf_l, npf_o, npc_s, npc_l, npc_o, pe_s, pe_l, pe_o, cs, xd_s, xd_r,
    tiles, sums, own, own_opp, ikf_opp, ys3, yo3, xs3, xr3, xo3, ext,
    load_sem, send_sem, recv_sem,
):
    n_z, n_y, n_x = counts
    zf, yf, xf = me.shape
    zc, yc, xc = cde.shape
    fine = Grid(
        z=zf, y=yf, x=xf, u=u, s=s, wide=fwide, source=st, stiff=stiff, third=0, prev=fprev, dens=dens, out=fout, inv=0.5,
        slabs=(1, 2), near=zf - 3, np_s=npf_s, np_l=npf_l, np_o=npf_o, ye_s=yef_s, ye_r=yef_r, xe_s=xef_s, xe_r=xef_r,
    )
    coarse = Grid(
        z=zc, y=yc, x=xc, u=uc, s=sc, wide=cwide, source=cst, stiff=cstiff, third=2, prev=cprev, dens=cdens, out=cout, inv=0.25,
        slabs=(0, 1), near=0, np_s=npc_s, np_l=npc_l, np_o=npc_o, ye_s=yec_s, ye_r=yec_r, xe_s=xec_s, xe_r=xec_r,
    )
    gz, gy, gx = lax.axis_index("gz"), lax.axis_index("gy"), lax.axis_index("gx")
    opp = n_z - 1 - gz
    is_c, is_f = gz == 0, gz == n_z - 1
    active = jnp.logical_or(is_c, is_f)
    has_y = {-1: gy > 0, 0: gy >= 0, 1: gy < n_y - 1}
    has_x = {-1: gx > 0, 0: gx >= 0, 1: gx < n_x - 1}
    has = (gz > 0, gz < n_z - 1, has_y[-1], has_y[1], has_x[-1], has_x[1])
    near = (
        (gz - 1, gy, gx), (gz + 1, gy, gx),
        (gz, gy - 1, gx), (gz, gy + 1, gx),
        (gz, gy, gx - 1), (gz, gy, gx + 1),
    )

    barrier = pltpu.get_barrier_semaphore()
    expected = jnp.int32(0)

    def greet(there, device):
        @pl.when(there)
        def _():
            pl.semaphore_signal(barrier, 1, device_id=device, device_id_type=pl.DeviceIdType.MESH)

        return there.astype(jnp.int32)

    for d in (2, 3, 4, 5, 0, 1):
        expected += greet(has[d], near[d])
    for a in (-1, 1):
        for b in (-1, 1):
            there = jnp.logical_and(active, jnp.logical_and(has_y[a], has_x[b]))
            expected += greet(there, (gz, gy + a, gx + b))
    expected += greet(active, (opp, gy, gx))

    loads = [
        pltpu.make_async_copy(src, dst, load_sem.at[i])
        for i, (src, dst) in enumerate((
            (fn, u.at[(slice(None),) + fine.own]),
            (cn, uc.at[(slice(None),) + coarse.own]),
            (de, dens), (cde, cdens), (fp, fprev), (cp, cprev),
            (st, stiff), (cst, cstiff), (me, metric),
        ))
    ]

    def wide_load(g):
        return pltpu.make_async_copy(
            g.source.at[:, g.near : g.near + 3], g.wide.at[(slice(None), slice(None)) + g.own[1:]], load_sem.at[9]
        )

    sides = ((is_f, fine), (is_c, coarse))
    for load in loads[:2]:
        load.start()
    for there, g in sides:
        @pl.when(there)
        def _(g=g):
            wide_load(g).start()
    for load in loads[2:4]:
        load.start()

    def clear(part):
        part[...] = jnp.zeros(part.shape, F32)

    for there, g in sides:
        @pl.when(there)
        def _(g=g):
            for rows in (pl.ds(0, PAD), pl.ds(PAD + g.y, PAD)):
                clear(g.u.at[:, g.near + 1 : g.near + 4, rows])
                clear(g.wide.at[:, :, rows])

    for g in (fine, coarse):
        for row in (PAD - 1, PAD + g.y):
            clear(g.u.at[:, 1 : g.z + 1, row : row + 1, 0 : g.x])
    for d in range(6):
        @pl.when(jnp.logical_not(has[d]))
        def _(d=d):
            side = d % 2
            if d < 2:
                for g in (fine, coarse):
                    plane = 0 if side == 0 else g.z + 1
                    clear(g.u.at[:, plane])
                    clear(g.s.at[3:6, plane, g.own[1], g.own[2]])
            elif d < 4:
                for r in range(2):
                    clear(yr.at[r, side])
                for g in (fine, coarse):
                    clear(g.ye_r.at[side])
                for b in range(2):
                    clear(xd_r.at[b, side])
            else:
                for r in range(2):
                    clear(xr.at[r, side])
                for g in (fine, coarse):
                    clear(g.xe_r.at[side])
                for b in range(2):
                    clear(xd_r.at[side, b])

    def rdma(src, dst, out, into, device):
        return pltpu.make_async_remote_copy(
            src_ref=src, dst_ref=dst, send_sem=send_sem.at[out], recv_sem=recv_sem.at[into],
            device_id=device, device_id_type=pl.DeviceIdType.MESH,
        )

    def round_copies(r, d):
        side = d % 2
        arrival = 1 - side
        if d < 2:
            comps = (slice(0, 3), slice(3, 6))[r]
            made = []
            for i, g in enumerate((fine, coarse)):
                ref = (g.u, g.s)[r]
                sent, landed = (1, g.z + 1) if side == 0 else (g.z, 0)
                made.append(rdma(
                    ref.at[comps, sent, g.own[1], g.own[2]], ref.at[comps, landed, g.own[1], g.own[2]],
                    (0, 29)[r] + 2 * d + i, 8 * r + 2 * d + i, near[d],
                ))
            return made
        if d < 4:
            return [rdma(ys.at[r, side], yr.at[r, arrival], (d + 2, d + 19)[r], 8 * r + d + 2, near[d])]
        return [rdma(xs.at[r], xr.at[r, arrival], (d + 2, d + 29)[r], 8 * r + d + 2, near[d])]

    def start_round(r, directions):
        for d in directions:
            @pl.when(has[d])
            def _(d=d):
                for copy in round_copies(r, d):
                    copy.start()

    def end_round(r, directions):
        for d in directions:
            @pl.when(has[d ^ 1])
            def _(d=d):
                for copy in round_copies(r, d):
                    copy.wait_recv()

    def row_parts(g, ref, c, row):
        if g is fine:
            return [(ref.at[c, 1 : zf + 1, row : row + 1, 0:xf], (c, slice(0, zf), slice(None), slice(0, xf)))]
        half = zc // 2
        return [
            (
                ref.at[c, 1 + i * half : 1 + (i + 1) * half, row : row + 1, 0:xc],
                (c, slice(zf, zf + half), slice(None), slice(i * xc, (i + 1) * xc)),
            )
            for i in range(2)
        ]

    def pack_rows(r, refs, face_y):
        for g, ref in ((fine, refs[0]), (coarse, refs[1])):
            for side, row in enumerate((PAD, PAD + g.y - 1)):
                for i, c in enumerate(face_y):
                    for part, place in row_parts(g, ref, c, row):
                        ys[(r, side, i) + place[1:]] = part[...]

    def pack_columns(r, refs, face_x):
        xs[r, 0:yf] = pack_x(refs[0], face_x, zf, yf, xf)
        xs[r, yf : yf + yc] = pack_x(refs[1], face_x, zc, yc, xc)

    def pack_stiff_rows():
        half = zc // 2
        for i, c in enumerate(EDGE_Y):
            for side in range(2):
                row = (0, yf - 1)[side]
                cs[side, i, 0:zf] = stiff[c, :, row : row + 1, :]
                row = (0, yc - 1)[side]
                for j in range(2):
                    cs[side, i, zf : zf + half, :, j * xc : (j + 1) * xc] = cstiff[
                        c, j * half : (j + 1) * half, row : row + 1, :
                    ]

    def complete_rows():
        for side, sign in enumerate((-1.0, 1.0)):
            for g, part in ((fine, slice(0, zf)), (coarse, slice(zf, zf + zc // 2))):
                ys[1, side, :, part] = ys[1, side, :, part] + cs[side, :, part] * yr[0, side, :, part] * (sign * g.inv)

    def unpack_rows(r, g, ref, face_y):
        for side, row in enumerate((PAD - 1, PAD + g.y)):
            for i, c in enumerate(face_y):
                for part, place in row_parts(g, ref, c, row):
                    part[...] = yr[(r, side, i) + place[1:]]

    def unpack_columns(r, refs, face_x):
        unpack_x(refs[0], face_x, zf, yf, xf, xr[r, 0, 0:yf], xr[r, 1, 0:yf])
        unpack_x(refs[1], face_x, zc, yc, xc, xr[r, 0, yf : yf + yc], xr[r, 1, yf : yf + yc])

    def pack_wide_rows(g):
        first = g.near + g.slabs[0]
        for side, (edge, second) in enumerate(((PAD, PAD + 1), (PAD + g.y - 1, PAD + g.y - 2))):
            out = g.ye_s.at[side]
            for c in range(3):
                out[2 * c : 2 * c + 2] = g.u[c, first + 1 : first + 3, second : second + 1, 0 : g.x]
            for i, c in enumerate(WIDE_Y):
                out[6 + 3 * i : 9 + 3 * i] = g.wide[c, :, edge : edge + 1, 0 : g.x]
            for i, row in enumerate((edge, second)):
                out[21 + 2 * i : 23 + 2 * i] = g.dens[first : first + 2, row - PAD : row - PAD + 1, :]
                if g is coarse:
                    for c in range(3):
                        out[25 + 3 * i + c] = g.wide[CH[c], 0, row : row + 1, 0 : g.x]

    def pack_wide_columns(g):
        lane = lanes_of(g.y)
        packed = jnp.zeros((g.y, LANES), F32)
        for k, (ref, index) in enumerate(wide_blocks(g)):
            tile = ref[index + (g.own[1], slice(0, LANES))]
            if g.x > LANES:
                last = ref[index + (g.own[1], slice(g.x - LANES, g.x))]
                tile = jnp.where(lane >= LANES // 2, last, tile)
            packed = jnp.where(lane // 4 == k, pltpu.roll(tile, 4 * k + 2, 1), packed)
        g.xe_s[...] = packed
        xd_s[0] = packed[0:1]
        xd_s[1] = packed[g.y - 1 : g.y]

    def wide_blocks(g):
        blocks = [(g.u, (c, g.near + l + 1)) for c in range(3) for l in range(3)]
        return blocks + [(g.wide, (c, l)) for c in WIDE_X for l in g.slabs]

    def wide_rows(g):
        return [
            (has_y[a], has_y[-a], rdma(g.ye_s.at[i], g.ye_r.at[1 - i], 11 + i, 19 + i, (gz, gy + a, gx)))
            for i, a in enumerate((-1, 1))
        ]

    def wide_columns(g, ups):
        made = []
        for i, b in enumerate((-1, 1)):
            for a in ups:
                if a == 0:
                    src, dst = g.xe_s, g.xe_r.at[1 - i]
                else:
                    src, dst = xd_s.at[(a + 1) // 2], xd_r.at[1 - i, (1 - a) // 2]
                made.append((
                    jnp.logical_and(has_y[a], has_x[b]), jnp.logical_and(has_y[-a], has_x[-b]),
                    rdma(src, dst, 13 + i * 3 + (a + 1), 21 + i * 3 + (a + 1), (gz, gy + a, gx + b)),
                ))
        return made

    def part_rows(g):
        made = []
        for i, a in enumerate((-1, 1)):
            for b in (-1, 1, 0):
                k = 3 * i + b + 1
                if b == 0:
                    src, dst = g.np_s.at[i], g.np_l.at[1 - i]
                else:
                    src, dst = pe_s.at[i], pe_l.at[1 - i, (1 - b) // 2]
                made.append((
                    jnp.logical_and(has_y[a], has_x[b]), jnp.logical_and(has_y[-a], has_x[-b]),
                    rdma(src, dst, 23 + k, 33 + k, (gz, gy + a, gx + b)),
                ))
        return made

    def pack_parts(g, count):
        lane1 = lanes_of(1)
        for side in range(2):
            packed = jnp.zeros((1, LANES), F32)
            for k in range(count):
                packed = jnp.where(lane1 // 4 == k, pltpu.roll(g.np_s[side, k], 4 * k + 2, 1), packed)
            pe_s[side] = packed

    def passed_parts(g):
        source, target = (npf_l.at[:, 0:6], npc_o) if g is fine else (npc_l, npf_o)
        return [(active, active, rdma(source, target, 9, 17, (opp, gy, gx))), (active, active, rdma(pe_l, pe_o, 10, 18, (opp, gy, gx)))]

    def squeeze_rows(row_of):
        for side in range(2):
            for c in range(3):
                both = row_of(side, c)
                for i in range(2):
                    k = side * 6 + 3 * i + c
                    for t in range(2):
                        sums[t, k : k + 1] = both[i, :, t * LANES : (t + 1) * LANES]
        pairs = [sums[t] + pltpu.roll(sums[t], LANES - 1, 1) for t in range(2)]
        lane16 = lanes_of(16)
        index = (2 * lane16) % LANES
        return jnp.where(lane16 < LANES // 2, pick(pairs[0], index), pick(pairs[1], index)) * 0.25

    def unpack_wide_rows(g):
        first = g.near + g.slabs[0]
        for side, (edge, second) in enumerate(((PAD - 1, PAD - 2), (PAD + g.y, PAD + g.y + 1))):
            landed = g.ye_r.at[side]
            for c in range(3):
                g.u[c, first + 1 : first + 3, second : second + 1, 0 : g.x] = landed[2 * c : 2 * c + 2]
            for i, c in enumerate(WIDE_Y):
                g.wide[c, :, edge : edge + 1, 0 : g.x] = landed[6 + 3 * i : 9 + 3 * i]

    def unpack_wide_columns(g, corners):
        own_rows = (slice(PAD, PAD + g.y), jnp.where(lanes_of(g.y) % 4 < 2, g.xe_r[0], g.xe_r[1]))
        rows = [own_rows]
        if corners:
            for side, row in enumerate((PAD - 1, PAD + g.y)):
                rows.append((slice(row, row + 1), jnp.where(lanes_of(1) % 4 < 2, xd_r[0, side], xd_r[1, side])))
        for k, (ref, index) in enumerate(wide_blocks(g)):
            for where, both in rows:
                ref[index + (where, slice(g.x, g.x + LANES))] = pltpu.roll(both, LANES - (4 * k + 2), 1)

    def interface_step(g, whole):
        if whole:
            stress_block(g.u, g.stiff, g.s, g.near + g.third, 1, g.y, g.x, g.inv, 1.0)
        for l in g.slabs:
            stress_ext(g.u, g.wide, g.s, g.near + l, l, g.y, g.x, g.inv)
        for l in g.slabs:
            step_block(g.u, g.s, g.prev, g.dens, g.out, g.near + l, 1, g.y, g.x, g.inv, 1.0)

    def beyond_edges(g):
        first = g.near + g.slabs[0]
        span = g.x + LANES
        result = []
        for side, (sign, edge, adjacent) in enumerate(((1.0, PAD, PAD - 1), (-1.0, PAD + g.y - 1, PAD + g.y))):
            scale = sign * g.inv
            d = [g.u[c, g.near + 1 : g.near + 4, edge : edge + 1, :] * scale for c in range(3)]
            w = {c: g.wide[c, :, adjacent : adjacent + 1, :] for c in WIDE_Y}
            s_xx, s_yy, s_zz, s_yz, s_xy = w[6] * d[1], w[1] * d[1], w[8] * d[1], w[3] * d[2], w[5] * d[0]

            def two(v):
                return v[g.slabs[0] : g.slabs[0] + 2, :, 0 : g.x]

            def along_x_of(v):
                v = v[g.slabs[0] : g.slabs[0] + 2]
                return (pltpu.roll(v, span - 1, 2) - pltpu.roll(v, 1, 2))[:, :, 0 : g.x] * g.inv

            def along_z_of(v):
                v = v[:, :, 0 : g.x]
                parts = []
                for l in g.slabs:
                    parts.append((v[l + 1 : l + 2] if l < 2 else 0.0) - (v[l - 1 : l] if l > 0 else 0.0))
                return jnp.concatenate(parts, 0) * g.inv

            def edge_stress(component):
                return g.s[component, first + 1 : first + 3, edge : edge + 1, 0 : g.x] * scale

            totals = (
                (
                    along_x_of(s_xx) + edge_stress(XY),
                    along_x_of(s_xy) + edge_stress(YY) + along_z_of(s_yz),
                    edge_stress(YZ) + along_z_of(s_zz),
                ),
                (two(s_xy) * scale, two(s_yy) * scale, two(s_yz) * scale),
            )
            rows = []
            for i in range(2):
                gain = (TIME_STEP * TIME_STEP) / g.ye_r[side, 21 + 2 * i : 23 + 2 * i]
                rows.append([gain * totals[i][c] for c in range(3)])
            result.append(rows)
        return result

    def start_all(copies):
        for there, _, copy in copies:
            @pl.when(there)
            def _(copy=copy):
                copy.start()

    def receive_all(copies):
        for _, comes, copy in copies:
            @pl.when(comes)
            def _(copy=copy):
                copy.wait_recv()

    def sent_all(copies):
        for there, _, copy in copies:
            @pl.when(there)
            def _(copy=copy):
                copy.wait_send()

    with jax.named_scope("load_pack"):
        loads[0].wait()
        loads[1].wait()
        for load in loads[4:]:
            load.start()
        for there, g in sides:
            @pl.when(there)
            def _(g=g):
                wide_load(g).wait()
                pack_wide_columns(g)
        pack_rows(0, (u, uc), (0, 1, 2))
        loads[2].wait()
        loads[3].wait()
        for there, g in sides:
            @pl.when(there)
            def _(g=g):
                pack_wide_rows(g)
        pack_columns(0, (u, uc), (0, 1, 2))
    with jax.named_scope("barrier"):
        pl.semaphore_wait(barrier, expected)
    with jax.named_scope("send_0"):
        for there, g in sides:
            @pl.when(there)
            def _(g=g):
                start_all(wide_columns(g, (0,)))
                start_all(wide_columns(g, (-1, 1)))
        start_round(0, (2, 3))
        for there, g in sides:
            @pl.when(there)
            def _(g=g):
                start_all(wide_rows(g))
        start_round(0, (4, 5, 0, 1))
        for load in loads[4:]:
            load.wait()
        pack_stiff_rows()

    lane = lanes_of(yc)
    even = (2 * lane) % LANES

    def squeeze(left, right, odd):
        return jnp.where(lane < LANES // 2, pick(left, even + odd), pick(right, even + odd))

    ikf_copy = rdma(own.at[6:18, 0:8], ikf_opp, 8, 16, (opp, gy, gx))
    @pl.when(is_f)
    def _():
        for c in range(3):
            inverse = 1.0 / stiff[CH[c], zf - 1]
            for t in range(2):
                tiles[c, t] = inverse[:, t * LANES : (t + 1) * LANES]
            for py in range(2):
                rows = pl.ds(py, yc, stride=2)
                left, right = tiles[c, 0, rows, :], tiles[c, 1, rows, :]
                for px in range(2):
                    own[6 + c * 4 + py * 2 + px, 0:8] = squeeze(left, right, px)

    k_copy = rdma(own.at[6:9, 0:8], own_opp.at[6:9], 8, 16, (opp, gy, gx))

    @pl.when(is_c)
    def _():
        for c in range(3):
            own[6 + c, 0:8] = cstiff[CH[c], 0] * 0.25

    def pack_own(first, last):
        lane4 = lanes_of(16) // 4
        packed = xs3[...]
        for k in range(first, last):
            packed = jnp.where(lane4 == k, pltpu.roll(own[k], 4 * k + 2, 1), packed)
        xs3[...] = packed

    @pl.when(is_f)
    def _():
        pack_own(6, 18)

    with jax.named_scope("wait_part"):
        for there, g in sides:
            @pl.when(there)
            def _(g=g):
                receive_all(wide_columns(g, (0,)))

    @pl.when(is_f)
    def _():
        unpack_wide_columns(fine, False)
        interface_step(fine, True)
        first = fine.near + fine.slabs[0]

        def two_rows(side, c):
            row = (0, yf - 2)[side]
            return fout[c, first : first + 2, row : row + 1, :] + fout[c, first : first + 2, row + 1 : row + 2, :]

        squeezed = squeeze_rows(two_rows)
        for side in range(2):
            for k in range(6):
                npf_s[side, k] = squeezed[side * 6 + k : side * 6 + k + 1]
            npf_s[side, 6:18] = own[6:18, (0, yc - 1)[side] : (1, yc)[side], :]
        pack_parts(fine, 18)
        start_all(part_rows(fine))
        ikf_copy.start()

    @pl.when(is_c)
    def _():
        unpack_wide_columns(coarse, False)
        interface_step(coarse, True)
        for side in range(2):
            for i in range(2):
                row = (i, yc - 1 - i)[side]
                for c in range(3):
                    start, below = cout[c, 0, row : row + 1, :], cout[c, 1, row : row + 1, :]
                    npc_s[side, 6 * i + c] = own[6 + c, row : row + 1] * (below - start)
                    npc_s[side, 6 * i + 3 + c] = below - 0.5 * start
        pack_parts(coarse, 12)
        start_all(part_rows(coarse))
        k_copy.start()

    def stretch_of(z):
        return jnp.where(gz * zf + z < n_z * zf // 2, metric[z : z + 1], 1.0)

    zb = min(4, zc)

    def stress_all():
        for z in range(zf):
            stress_block(u, stiff, s, z, 1, yf, xf, 0.5, stretch_of(z))
        for z in range(0, zc, zb):
            stress_block(uc, cstiff, sc, z, zb, yc, xc, 0.25, 1.0)

    def complete_stress():
        for g in (fine, coarse):
            for row, beyond, sign in ((0, PAD - 1, -1.0), (g.y - 1, PAD + g.y, 1.0)):
                d = [g.u[c, 1 : g.z + 1, beyond : beyond + 1, 0 : g.x] * (sign * g.inv) for c in range(3)]
                for component, channel, c in ((XX, 6, 1), (YY, 1, 1), (ZZ, 8, 1), (YZ, 3, 2), (XY, 5, 0)):
                    g.s[component, 1 : g.z + 1, PAD + row : PAD + row + 1, 0 : g.x] += (
                        g.stiff[channel, :, row : row + 1, :] * d[c]
                    )

    with jax.named_scope("wait_near"):
        end_round(0, (4, 5, 0, 1))
    with jax.named_scope("part_stress"):
        unpack_columns(0, (u, uc), (0, 1, 2))
        stress_all()
        pack_rows(1, (s, sc), FACE_Y)

    with jax.named_scope("wait_rows"):
        end_round(0, (2, 3))
        complete_rows()
        start_round(1, (2, 3))
        unpack_rows(0, fine, u, (0, 1, 2))
        unpack_rows(0, coarse, uc, (0, 1, 2))

    with jax.named_scope("stress"):
        complete_stress()
        pack_columns(1, (s, sc), FACE_X)
        start_round(1, (4, 5, 0, 1))

    with jax.named_scope("wait_wide"):
        for there, g in sides:
            @pl.when(there)
            def _(g=g):
                receive_all(wide_rows(g))
                receive_all(wide_columns(g, (-1, 1)))

    def pack_strips(first, last):
        pack_own(first, last)
        ys3[0] = own[0:9, 14:16, :]
        ys3[1] = own[0:9, 8:10, :]

    @pl.when(is_c)
    def _():
        unpack_wide_rows(coarse)
        unpack_wide_columns(coarse, True)
        interface_step(coarse, False)
        for c in range(3):
            start, below = cout[c, 0], cout[c, 1]
            own[c, 0:8] = own[6 + c, 0:8] * (below - start)
            own[3 + c, 0:8] = below - 0.5 * start
        for side, rows in enumerate(beyond_edges(coarse)):
            for i in range(2):
                place = (15 - i) if side == 0 else (8 + i)
                for c in range(3):
                    start, below = rows[i][c][0], rows[i][c][1]
                    k = yec_r[side, 25 + 3 * i + c] * 0.25
                    own[c, place : place + 1] = k * (below - start)
                    own[3 + c, place : place + 1] = below - 0.5 * start
                    own[6 + c, place : place + 1] = k
        pack_strips(0, 9)

    @pl.when(is_f)
    def _():
        unpack_wide_rows(fine)
        unpack_wide_columns(fine, True)
        interface_step(fine, False)
        beyond = beyond_edges(fine)
        squeezed = squeeze_rows(lambda side, c: beyond[side][0][c] + beyond[side][1][c])
        for c in range(3):
            for i, z in enumerate((zf - 2, zf - 1)):
                pairs = []
                k = 3 * i + c
                for t in range(2):
                    tiles[k, t] = fout[c, z, :, t * LANES : (t + 1) * LANES]
                    pair = tiles[k, t, pl.ds(0, yc, stride=2), :] + tiles[k, t, pl.ds(1, yc, stride=2), :]
                    pairs.append(pair + pltpu.roll(pair, LANES - 1, 1))
                own[k, 0:8] = squeeze(pairs[0], pairs[1], 0) * 0.25
        for side, place in enumerate((15, 8)):
            for k in range(6):
                own[k, place : place + 1] = squeezed[side * 6 + k : side * 6 + k + 1]
        pack_strips(0, 6)

    strips = [
        (active, active, rdma(own.at[0:6, 0:8], own_opp.at[0:6], 13, 27, (opp, gy, gx))),
        (is_f, is_c, rdma(ys3.at[:, 3:6], yo3.at[:, 3:6], 14, 28, (opp, gy, gx))),
        (is_c, is_f, rdma(ys3, yo3, 14, 28, (opp, gy, gx))),
    ]
    for level, tile_to, out, into in ((opp, xo3, 15, 31), (gz, xr3, 17, 29)):
        for i, b in enumerate((-1, 1)):
            strips.append((
                jnp.logical_and(active, has_x[b]), jnp.logical_and(active, has_x[-b]),
                rdma(xs3, tile_to.at[1 - i], out + i, into + i, (level, gy, gx + b)),
            ))
    opp_strips, level_strips = strips[:5], strips[5:]

    for there, g in sides:
        @pl.when(there)
        def _(g=g):
            sent_all(wide_columns(g, (-1, 0, 1)))

    start_all(strips)

    with jax.named_scope("wait_parts"):
        for there, g in sides:
            @pl.when(there)
            def _(g=g):
                receive_all(part_rows(g))
                start_all(passed_parts(g))

    with jax.named_scope("wait_1"):
        end_round(1, (4, 5, 0, 1))
    with jax.named_scope("step"):
        for g in (fine, coarse):
            for row in (PAD - 1, PAD + g.y):
                for c in FACE_Y:
                    clear(g.s.at[c, 1 : g.z + 1, row : row + 1, 0 : g.x])
        unpack_columns(1, (s, sc), FACE_X)
        for z in range(zf):
            step_block(u, s, fprev, dens, fout, z, 1, yf, xf, 0.5, stretch_of(z))
        for z in range(0, zc, zb):
            step_block(uc, sc, cprev, cdens, cout, z, zb, yc, xc, 0.25, 1.0)
    with jax.named_scope("wait_rows_1"):
        end_round(1, (2, 3))
        half = zc // 2
        for side, sign in enumerate((-1.0, 1.0)):
            row = (0, yf - 1)[side]
            gain = (sign * 0.5 * TIME_STEP * TIME_STEP) / dens[:, row : row + 1, :]
            for c in range(3):
                fout[c, :, row : row + 1, :] += gain * yr[1, side, c, 0:zf]
            row = (0, yc - 1)[side]
            gain = (sign * 0.25 * TIME_STEP * TIME_STEP) / cdens[:, row : row + 1, :]
            for j in range(2):
                part, cols = slice(j * half, (j + 1) * half), slice(j * xc, (j + 1) * xc)
                for c in range(3):
                    cout[c, part, row : row + 1, :] += gain[part] * yr[1, side, c, zf : zf + half, :, cols]

    lane16 = lanes_of(16)
    wide_row = lax.broadcasted_iota(jnp.int32, (16, 2 * LANES), 0)
    wide_lane = lax.broadcasted_iota(jnp.int32, (16, 2 * LANES), 1)

    def extend(k, field, centre, rims, row, edges):
        ext[k, 0:8, 0:LANES] = centre
        ext[k, 14:16, 0:LANES] = rims[0, row]
        ext[k, 8:10, 0:LANES] = rims[1, row]
        ext[k, :, LANES : 2 * LANES] = pltpu.roll(edges, LANES - (4 * field + 2), 1)

    def clamp(t):
        t = jnp.where(jnp.logical_and(wide_row == 15, gy == 0), pltpu.roll(t, 15, 0), t)
        t = jnp.where(jnp.logical_and(wide_row == 8, gy == n_y - 1), pltpu.roll(t, 1, 0), t)
        t = jnp.where(jnp.logical_and(wide_lane == 2 * LANES - 1, gx == 0), pltpu.roll(t, 2 * LANES - 1, 1), t)
        return jnp.where(jnp.logical_and(wide_lane == LANES, gx == n_x - 1), pltpu.roll(t, 1, 1), t)

    def along_y(t):
        return (0.75 * t + 0.25 * pltpu.roll(t, 1, 0), 0.75 * t + 0.25 * pltpu.roll(t, 15, 0))

    def along_x(t):
        return (0.75 * t + 0.25 * pltpu.roll(t, 1, 1), 0.75 * t + 0.25 * pltpu.roll(t, 2 * LANES - 1, 1))

    def extend_own(k, field, edges):
        ext[k, :, 0:LANES] = own[field]
        ext[k, :, LANES : 2 * LANES] = pltpu.roll(edges, LANES - (4 * field + 2), 1)

    with jax.named_scope("wait_level"):
        receive_all(level_strips)

    @pl.when(is_c)
    def _():
        edges = jnp.where(lane16 % 4 < 2, xr3[0], xr3[1])
        for k in range(3, 9):
            extend_own(k, k, edges)
        ikf_copy.wait_recv()

    @pl.when(is_f)
    def _():
        edges = jnp.where(lane16 % 4 < 2, xr3[0], xr3[1])
        for k in range(3):
            extend_own(9 + k, k, edges)
        for k in range(12):
            extend_own(12 + k, 6 + k, edges)

    with jax.named_scope("wait_opp"):
        receive_all(opp_strips)

    with jax.named_scope("wait_passed"):
        for there, g in sides:
            @pl.when(there)
            def _(g=g):
                receive_all(passed_parts(coarse if g is fine else fine))

    def part_of(parts, rims, side, field):
        edges = jnp.where(lanes_of(1) % 4 < 2, rims[side, 0], rims[side, 1])
        return jnp.concatenate([parts[side, field], pltpu.roll(edges, LANES - (4 * field + 2), 1)], 1)

    def add_part(k, parts, rims, side, field, place):
        ext[k, place : place + 1] += part_of(parts, rims, side, field)

    def set_part(k, parts, rims, side, field, place):
        ext[k, place : place + 1] = part_of(parts, rims, side, field)

    @pl.when(is_f)
    def _():
        k_copy.wait_recv()

    @pl.when(is_c)
    def _():
        edges = jnp.where(lane16 % 4 < 2, xo3[0], xo3[1])
        for c in range(3):
            extend(9 + c, 3 + c, own_opp[3 + c], yo3, 3 + c, edges)
            for side, place in enumerate((15, 8)):
                add_part(9 + c, npc_o, pe_o, side, 3 + c, place)
                add_part(3 + c, npc_l, pe_l, side, 3 + c, place)
            t1 = clamp(ext[6 + c] * (ext[3 + c] - 0.5 * ext[9 + c]))
            total = jnp.zeros((yc, LANES), F32)
            for py, part in enumerate(along_y(t1)):
                for px, full in enumerate(along_x(part[0:8])):
                    total += full[:, 0:LANES] * ikf_opp[c * 4 + py * 2 + px]
            cout[c, 0] = 0.5 * (cout[c, 0] + own_opp[c] + 0.25 * total)

    @pl.when(is_f)
    def _():
        edges = jnp.where(lane16 % 4 < 2, xo3[0], xo3[1])
        half = lane // 2
        for c in range(3):
            for k in (c, 3 + c, 6 + c):
                extend(k, k, own_opp[k], yo3, k, edges)
            for side, (place, after) in enumerate(((15, 14), (8, 9))):
                add_part(c, npf_o, pe_o, side, c, place)
                add_part(c, npf_o, pe_o, side, 6 + c, after)
                add_part(3 + c, npf_o, pe_o, side, 3 + c, place)
                add_part(9 + c, npf_l, pe_l, side, c, place)
                for k in range(4 * c, 4 * c + 4):
                    set_part(12 + k, npf_l, pe_l, side, 6 + k, place)
            total = jnp.zeros((16, 2 * LANES), F32)
            for py, part in enumerate(along_y(clamp(ext[c]))):
                for px, full in enumerate(along_x(part)):
                    total += full * ext[12 + c * 4 + py * 2 + px]
            t2 = clamp(ext[6 + c] * (ext[3 + c] - 0.5 * (ext[9 + c] + 0.25 * total)))
            for py, part in enumerate(along_y(t2)):
                evens, odds = along_x(part[0:8])
                evens, odds = evens[:, 0:LANES], odds[:, 0:LANES]
                for t in range(2):
                    index = half + t * (LANES // 2)
                    tiles[c, t, pl.ds(py, yc, stride=2), :] = jnp.where(
                        lane % 2 == 0, pick(evens, index), pick(odds, index)
                    )
            for t in range(2):
                cols = slice(t * LANES, (t + 1) * LANES)
                fout[c, zf - 1, :, cols] = fout[c, zf - 2, :, cols] + tiles[c, t] / stiff[CH[c], zf - 1, :, cols]

    with jax.named_scope("drain"):
        for d in range(6):
            @pl.when(has[d])
            def _(d=d):
                for copy in round_copies(1, d):
                    copy.wait_send()
        for d in range(6):
            @pl.when(has[d])
            def _(d=d):
                for copy in round_copies(0, d):
                    copy.wait_send()
        sent_all(strips)
        for there, g in sides:
            @pl.when(there)
            def _(g=g):
                sent_all(wide_rows(g))
                sent_all(part_rows(g))
                sent_all(passed_parts(g))

        @pl.when(is_f)
        def _():
            ikf_copy.wait_send()

        @pl.when(is_c)
        def _():
            k_copy.wait_send()


def write_out(fine, coarse, fine_out, coarse_out, sem):
    copies = [
        pltpu.make_async_copy(fine, fine_out, sem.at[0]),
        pltpu.make_async_copy(coarse, coarse_out, sem.at[1]),
    ]
    for copy in copies:
        copy.start()
    for copy in copies:
        copy.wait()


def per_device(counts, *args):
    fine, coarse = args[0].shape, args[5].shape
    _, zf, yf, xf = fine
    _, zc, yc, xc = coarse
    vmem = lambda *shape: pltpu.VMEM(shape, F32)
    anywhere = pl.BlockSpec(memory_space=pl.ANY)
    in_vmem = pl.BlockSpec(memory_space=pltpu.VMEM)
    made = pl.pallas_call(
        functools.partial(kernel, counts),
        out_shape=(pltpu.VMEM(fine, F32), pltpu.VMEM(coarse, F32)),
        in_specs=[anywhere] * 9,
        out_specs=(in_vmem, in_vmem),
        scratch_shapes=[
            vmem(3, zf + 2, yf + 2 * PAD, xf + LANES),
            vmem(3, zc + 2, yc + 2 * PAD, xc + LANES),
            vmem(6, zf + 2, yf + 2 * PAD, xf + LANES),
            vmem(6, zc + 2, yc + 2 * PAD, xc + LANES),
            vmem(3, zf, yf, xf), vmem(9, zf, yf, xf), vmem(zf, yf, xf), vmem(zf, yf, xf),
            vmem(3, zc, yc, xc), vmem(9, zc, yc, xc), vmem(zc, yc, xc),
            vmem(2, yf + yc, LANES), vmem(2, 2, yf + yc, LANES),
            vmem(2, 2, 3, zf + zc // 2, 1, xf), vmem(2, 2, 3, zf + zc // 2, 1, xf),
            vmem(9, 3, yf + 2 * PAD, xf + LANES), vmem(9, 3, yc + 2 * PAD, xc + LANES),
            vmem(2, 25, 1, xf), vmem(2, 25, 1, xf), vmem(2, 31, 1, xc), vmem(2, 31, 1, xc),
            vmem(yf, LANES), vmem(2, yf, LANES), vmem(yc, LANES), vmem(2, yc, LANES),
            vmem(2, 18, 1, LANES), vmem(2, 18, 1, LANES), vmem(2, 12, 1, LANES),
            vmem(2, 12, 1, LANES), vmem(2, 12, 1, LANES), vmem(2, 6, 1, LANES),
            vmem(2, 1, LANES), vmem(2, 2, 1, LANES), vmem(2, 2, 1, LANES),
            vmem(2, 3, zf + zc // 2, 1, xf), vmem(2, 1, LANES), vmem(2, 2, 1, LANES),
            vmem(6, 2, yf, LANES), vmem(2, 16, LANES), vmem(18, 16, LANES), vmem(9, yc, LANES), vmem(12, yc, LANES),
            vmem(2, 9, 2, LANES), vmem(2, 9, 2, LANES),
            vmem(16, LANES), vmem(2, 16, LANES), vmem(2, 16, LANES),
            vmem(24, 16, 2 * LANES),
            pltpu.SemaphoreType.DMA((10,)),
            pltpu.SemaphoreType.DMA((35,)),
            pltpu.SemaphoreType.DMA((39,)),
        ],
        compiler_params=pltpu.CompilerParams(
            collective_id=0, has_side_effects=True, vmem_limit_bytes=56 * 1024 * 1024
        ),
        name="elastic_step",
    )(*args)
    made = [pltpu.with_memory_space_constraint(part, pltpu.VMEM) for part in made]
    return pl.pallas_call(
        write_out,
        out_shape=(jax.ShapeDtypeStruct(fine, F32), jax.ShapeDtypeStruct(coarse, F32)),
        in_specs=[in_vmem, in_vmem],
        out_specs=(anywhere, anywhere),
        scratch_shapes=[pltpu.SemaphoreType.DMA((2,))],
        name="write_out",
    )(*made)


def solution(mesh):
    counts = tuple(mesh.shape[name] for name in ("gz", "gy", "gx"))
    volume, field = P(None, "gz", "gy", "gx"), P("gz", "gy", "gx")
    return jax.shard_map(
        functools.partial(per_device, counts),
        mesh=mesh,
        in_specs=(volume, volume, volume, field, field, volume, volume, volume, field),
        out_specs=(volume, volume),
        check_vma=False,
    )
```
